128 devices in a mesh: dp: 16 (over z, y), ep: 8 (over x, core).
Axes of the slice: x: 4, y: 4, z: 4, core: 2. Of those that a mesh axis runs over, the one named last changes fastest.
Arguments:
- x_tokens: bfloat16 [196608, 768], P(('dp', 'ep'))
- modality: int32 [196608], P(('dp', 'ep'))
- router: float32 [768, 8], replicated
- expert_ids: int32 [196608], P(('dp', 'ep'))
- priority: int32 [196608], P(('dp', 'ep'))
- w_in: bfloat16 [8, 768, 3072], P('ep')
- b_in: bfloat16 [8, 3072], P('ep')
- w_out: bfloat16 [8, 3072, 768], P('ep')
- b_out: bfloat16 [8, 768], P('ep')
- dy_out: bfloat16 [196608, 768], P(('dp', 'ep'))
Outputs:
- output 1: bfloat16 [196608, 768], P(('dp', 'ep'))
- output 2: float32 [], replicated
- output 3: bfloat16 [196608, 768], P(('dp', 'ep'))
- output 4: float32 [768, 8], replicated
- output 5: bfloat16 [8, 768, 3072], P('ep')
- output 6: bfloat16 [8, 3072], P('ep')
- output 7: bfloat16 [8, 3072, 768], P('ep')
- output 8: bfloat16 [8, 768], P('ep')
All inputs are finite; a program needn't handle non-finite values.
Results may differ from the reference program's by a relative error of at most 0.0160492.
Values are sent between devices in bfloat16 or wider.
A program may use at most 1 GiB of HBM per device.

```python
import jax
import jax.numpy as jnp
from jax import lax

TOKENS = 1536
WIDTH = 768
HIDDEN = 3072
EXPERTS = 8
GROUPS = 128


def setup_inputs(seed: int = 0) -> dict:
    total_tokens = TOKENS * GROUPS
    key_set = jax.random.split(jax.random.key(seed), 16)
    local_index = jnp.arange(TOKENS)[None, :]
    text_pct = jax.random.randint(key_set[0], (GROUPS, 1), 5, 41)
    modality = (jax.random.randint(key_set[1], (GROUPS, TOKENS), 0, 100) < text_pct).astype(jnp.int32)
    modality = jnp.where(local_index == 0, 0, jnp.where(local_index == 1, 1, modality))
    hot_base = jax.random.randint(key_set[2], (GROUPS, 1), 0, EXPERTS)
    hot_pick = (hot_base + jax.random.randint(key_set[3], (GROUPS, TOKENS), 0, 4)) % EXPERTS
    spread_pick = jax.random.randint(key_set[4], (GROUPS, TOKENS), 0, EXPERTS)
    use_hot = (modality == 1) & (jax.random.randint(key_set[5], (GROUPS, TOKENS), 0, 4) < 3)
    expert_ids = jnp.where(local_index < EXPERTS, local_index, jnp.where(use_hot, hot_pick, spread_pick))
    priority = jax.vmap(lambda perm_key: jax.random.permutation(perm_key, TOKENS))(jax.random.split(key_set[6], GROUPS))
    router = jax.random.normal(key_set[7], (WIDTH, EXPERTS), jnp.float32) * WIDTH ** -0.5
    boost_dir = router.T / jnp.sum(router * router, axis=0)[:, None]
    expert_onehot = (expert_ids.reshape(total_tokens, 1) == jnp.arange(EXPERTS)[None, :]).astype(jnp.float32)
    base_noise = jax.random.normal(key_set[8], (GROUPS, TOKENS, WIDTH), jnp.float32)
    group_shift = 0.5 * jax.random.normal(key_set[9], (GROUPS, 1, WIDTH), jnp.float32)
    text_shift = 0.5 * jax.random.normal(key_set[10], (WIDTH,), jnp.float32)
    x_tokens = (base_noise + group_shift + modality[:, :, None] * text_shift).reshape(total_tokens, WIDTH)
    x_tokens = x_tokens + 4.0 * jnp.dot(expert_onehot, boost_dir)
    w_in = jax.random.normal(key_set[11], (EXPERTS, WIDTH, HIDDEN), jnp.float32) * WIDTH ** -0.5
    b_in = 0.5 * jax.random.normal(key_set[12], (EXPERTS, HIDDEN), jnp.float32)
    w_out = jax.random.normal(key_set[13], (EXPERTS, HIDDEN, WIDTH), jnp.float32) * HIDDEN ** -0.5
    b_out = 0.5 * jax.random.normal(key_set[14], (EXPERTS, WIDTH), jnp.float32)
    dy_out = jax.random.normal(key_set[15], (total_tokens, WIDTH), jnp.float32) * (total_tokens * WIDTH) ** -0.5
    return dict(
        x_tokens=x_tokens.astype(jnp.bfloat16),
        modality=modality.reshape(total_tokens).astype(jnp.int32),
        router=router,
        expert_ids=expert_ids.reshape(total_tokens).astype(jnp.int32),
        priority=priority.reshape(total_tokens).astype(jnp.int32),
        w_in=w_in.astype(jnp.bfloat16),
        b_in=b_in.astype(jnp.bfloat16),
        w_out=w_out.astype(jnp.bfloat16),
        b_out=b_out.astype(jnp.bfloat16),
        dy_out=dy_out.astype(jnp.bfloat16),
    )


def route_group(expert_ids, priority):
    capacity = TOKENS // EXPERTS
    sort_order = jnp.argsort(expert_ids * TOKENS + priority)
    sorted_rank = jnp.argsort(sort_order)
    counts = jnp.sum((expert_ids[:, None] == jnp.arange(EXPERTS)[None, :]).astype(jnp.int32), axis=0)
    starts = jnp.cumsum(counts) - counts
    slot_rank = jnp.arange(capacity)
    slot_token = sort_order[jnp.minimum(starts[:, None] + slot_rank[None, :], TOKENS - 1)]
    slot_valid = slot_rank[None, :] < counts[:, None]
    position = sorted_rank - starts[expert_ids]
    return slot_token, slot_valid, position


def expert_block(operands):
    slot_rows, w_first, b_first, w_second, b_second = operands
    act_in = jnp.dot(slot_rows, w_first, preferred_element_type=jnp.float32) + b_first.astype(jnp.float32)
    hidden = jax.nn.gelu(act_in).astype(jnp.bfloat16)
    expert_out = jnp.dot(hidden, w_second, preferred_element_type=jnp.float32) + b_second.astype(jnp.float32)
    return expert_out.astype(jnp.bfloat16)


def reference(x_tokens, modality, router, expert_ids, priority, w_in, b_in, w_out, b_out, dy_out):
    total_tokens = x_tokens.shape[0]
    groups = total_tokens // TOKENS
    capacity = TOKENS // EXPERTS
    slot_token, slot_valid, position = jax.vmap(route_group)(expert_ids.reshape(groups, TOKENS), priority.reshape(groups, TOKENS))
    group_base = jnp.arange(groups)[:, None, None] * TOKENS
    slot_global = jnp.transpose(slot_token + group_base, (1, 0, 2)).reshape(EXPERTS, groups * capacity)
    valid_global = jnp.transpose(slot_valid, (1, 0, 2)).reshape(EXPERTS, groups * capacity, 1)
    position = position.reshape(total_tokens)
    keep_mask = (position < capacity)[:, None]
    group_of = jnp.arange(total_tokens) // TOKENS
    token_slot = expert_ids * (groups * capacity) + group_of * capacity + jnp.minimum(position, capacity - 1)
    expert_onehot = (expert_ids[:, None] == jnp.arange(EXPERTS)[None, :]).astype(jnp.float32)
    mod_mask = jnp.stack([modality == 0, modality == 1]).astype(jnp.float32)
    mod_count = jnp.sum(mod_mask, axis=1)

    def forward(x_in, router_in, w_first, b_first, w_second, b_second):
        logits = jnp.dot(x_in.astype(jnp.float32), router_in)
        log_probs = jax.nn.log_softmax(logits, axis=-1)
        router_probs = jnp.exp(log_probs)
        gate_prob = jnp.sum(router_probs * expert_onehot, axis=-1, keepdims=True)
        entropy = -jnp.sum(router_probs * log_probs, axis=-1)
        mean_probs = jnp.dot(mod_mask, router_probs) / mod_count[:, None]
        aux_loss = jnp.sum(jnp.dot(mod_mask, entropy) / mod_count) + jnp.sum(mean_probs * jnp.log(mean_probs))
        gathered = jnp.where(valid_global, x_in[slot_global], 0.0).astype(x_in.dtype)
        expert_out = lax.map(jax.checkpoint(expert_block), (gathered, w_first, b_first, w_second, b_second))
        y_tok = expert_out.reshape(EXPERTS * groups * capacity, WIDTH)[token_slot]
        out_tokens = jnp.where(keep_mask, gate_prob * y_tok.astype(jnp.float32), 0.0).astype(jnp.bfloat16)
        return out_tokens, aux_loss

    (out_tokens, aux_loss), pullback = jax.vjp(forward, x_tokens, router, w_in, b_in, w_out, b_out)
    dx_tokens, d_router, d_w_in, d_b_in, d_w_out, d_b_out = pullback((dy_out, jnp.ones_like(aux_loss)))
    return out_tokens, aux_loss, dx_tokens, d_router, d_w_in, d_b_in, d_w_out, d_b_out
```

```python
import functools

import jax
import jax.numpy as jnp
from jax import lax
from jax.experimental import pallas as pl
from jax.experimental.pallas import tpu as pltpu
from jax.sharding import PartitionSpec as P

ALL_AXES = ("dp", "ep")
MESH = pl.DeviceIdType.MESH
F32 = jnp.float32
BF16 = jnp.bfloat16
NOWHERE = -1.0


def col_of(row):
    return jnp.transpose(jnp.broadcast_to(row, (8, row.shape[1])))


def row_of(col):
    return jnp.transpose(jnp.broadcast_to(col, (col.shape[0], 8)))


def split3(a):
    hi = a.astype(BF16)
    rest = a - hi.astype(F32)
    mid = rest.astype(BF16)
    lo = (rest - mid.astype(F32)).astype(BF16)
    return hi, mid, lo


def nt(a, b):
    return lax.dot_general(a, b, (((1,), (1,)), ((), ())), preferred_element_type=F32)


def tn(a, b):
    return lax.dot_general(a, b, (((0,), (0,)), ((), ())), preferred_element_type=F32)


def nn(a, b):
    return jnp.dot(a, b, preferred_element_type=F32)


def route_kernel(capacity, ids_ref, prio_ref, x_ref, slot_ref, send_ref, keycol):
    n = ids_ref.shape[1]
    experts = n // capacity
    ids = ids_ref[...].astype(F32)
    key = ids * n + prio_ref[...].astype(F32)
    low = ids * n
    keycol[...] = col_of(key)

    def count(j, acc):
        col = keycol[pl.ds(pl.multiple_of(j * 128, 128), 128), :][:, 0:1]
        before = jnp.logical_and(col < key, col >= low)
        return acc + jnp.sum(before.astype(F32), axis=0, keepdims=True)

    position = lax.fori_loop(0, n // 128, count, jnp.zeros((1, n), F32))
    slot = jnp.where(position < capacity, ids * capacity + position, NOWHERE)
    slot_ref[...] = jnp.broadcast_to(slot, slot_ref.shape)

    def gather(e, carry):
        index = (lax.broadcasted_iota(jnp.int32, (capacity, n), 0) + e * capacity).astype(F32)
        pick = (index == slot).astype(BF16)
        send_ref[e] = nn(pick, x_ref[...]).astype(BF16)
        return carry

    lax.fori_loop(0, experts, gather, 0)


def router_kernel(capacity, ids_ref, mod_ref, slot_ref, x_ref, dy_ref, router3_ref, logp_ref, stats_ref, send_ref, dyt):
    n = ids_ref.shape[1]
    experts = n // capacity
    logits3 = nt(router3_ref[...], x_ref[...])
    logits = logits3[0:experts] + logits3[experts:2 * experts] + logits3[2 * experts:3 * experts]
    shifted = logits - jnp.max(logits, axis=0, keepdims=True)
    logp = shifted - jnp.log(jnp.sum(jnp.exp(shifted), axis=0, keepdims=True))
    logp_ref[...] = logp
    probs = jnp.exp(logp)
    onehot = (lax.broadcasted_iota(jnp.int32, (experts, n), 0) == ids_ref[...]).astype(F32)
    gate = jnp.sum(probs * onehot, axis=0, keepdims=True)
    entropy = -jnp.sum(probs * logp, axis=0, keepdims=True)
    stats = []
    for m in range(2):
        mask = (mod_ref[...] == m).astype(F32)
        stats.append(jnp.broadcast_to(jnp.sum(probs * mask, axis=1, keepdims=True), (experts, 128)))
        stats.append(jnp.broadcast_to(jnp.sum(entropy * mask, axis=1, keepdims=True), (8, 128)))
        stats.append(jnp.broadcast_to(jnp.sum(mask, axis=1, keepdims=True), (8, 128)))
    stats_ref[...] = jnp.concatenate(stats, axis=0)
    dyt[...] = (col_of(gate)[:, 0:1] * dy_ref[...].astype(F32)).astype(BF16)
    slot = slot_ref[0:1, :]

    def gather(e, carry):
        index = (lax.broadcasted_iota(jnp.int32, (capacity, n), 0) + e * capacity).astype(F32)
        pick = (index == slot).astype(BF16)
        send_ref[e] = nn(pick, dyt[...]).astype(BF16)
        return carry

    lax.fori_loop(0, experts, gather, 0)


def forward_kernel(steps, chunks, rows_ref, w_in_ref, b_in_ref, w_out_ref, b_out_ref, hidden_ref, slope_ref, y_ref, acc):
    step = pl.program_id(0)
    n = rows_ref.shape[0]
    size = n // chunks

    @pl.when(step == 0)
    def _():
        acc[...] = jnp.broadcast_to(b_out_ref[...].astype(F32), acc.shape)

    for c in range(chunks):
        part = pl.ds(c * size, size)
        a = nn(rows_ref[part, :], w_in_ref[...]) + b_in_ref[...].astype(F32)
        root = 0.7978845608028654
        sq = a * a
        t = jnp.tanh(root * (a + 0.044715 * (sq * a)))
        half = 0.5 * (1.0 + t)
        hidden = (a * half).astype(BF16)
        slope_ref[part, :] = half + (0.5 * root) * a * (1.0 - t * t) * (1.0 + (3 * 0.044715) * sq)
        hidden_ref[part, :] = hidden
        acc[part, :] += nn(hidden, w_out_ref[...])

    @pl.when(step == steps - 1)
    def _():
        y_ref[...] = acc[...].astype(BF16)


def dwout_kernel(hidden_ref, d_ref, dw_ref):
    dw_ref[...] = tn(hidden_ref[...], d_ref[...])


def backward_kernel(steps, chunks, rows_ref, d_ref, slope_ref, w_in_ref, w_out_ref, dw_ref, db_in_ref, db_out_ref, d_rows_ref, acc, act):
    step = pl.program_id(0)
    n = rows_ref.shape[0]
    size = n // chunks

    @pl.when(step == 0)
    def _():
        db_out_ref[...] = jnp.sum(d_ref[...].astype(F32), axis=0, keepdims=True)
        acc[...] = jnp.zeros_like(acc)

    total = jnp.zeros(db_in_ref.shape, F32)
    for c in range(chunks):
        part = pl.ds(c * size, size)
        d_hidden = nt(d_ref[part, :], w_out_ref[...]).astype(BF16)
        d_act = d_hidden.astype(F32) * slope_ref[part, :]
        total += jnp.sum(d_act, axis=0, keepdims=True)
        d_act_bf = d_act.astype(BF16)
        act[part, :] = d_act_bf
        acc[part, :] += nt(d_act_bf, w_in_ref[...])
    db_in_ref[...] = total
    dw_ref[...] = tn(rows_ref[...], act[...])

    @pl.when(step == steps - 1)
    def _():
        d_rows_ref[...] = acc[...].astype(BF16)


def global_terms(stats, experts):
    loss = jnp.zeros((1, 128), F32)
    terms = []
    inv = []
    for m in range(2):
        base = 24 * m
        count = stats[base + 16:base + 17]
        mean = stats[base:base + 8] / count
        log_mean = jnp.log(mean)
        loss = loss + stats[base + 8:base + 9] / count + jnp.sum(mean * log_mean, axis=0, keepdims=True)
        terms.append(log_mean / count)
        inv.append(1.0 / count)
    return loss, terms, inv


def combine_kernel(capacity, chunks, ids_ref, mod_ref, slot_ref, logp_ref, back_ref, dy_ref, x_ref, stats_ref, out_ref, dlog_ref, dr_ref, loss_ref):
    n = ids_ref.shape[1]
    experts = n // capacity
    size = n // chunks
    loss, terms, inv = global_terms(stats_ref[...], experts)
    loss_ref[...] = jnp.broadcast_to(loss, loss_ref.shape)
    dr = jnp.zeros((3 * experts, x_ref.shape[1]), F32)
    for c in range(chunks):
        part = pl.ds(c * size, size)
        lanes = pl.ds(c * size, size)
        slot_col = col_of(slot_ref[0:1, lanes])[:, 0:1]
        pick = (lax.broadcasted_iota(jnp.int32, (size, n), 1).astype(F32) == slot_col).astype(BF16)
        y = nn(pick, back_ref[...])
        logp = logp_ref[:, lanes]
        probs = jnp.exp(logp)
        onehot = (lax.broadcasted_iota(jnp.int32, (experts, size), 0) == ids_ref[:, lanes]).astype(F32)
        gate = jnp.sum(probs * onehot, axis=0, keepdims=True)
        out_ref[part, :] = (col_of(gate)[:, 0:1] * y).astype(BF16)
        d_gate = row_of(jnp.sum(dy_ref[part, :].astype(F32) * y, axis=1, keepdims=True))[0:1]
        is_text = mod_ref[:, lanes] == 1
        global_part = jnp.where(is_text, terms[1][:, 0:1], terms[0][:, 0:1])
        inv_count = jnp.where(is_text, inv[1][:, 0:1], inv[0][:, 0:1])
        d_probs = onehot * d_gate + global_part - logp * inv_count
        d_log = probs * (d_probs - jnp.sum(d_probs * probs, axis=0, keepdims=True))
        dlog_ref[:, lanes] = d_log
        dr += nn(jnp.concatenate(split3(d_log), axis=0), x_ref[part, :])
    dr_ref[...] = dr[0:experts] + dr[experts:2 * experts] + dr[2 * experts:]


def token_grad_kernel(chunks, slot_ref, dlog_ref, back_ref, router_ref, dx_ref):
    n = slot_ref.shape[1]
    size = n // chunks
    r = split3(router_ref[...])
    rights = jnp.concatenate([r[0], r[1], r[0], r[1], r[2], r[0]], axis=0)
    for c in range(chunks):
        part = pl.ds(c * size, size)
        lanes = pl.ds(c * size, size)
        slot_col = col_of(slot_ref[0:1, lanes])[:, 0:1]
        pick = (lax.broadcasted_iota(jnp.int32, (size, n), 1).astype(F32) == slot_col).astype(BF16)
        d = split3(dlog_ref[:, lanes])
        lefts = jnp.concatenate([d[0], d[0], d[1], d[1], d[0], d[2]], axis=0)
        routed = tn(lefts, rights).astype(BF16)
        expert = nn(pick, back_ref[...])
        dx_ref[part, :] = (expert + routed.astype(F32)).astype(BF16)


def reduce_kernel(whole_rows, a_ref, o_ref, bufs, send_sem, recv_sem, pair_send, pair_recv, work):
    dp = lax.axis_index("dp")
    ep = lax.axis_index("ep")
    z, y = dp // 4, lax.rem(dp, 4)
    x, core = ep // 2, lax.rem(ep, 2)
    partner = (dp, x * 2 + 1 - core)
    rings = []
    for axis in range(3):
        me = (x, y, z)[axis]
        peers = []
        for k in range(1, 4):
            to = lax.rem(me + k, 4)
            peers.append(((dp, to * 2 + core), (z * 4 + to, ep), (to * 4 + y, ep))[axis])
        rings.append((me, peers))

    barrier = pltpu.get_barrier_semaphore()
    everyone = [partner] + [p for _, peers in rings for p in peers]
    for p in everyone:
        pl.semaphore_signal(barrier, inc=1, device_id=p, device_id_type=MESH)
    pl.semaphore_wait(barrier, len(everyone))

    head = pl.ds(0, whole_rows)
    work[0] = a_ref[...]
    pair = pltpu.make_async_remote_copy(
        src_ref=work.at[0, head], dst_ref=work.at[1, head], send_sem=pair_send, recv_sem=pair_recv,
        device_id=partner, device_id_type=MESH)
    pair.start()
    pair.wait()
    work[2] = a_ref[...]
    work[2, head, :] = work[0, head, :] + work[1, head, :]
    for axis in range(3):
        me, peers = rings[axis]
        rows = head if axis == 0 else pl.ds(0, a_ref.shape[0])
        bufs[axis, me] = work[axis + 2]
        copies = []
        for k in range(3):
            copy = pltpu.make_async_remote_copy(
                src_ref=work.at[axis + 2, rows], dst_ref=bufs.at[axis, me, rows], send_sem=send_sem.at[axis, k],
                recv_sem=recv_sem.at[axis, k], device_id=peers[k], device_id_type=MESH)
            copy.start()
            copies.append(copy)
        for copy in copies:
            copy.wait()
        total = bufs[axis, 0, rows, :] + bufs[axis, 1, rows, :] + bufs[axis, 2, rows, :] + bufs[axis, 3, rows, :]
        if axis == 2:
            o_ref[...] = total
        else:
            work[axis + 3] = work[axis + 2]
            work[axis + 3, rows, :] = total


def small_reduce(a, whole_rows, collective_id):
    rows, cols = a.shape
    return pl.pallas_call(
        functools.partial(reduce_kernel, whole_rows),
        out_shape=jax.ShapeDtypeStruct((rows, cols), F32),
        in_specs=[pl.BlockSpec(memory_space=pltpu.VMEM)],
        out_specs=pl.BlockSpec(memory_space=pltpu.VMEM),
        scratch_shapes=[
            pltpu.VMEM((3, 4, rows, cols), F32),
            pltpu.SemaphoreType.DMA((3, 3)),
            pltpu.SemaphoreType.DMA((3, 3)),
            pltpu.SemaphoreType.DMA,
            pltpu.SemaphoreType.DMA,
            pltpu.VMEM((5, rows, cols), F32),
        ],
        compiler_params=pltpu.CompilerParams(collective_id=collective_id, has_side_effects=True),
        cost_estimate=pl.CostEstimate(flops=2_000_000_000, bytes_accessed=100_000, transcendentals=0),
        name=f"small_reduce_{collective_id}",
    )(a)


def vmem(count):
    return [pl.BlockSpec(memory_space=pltpu.VMEM)] * count


def params():
    return pltpu.CompilerParams(vmem_limit_bytes=60 * 1024 * 1024)


def cost(flops, size):
    return pl.CostEstimate(flops=int(flops), bytes_accessed=int(size), transcendentals=0)


def solution(mesh):
    token_spec = P(ALL_AXES)
    expert_spec = P("ep")

    def local_step(x, modality, router, expert_ids, priority, w_in, b_in, w_out, b_out, dy):
        n, width = x.shape
        experts = router.shape[1]
        hid = w_in.shape[2]
        capacity = n // experts
        w_in, w_out = w_in[0], w_out[0]
        ids = expert_ids.reshape(1, n)
        prio = priority.reshape(1, n)
        mod = modality.reshape(1, n)
        router_t = jnp.transpose(router)
        router3 = jnp.concatenate(split3_outside(router_t), axis=0)
        shape = jax.ShapeDtypeStruct
        gather_flops = 2 * n * n * width

        slot, send_rows = pl.pallas_call(
            functools.partial(route_kernel, capacity),
            out_shape=(shape((8, n), F32), shape((experts, capacity, width), BF16)),
            in_specs=vmem(3), out_specs=tuple(vmem(2)),
            scratch_shapes=[pltpu.VMEM((n, 8), F32)],
            compiler_params=params(), cost_estimate=cost(gather_flops, 4 * n * width), name="route",
        )(ids, prio, x)
        recv_rows = lax.all_to_all(send_rows, "ep", 0, 0, tiled=True).reshape(n, width)

        logp, stats_part, send_d = pl.pallas_call(
            functools.partial(router_kernel, capacity),
            out_shape=(shape((experts, n), F32), shape((48, 128), F32), shape((experts, capacity, width), BF16)),
            in_specs=vmem(6), out_specs=tuple(vmem(3)),
            scratch_shapes=[pltpu.VMEM((n, width), BF16)],
            compiler_params=params(), cost_estimate=cost(gather_flops, 6 * n * width), name="router",
        )(ids, mod, slot, x, dy, router3)
        d_recv = lax.all_to_all(send_d, "ep", 0, 0, tiled=True).reshape(n, width)
        stats = small_reduce(stats_part, 48, 1)

        tile = 512
        steps = hid // tile
        whole = pl.BlockSpec((n, width), lambda i: (0, 0))
        w_in_spec = pl.BlockSpec((width, tile), lambda i: (0, i))
        w_out_spec = pl.BlockSpec((tile, width), lambda i: (i, 0))
        act_spec = pl.BlockSpec((n, tile), lambda i: (0, i))
        hid_row = pl.BlockSpec((1, tile), lambda i: (0, i))
        width_row = pl.BlockSpec((1, width), lambda i: (0, 0))
        mm = 2 * n * width * hid

        hidden, slope, y = pl.pallas_call(
            functools.partial(forward_kernel, steps, 4),
            grid=(steps,),
            out_shape=(shape((n, hid), BF16), shape((n, hid), F32), shape((n, width), BF16)),
            in_specs=[whole, w_in_spec, hid_row, w_out_spec, width_row],
            out_specs=(act_spec, act_spec, whole),
            scratch_shapes=[pltpu.VMEM((n, width), F32)],
            compiler_params=params(), cost_estimate=cost(2 * mm, 6 * n * hid), name="expert_forward",
        )(recv_rows, w_in, b_in, w_out, b_out)
        back_y = lax.all_to_all(y.reshape(experts, capacity, width), "ep", 0, 0, tiled=True).reshape(n, width)

        d_w_out = pl.pallas_call(
            dwout_kernel,
            grid=(steps,),
            out_shape=shape((hid, width), F32),
            in_specs=[act_spec, whole],
            out_specs=w_out_spec,
            compiler_params=params(), cost_estimate=cost(mm, 2 * n * hid), name="expert_dwout",
        )(hidden, d_recv)
        d_w_out = gather_sum(d_w_out)

        d_w_in, d_b_in, d_b_out, d_rows = pl.pallas_call(
            functools.partial(backward_kernel, steps, 4),
            grid=(steps,),
            out_shape=(shape((width, hid), F32), shape((1, hid), F32), shape((1, width), F32), shape((n, width), BF16)),
            in_specs=[whole, whole, act_spec, w_in_spec, w_out_spec],
            out_specs=(w_in_spec, hid_row, width_row, whole),
            scratch_shapes=[pltpu.VMEM((n, width), F32), pltpu.VMEM((n, tile), BF16)],
            compiler_params=params(), cost_estimate=cost(3 * mm, 6 * n * hid), name="expert_backward",
        )(recv_rows, d_recv, slope, w_in, w_out)
        d_w_in = gather_sum(d_w_in)
        d_back = lax.all_to_all(d_rows.reshape(experts, capacity, width), "ep", 0, 0, tiled=True).reshape(n, width)

        out, d_log, d_router_part, loss = pl.pallas_call(
            functools.partial(combine_kernel, capacity, 4),
            out_shape=(shape((n, width), BF16), shape((experts, n), F32), shape((experts, width), F32), shape((8, 128), F32)),
            in_specs=vmem(8), out_specs=tuple(vmem(4)),
            compiler_params=params(), cost_estimate=cost(gather_flops, 8 * n * width), name="combine",
        )(ids, mod, slot, logp, back_y, dy, x, stats)

        d_x = pl.pallas_call(
            functools.partial(token_grad_kernel, 4),
            out_shape=shape((n, width), BF16),
            in_specs=vmem(4), out_specs=vmem(1)[0],
            compiler_params=params(), cost_estimate=cost(gather_flops, 6 * n * width), name="token_grad",
        )(slot, d_log, d_back, router_t)

        small = jnp.concatenate([d_router_part, d_b_in.reshape(hid // width, width), d_b_out, jnp.zeros((3, width), F32)], axis=0)
        small = small_reduce(small, experts, 2)
        d_router = jnp.transpose(small[0:experts])
        d_b_in = small[experts:experts + hid // width].reshape(1, hid).astype(BF16)
        d_b_out = small[experts + hid // width:experts + hid // width + 1].astype(BF16)
        return out, loss[0, 0], d_x, d_router, d_w_in[None], d_b_in, d_w_out[None], d_b_out

    def gather_sum(part):
        own = lax.psum_scatter(part, "dp", scatter_dimension=0, tiled=True)
        return lax.all_gather(own.astype(BF16), "dp", axis=0, tiled=True)

    def split3_outside(a):
        hi = lax.reduce_precision(a, 8, 7)
        mid = lax.reduce_precision(a - hi, 8, 7)
        return hi.astype(BF16), mid.astype(BF16), (a - hi - mid).astype(BF16)

    return jax.shard_map(
        local_step,
        mesh=mesh,
        in_specs=(token_spec, token_spec, P(), token_spec, token_spec, expert_spec, expert_spec, expert_spec, expert_spec, token_spec),
        out_specs=(token_spec, P(), token_spec, P(), expert_spec, expert_spec, expert_spec, expert_spec),
        check_vma=False,
    )
```

```python
import functools

import jax
import jax.numpy as jnp
from jax import lax
from jax.experimental import pallas as pl
from jax.experimental.pallas import tpu as pltpu
from jax.sharding import PartitionSpec as P

ALL_AXES = ("dp", "ep")
MESH = pl.DeviceIdType.MESH
F32 = jnp.float32
BF16 = jnp.bfloat16
NOWHERE = -1.0
TILE = 256


def col_of(row):
    return jnp.transpose(jnp.broadcast_to(row, (8, row.shape[1])))


def row_of(col):
    return jnp.transpose(jnp.broadcast_to(col, (col.shape[0], 8)))


def split3(a):
    hi = a.astype(BF16)
    rest = a - hi.astype(F32)
    mid = rest.astype(BF16)
    lo = (rest - mid.astype(F32)).astype(BF16)
    return hi, mid, lo


def nt(a, b):
    return lax.dot_general(a, b, (((1,), (1,)), ((), ())), preferred_element_type=F32)


def tn(a, b):
    return lax.dot_general(a, b, (((0,), (0,)), ((), ())), preferred_element_type=F32)


def nn(a, b):
    return jnp.dot(a, b, preferred_element_type=F32)


def route_kernel(capacity, ids_ref, prio_ref, x_ref, slot_ref, send_ref, keycol):
    n = ids_ref.shape[1]
    experts = n // capacity
    ids = ids_ref[...].astype(F32)
    key = ids * n + prio_ref[...].astype(F32)
    low = ids * n
    keycol[...] = col_of(key)

    def count(j, acc):
        col = keycol[pl.ds(pl.multiple_of(j * 128, 128), 128), :][:, 0:1]
        before = jnp.logical_and(col < key, col >= low)
        return acc + jnp.sum(before.astype(F32), axis=0, keepdims=True)

    position = lax.fori_loop(0, n // 128, count, jnp.zeros((1, n), F32))
    slot = jnp.where(position < capacity, ids * capacity + position, NOWHERE)
    slot_ref[...] = jnp.broadcast_to(slot, slot_ref.shape)

    def gather(e, carry):
        index = (lax.broadcasted_iota(jnp.int32, (capacity, n), 0) + e * capacity).astype(F32)
        pick = (index == slot).astype(BF16)
        send_ref[e] = nn(pick, x_ref[...]).astype(BF16)
        return carry

    lax.fori_loop(0, experts, gather, 0)


def router_kernel(capacity, ids_ref, mod_ref, slot_ref, x_ref, dy_ref, router3_ref, logp_ref, stats_ref, send_ref, dyt):
    n = ids_ref.shape[1]
    experts = n // capacity
    logits3 = nt(router3_ref[...], x_ref[...])
    logits = logits3[0:experts] + logits3[experts:2 * experts] + logits3[2 * experts:3 * experts]
    shifted = logits - jnp.max(logits, axis=0, keepdims=True)
    logp = shifted - jnp.log(jnp.sum(jnp.exp(shifted), axis=0, keepdims=True))
    logp_ref[...] = logp
    probs = jnp.exp(logp)
    onehot = (lax.broadcasted_iota(jnp.int32, (experts, n), 0) == ids_ref[...]).astype(F32)
    gate = jnp.sum(probs * onehot, axis=0, keepdims=True)
    entropy = -jnp.sum(probs * logp, axis=0, keepdims=True)
    stats = []
    for m in range(2):
        mask = (mod_ref[...] == m).astype(F32)
        stats.append(jnp.broadcast_to(jnp.sum(probs * mask, axis=1, keepdims=True), (experts, 128)))
        stats.append(jnp.broadcast_to(jnp.sum(entropy * mask, axis=1, keepdims=True), (8, 128)))
        stats.append(jnp.broadcast_to(jnp.sum(mask, axis=1, keepdims=True), (8, 128)))
    stats_ref[...] = jnp.concatenate(stats, axis=0)
    dyt[...] = (col_of(gate)[:, 0:1] * dy_ref[...].astype(F32)).astype(BF16)
    slot = slot_ref[0:1, :]

    def gather(e, carry):
        index = (lax.broadcasted_iota(jnp.int32, (capacity, n), 0) + e * capacity).astype(F32)
        pick = (index == slot).astype(BF16)
        send_ref[e] = nn(pick, dyt[...]).astype(BF16)
        return carry

    lax.fori_loop(0, experts, gather, 0)


def forward_kernel(steps, chunks, rows_ref, w_in_ref, b_in_ref, w_out_ref, b_out_ref, hidden_t_ref, slope_ref, rows_t_ref, y_ref, acc):
    step = pl.program_id(0)
    n = rows_ref.shape[0]
    size = n // chunks

    @pl.when(step == 0)
    def _():
        acc[...] = jnp.broadcast_to(b_out_ref[...].astype(F32), acc.shape)
        rows_t_ref[...] = jnp.transpose(rows_ref[...])

    for c in range(chunks):
        part = pl.ds(c * size, size)
        a = nn(rows_ref[part, :], w_in_ref[...]) + b_in_ref[...].astype(F32)
        root = 0.7978845608028654
        sq = a * a
        t = jnp.tanh(root * (a + 0.044715 * (sq * a)))
        half = 0.5 * (1.0 + t)
        hidden = (a * half).astype(BF16)
        slope = half + (0.5 * root) * a * (1.0 - t * t) * (1.0 + (3 * 0.044715) * sq)
        for j in range(slope_ref.shape[0]):
            slope_ref[j, part, :] = slope[:, j * TILE:(j + 1) * TILE]
        hidden_t_ref[:, part] = jnp.transpose(hidden)
        acc[part, :] += nn(hidden, w_out_ref[...])

    @pl.when(step == steps - 1)
    def _():
        y_ref[...] = acc[...].astype(BF16)


def grads_kernel(
    hidden_t, slope, w_in, w_out, rows_t, d_rows_in, y, summed, db_in, db_out, back_y, back_d,
    part_sum, land_a, land_b, own, hbuf, sbuf, ibuf, obuf, act, acc, d_out,
    send_sem, recv_sem, own_sem, load_sem, load2_sem, y_send, y_recv, d_send, d_recv, self_sem,
):
    dp = lax.axis_index("dp")
    ep = lax.axis_index("ep")
    z, yy = dp // 4, lax.rem(dp, 4)
    tiles = part_sum.shape[0]
    units = tiles // 4
    half = tiles // 2
    experts = y.shape[0]
    n, width = acc.shape
    chunks = 4
    size = n // chunks

    def place(stream):
        way = 1 - 2 * lax.rem(stream, 2)
        first_z = stream // 2
        pa = yy * (1 - first_z) + z * first_z
        pb = z * (1 - first_z) + yy * first_z
        y_next, z_next = lax.rem(yy + way + 4, 4), lax.rem(z + way + 4, 4)
        along_y, along_z = z * 4 + y_next, z_next * 4 + yy
        next_a = along_y * (1 - first_z) + along_z * first_z
        next_b = along_z * (1 - first_z) + along_y * first_z
        return way, pa, pb, next_a, next_b

    def wrap(v):
        return lax.rem(v + 16, 4)

    def send(tile, k):
        way, pa, pb, next_a, next_b = place(lax.rem(tile, 4))
        if k < 3:
            src, dst, to = part_sum.at[tile, wrap(pa - way * (k + 1))], land_a.at[tile, k], next_a
        elif k < 6:
            src, dst, to = part_sum.at[tile, pa, wrap(pb - way * (k - 2))], land_b.at[tile, k - 3], next_b
        elif k == 6:
            src, dst, to = own.at[tile], summed.at[tile, pa, pb], next_b
        elif k < 9:
            src = summed.at[tile, pa, wrap(pb - way * (k - 6))]
            dst, to = src, next_b
        else:
            src = summed.at[tile, wrap(pa - way * (k - 9))]
            dst, to = src, next_a
        return pltpu.make_async_remote_copy(
            src_ref=src, dst_ref=dst, send_sem=send_sem.at[tile, k], recv_sem=recv_sem.at[tile, k],
            device_id=(to, ep), device_id_type=MESH)

    def keep(tile):
        way, pa, pb, _, _ = place(lax.rem(tile, 4))
        return pltpu.make_async_copy(own.at[tile], summed.at[tile, pa, pb], own_sem.at[tile])

    def advance(tile, k):
        way, pa, pb, _, _ = place(lax.rem(tile, 4))
        send(tile, k - 1).wait_recv()
        if k <= 3:
            block = wrap(pa - way * (k + 1))
            part_sum[tile, block] = part_sum[tile, block] + land_a[tile, k - 1]
        elif k <= 6:
            block = wrap(pb - way * (k - 2))
            total = part_sum[tile, pa, block] + land_b[tile, k - 4]
            if k < 6:
                part_sum[tile, pa, block] = total
            else:
                own[tile] = total.astype(BF16)
                keep(tile).start()
        elif k == 9:
            keep(tile).wait()
        if k < 12:
            send(tile, k).start()

    def wave(t, stream):
        for k in range(12, 0, -1):
            unit = t - k

            @pl.when(jnp.logical_and(unit >= 0, unit < units))
            def _():
                advance(unit * 4 + stream, k)

    def exchange(src, dst, send_sems, recv_sems):
        copies = []
        for j in range(1, experts):
            to = lax.rem(ep + j, experts)
            copies.append(pltpu.make_async_remote_copy(
                src_ref=src.at[to], dst_ref=dst.at[ep], send_sem=send_sems.at[j - 1], recv_sem=recv_sems.at[j - 1],
                device_id=(dp, to), device_id_type=MESH))
        return copies

    def load_hidden(i):
        slot = lax.rem(i, 2)
        return pltpu.make_async_copy(hidden_t.at[pl.ds(pl.multiple_of(i * TILE, TILE), TILE)], hbuf.at[slot], load_sem.at[slot])

    def load_rest(i):
        slot = lax.rem(i, 2)
        at = pl.ds(pl.multiple_of(i * TILE, TILE), TILE)
        return (
            pltpu.make_async_copy(slope.at[i], sbuf.at[slot], load2_sem.at[slot, 0]),
            pltpu.make_async_copy(w_in.at[:, at], ibuf.at[slot], load2_sem.at[slot, 1]),
            pltpu.make_async_copy(w_out.at[at], obuf.at[slot], load2_sem.at[slot, 2]),
        )

    load_hidden(0).start()
    for copy in load_rest(0):
        copy.start()

    barrier = pltpu.get_barrier_semaphore()
    peers = [(z * 4 + wrap(yy + 1), ep), (z * 4 + wrap(yy - 1), ep), (wrap(z + 1) * 4 + yy, ep), (wrap(z - 1) * 4 + yy, ep)]
    peers += [(dp, lax.rem(ep + j, experts)) for j in range(1, experts)]
    for peer in peers:
        pl.semaphore_signal(barrier, inc=1, device_id=peer, device_id_type=MESH)
    pl.semaphore_wait(barrier, len(peers))

    send_y = exchange(y, back_y, y_send, y_recv)
    for copy in send_y:
        copy.start()
    self_y = pltpu.make_async_copy(y.at[ep], back_y.at[ep], self_sem.at[0])
    self_y.start()
    acc[...] = jnp.zeros_like(acc)
    db_out[...] = jnp.sum(d_rows_in[...].astype(F32), axis=0, keepdims=True)

    def out_tile(i, carry):
        wave(i // 4, lax.rem(i, 4))
        slot = lax.rem(i, 2)
        load_hidden(i).wait()

        @pl.when(i + 1 < half)
        def _():
            load_hidden(i + 1).start()

        grad = nn(hbuf[slot], d_rows_in[...])
        part_sum[i] = grad.reshape(part_sum.shape[1:])
        send(i, 0).start()
        return carry

    lax.fori_loop(0, half, out_tile, 0)

    def in_tile(i, carry):
        g = i + half
        wave(g // 4, lax.rem(g, 4))
        slot = lax.rem(i, 2)
        for copy in load_rest(i):
            copy.wait()

        @pl.when(i + 1 < half)
        def _():
            for copy in load_rest(i + 1):
                copy.start()

        total = jnp.zeros((1, TILE), F32)
        for c in range(chunks):
            part = pl.ds(c * size, size)
            d_hidden = nt(d_rows_in[part, :], obuf[slot]).astype(BF16)
            d_act = d_hidden.astype(F32) * sbuf[slot, part, :]
            total += jnp.sum(d_act, axis=0, keepdims=True)
            d_act_bf = d_act.astype(BF16)
            act[part, :] = d_act_bf
            acc[part, :] += nt(d_act_bf, ibuf[slot])
        db_in[:, pl.ds(pl.multiple_of(i * TILE, TILE), TILE)] = total
        rows = width // 4
        for a in range(4):
            grad = nn(rows_t[pl.ds(a * rows, rows), :], act[...])
            for b in range(4):
                for j in range(3):
                    at = b * (rows // 4) + j * 16
                    part_sum[g, a, b, :, j * TILE:(j + 1) * TILE] = grad[at:at + 16, :]
        send(g, 0).start()
        return carry

    lax.fori_loop(0, half, in_tile, 0)

    d_out[...] = acc[...].astype(BF16).reshape(d_out.shape)
    send_d = exchange(d_out, back_d, d_send, d_recv)
    for copy in send_d:
        copy.start()
    self_d = pltpu.make_async_copy(d_out.at[ep], back_d.at[ep], self_sem.at[1])
    self_d.start()

    def rest(t, carry):
        def streams(s, inner):
            wave(t, s)
            return inner

        return lax.fori_loop(0, 4, streams, carry)

    lax.fori_loop(units, units + 12, rest, 0)

    def drain(tile, carry):
        for k in range(12):
            send(tile, k).wait_send()
        return carry

    lax.fori_loop(0, tiles, drain, 0)
    for copy in send_y + send_d:
        copy.wait()
    self_y.wait()
    self_d.wait()


def unpack_kernel(sum_ref, dw_ref):
    width = dw_ref.shape[0]
    rows = width // 4
    for a in range(4):
        for b in range(4):
            for j in range(3):
                at = a * rows + b * (rows // 4) + j * 16
                dw_ref[at:at + 16, :] = sum_ref[0, a, b, :, j * TILE:(j + 1) * TILE]


def global_terms(stats, experts):
    loss = jnp.zeros((1, 128), F32)
    terms = []
    inv = []
    for m in range(2):
        base = 24 * m
        count = stats[base + 16:base + 17]
        mean = stats[base:base + 8] / count
        log_mean = jnp.log(mean)
        loss = loss + stats[base + 8:base + 9] / count + jnp.sum(mean * log_mean, axis=0, keepdims=True)
        terms.append(log_mean / count)
        inv.append(1.0 / count)
    return loss, terms, inv


def combine_kernel(capacity, chunks, ids_ref, mod_ref, slot_ref, logp_ref, back_ref, dy_ref, x_ref, stats_ref, out_ref, dlog_ref, dr_ref, loss_ref):
    n = ids_ref.shape[1]
    experts = n // capacity
    size = n // chunks
    loss, terms, inv = global_terms(stats_ref[...], experts)
    loss_ref[...] = jnp.broadcast_to(loss, loss_ref.shape)
    dr = jnp.zeros((3 * experts, x_ref.shape[1]), F32)
    for c in range(chunks):
        part = pl.ds(c * size, size)
        lanes = pl.ds(c * size, size)
        slot_col = col_of(slot_ref[0:1, lanes])[:, 0:1]
        pick = (lax.broadcasted_iota(jnp.int32, (size, n), 1).astype(F32) == slot_col).astype(BF16)
        y = nn(pick, back_ref[...])
        logp = logp_ref[:, lanes]
        probs = jnp.exp(logp)
        onehot = (lax.broadcasted_iota(jnp.int32, (experts, size), 0) == ids_ref[:, lanes]).astype(F32)
        gate = jnp.sum(probs * onehot, axis=0, keepdims=True)
        out_ref[part, :] = (col_of(gate)[:, 0:1] * y).astype(BF16)
        d_gate = row_of(jnp.sum(dy_ref[part, :].astype(F32) * y, axis=1, keepdims=True))[0:1]
        is_text = mod_ref[:, lanes] == 1
        global_part = jnp.where(is_text, terms[1][:, 0:1], terms[0][:, 0:1])
        inv_count = jnp.where(is_text, inv[1][:, 0:1], inv[0][:, 0:1])
        d_probs = onehot * d_gate + global_part - logp * inv_count
        d_log = probs * (d_probs - jnp.sum(d_probs * probs, axis=0, keepdims=True))
        dlog_ref[:, lanes] = d_log
        dr += nn(jnp.concatenate(split3(d_log), axis=0), x_ref[part, :])
    dr_ref[...] = dr[0:experts] + dr[experts:2 * experts] + dr[2 * experts:]


def token_grad_kernel(chunks, slot_ref, dlog_ref, back_ref, router_ref, dx_ref):
    n = slot_ref.shape[1]
    size = n // chunks
    r = split3(router_ref[...])
    rights = jnp.concatenate([r[0], r[1], r[0], r[1], r[2], r[0]], axis=0)
    for c in range(chunks):
        part = pl.ds(c * size, size)
        lanes = pl.ds(c * size, size)
        slot_col = col_of(slot_ref[0:1, lanes])[:, 0:1]
        pick = (lax.broadcasted_iota(jnp.int32, (size, n), 1).astype(F32) == slot_col).astype(BF16)
        d = split3(dlog_ref[:, lanes])
        lefts = jnp.concatenate([d[0], d[0], d[1], d[1], d[0], d[2]], axis=0)
        routed = tn(lefts, rights).astype(BF16)
        expert = nn(pick, back_ref[...])
        dx_ref[part, :] = (expert + routed.astype(F32)).astype(BF16)


def reduce_kernel(whole_rows, a_ref, o_ref, bufs, send_sem, recv_sem, pair_send, pair_recv, work):
    dp = lax.axis_index("dp")
    ep = lax.axis_index("ep")
    z, y = dp // 4, lax.rem(dp, 4)
    x, core = ep // 2, lax.rem(ep, 2)
    partner = (dp, x * 2 + 1 - core)
    rings = []
    for axis in range(3):
        me = (x, y, z)[axis]
        peers = []
        for k in range(1, 4):
            to = lax.rem(me + k, 4)
            peers.append(((dp, to * 2 + core), (z * 4 + to, ep), (to * 4 + y, ep))[axis])
        rings.append((me, peers))

    barrier = pltpu.get_barrier_semaphore()
    everyone = [partner] + [p for _, peers in rings for p in peers]
    for p in everyone:
        pl.semaphore_signal(barrier, inc=1, device_id=p, device_id_type=MESH)
    pl.semaphore_wait(barrier, len(everyone))

    head = pl.ds(0, whole_rows)
    work[0] = a_ref[...]
    pair = pltpu.make_async_remote_copy(
        src_ref=work.at[0, head], dst_ref=work.at[1, head], send_sem=pair_send, recv_sem=pair_recv,
        device_id=partner, device_id_type=MESH)
    pair.start()
    pair.wait()
    work[2] = a_ref[...]
    work[2, head, :] = work[0, head, :] + work[1, head, :]
    for axis in range(3):
        me, peers = rings[axis]
        rows = head if axis == 0 else pl.ds(0, a_ref.shape[0])
        bufs[axis, me] = work[axis + 2]
        copies = []
        for k in range(3):
            copy = pltpu.make_async_remote_copy(
                src_ref=work.at[axis + 2, rows], dst_ref=bufs.at[axis, me, rows], send_sem=send_sem.at[axis, k],
                recv_sem=recv_sem.at[axis, k], device_id=peers[k], device_id_type=MESH)
            copy.start()
            copies.append(copy)
        for copy in copies:
            copy.wait()
        total = bufs[axis, 0, rows, :] + bufs[axis, 1, rows, :] + bufs[axis, 2, rows, :] + bufs[axis, 3, rows, :]
        if axis == 2:
            o_ref[...] = total
        else:
            work[axis + 3] = work[axis + 2]
            work[axis + 3, rows, :] = total


def small_reduce(a, whole_rows, collective_id):
    rows, cols = a.shape
    return pl.pallas_call(
        functools.partial(reduce_kernel, whole_rows),
        out_shape=jax.ShapeDtypeStruct((rows, cols), F32),
        in_specs=[pl.BlockSpec(memory_space=pltpu.VMEM)],
        out_specs=pl.BlockSpec(memory_space=pltpu.VMEM),
        scratch_shapes=[
            pltpu.VMEM((3, 4, rows, cols), F32),
            pltpu.SemaphoreType.DMA((3, 3)),
            pltpu.SemaphoreType.DMA((3, 3)),
            pltpu.SemaphoreType.DMA,
            pltpu.SemaphoreType.DMA,
            pltpu.VMEM((5, rows, cols), F32),
        ],
        compiler_params=pltpu.CompilerParams(collective_id=collective_id, has_side_effects=True),
        cost_estimate=pl.CostEstimate(flops=2_000_000_000, bytes_accessed=100_000, transcendentals=0),
        name=f"small_reduce_{collective_id}",
    )(a)


def vmem(count):
    return [pl.BlockSpec(memory_space=pltpu.VMEM)] * count


def params():
    return pltpu.CompilerParams(vmem_limit_bytes=60 * 1024 * 1024)


def cost(flops, size):
    return pl.CostEstimate(flops=int(flops), bytes_accessed=int(size), transcendentals=0)


def solution(mesh):
    token_spec = P(ALL_AXES)
    expert_spec = P("ep")

    def local_step(x, modality, router, expert_ids, priority, w_in, b_in, w_out, b_out, dy):
        n, width = x.shape
        experts = router.shape[1]
        hid = w_in.shape[2]
        capacity = n // experts
        w_in, w_out = w_in[0], w_out[0]
        ids = expert_ids.reshape(1, n)
        prio = priority.reshape(1, n)
        mod = modality.reshape(1, n)
        router_t = jnp.transpose(router)
        router3 = jnp.concatenate(split3_outside(router_t), axis=0)
        shape = jax.ShapeDtypeStruct
        gather_flops = 2 * n * n * width

        slot, send_rows = pl.pallas_call(
            functools.partial(route_kernel, capacity),
            out_shape=(shape((8, n), F32), shape((experts, capacity, width), BF16)),
            in_specs=vmem(3), out_specs=tuple(vmem(2)),
            scratch_shapes=[pltpu.VMEM((n, 8), F32)],
            compiler_params=params(), cost_estimate=cost(gather_flops, 4 * n * width), name="route",
        )(ids, prio, x)
        recv_rows = lax.all_to_all(send_rows, "ep", 0, 0, tiled=True).reshape(n, width)

        logp, stats_part, send_d = pl.pallas_call(
            functools.partial(router_kernel, capacity),
            out_shape=(shape((experts, n), F32), shape((48, 128), F32), shape((experts, capacity, width), BF16)),
            in_specs=vmem(6), out_specs=tuple(vmem(3)),
            scratch_shapes=[pltpu.VMEM((n, width), BF16)],
            compiler_params=params(), cost_estimate=cost(gather_flops, 6 * n * width), name="router",
        )(ids, mod, slot, x, dy, router3)
        d_recv = lax.all_to_all(send_d, "ep", 0, 0, tiled=True).reshape(n, width)
        stats = small_reduce(stats_part, 48, 1)

        tile = 512
        steps = hid // tile
        whole = pl.BlockSpec((n, width), lambda i: (0, 0))
        w_in_spec = pl.BlockSpec((width, tile), lambda i: (0, i))
        w_out_spec = pl.BlockSpec((tile, width), lambda i: (i, 0))
        hid_row = pl.BlockSpec((1, tile), lambda i: (0, i))
        width_row = pl.BlockSpec((1, width), lambda i: (0, 0))
        mm = 2 * n * width * hid

        tiles = hid // TILE
        recv_rows, stats = lax.optimization_barrier((recv_rows, stats))
        hidden_t, slope, rows_t, y = pl.pallas_call(
            functools.partial(forward_kernel, steps, 4),
            grid=(steps,),
            out_shape=(shape((hid, n), BF16), shape((tiles, n, TILE), F32), shape((width, n), BF16), shape((n, width), BF16)),
            in_specs=[whole, w_in_spec, hid_row, w_out_spec, width_row],
            out_specs=(
                pl.BlockSpec((tile, n), lambda i: (i, 0)),
                pl.BlockSpec((tile // TILE, n, TILE), lambda i: (i, 0, 0)),
                pl.BlockSpec((width, n), lambda i: (0, 0)),
                whole,
            ),
            scratch_shapes=[pltpu.VMEM((n, width), F32)],
            compiler_params=params(), cost_estimate=cost(2 * mm, 6 * n * hid), name="expert_forward",
        )(recv_rows, w_in, b_in, w_out, b_out)

        anywhere = pl.BlockSpec(memory_space=pl.ANY)
        dma = pltpu.SemaphoreType.DMA
        slots = (experts, capacity, width)
        summed, d_b_in, d_b_out, back_y, d_back = pl.pallas_call(
            grads_kernel,
            out_shape=(
                shape((2 * tiles, 4, 4, 16, width), BF16), shape((1, hid), F32), shape((1, width), F32),
                shape(slots, BF16), shape(slots, BF16),
            ),
            in_specs=[anywhere] * 4 + vmem(2) + [anywhere],
            out_specs=(anywhere, *vmem(2), anywhere, anywhere),
            scratch_shapes=[
                pltpu.VMEM((2 * tiles, 4, 4, 16, width), F32),
                pltpu.VMEM((2 * tiles, 3, 4, 16, width), F32),
                pltpu.VMEM((2 * tiles, 3, 16, width), F32),
                pltpu.VMEM((2 * tiles, 16, width), BF16),
                pltpu.VMEM((2, TILE, n), BF16),
                pltpu.VMEM((2, n, TILE), F32),
                pltpu.VMEM((2, width, TILE), BF16),
                pltpu.VMEM((2, TILE, width), BF16),
                pltpu.VMEM((n, TILE), BF16),
                pltpu.VMEM((n, width), F32),
                pltpu.VMEM(slots, BF16),
                dma((2 * tiles, 12)), dma((2 * tiles, 12)), dma((2 * tiles,)), dma((2,)), dma((2, 3)),
                dma((experts - 1,)), dma((experts - 1,)), dma((experts - 1,)), dma((experts - 1,)), dma((2,)),
            ],
            compiler_params=pltpu.CompilerParams(collective_id=3, has_side_effects=True, vmem_limit_bytes=67_000_000),
            cost_estimate=cost(4 * mm, 6 * n * hid), name="expert_grads",
        )(hidden_t, slope, w_in, w_out, rows_t, d_recv, y.reshape(slots))
        back_y, d_back = back_y.reshape(n, width), d_back.reshape(n, width)
        d_w_out = summed[:tiles].reshape(hid, width)
        d_w_in = pl.pallas_call(
            unpack_kernel,
            grid=(tiles,),
            out_shape=shape((width, hid), BF16),
            in_specs=[pl.BlockSpec((1, 4, 4, 16, width), lambda i: (i + tiles, 0, 0, 0, 0))],
            out_specs=pl.BlockSpec((width, TILE), lambda i: (0, i)),
            name="unpack",
        )(summed)

        out, d_log, d_router_part, loss = pl.pallas_call(
            functools.partial(combine_kernel, capacity, 4),
            out_shape=(shape((n, width), BF16), shape((experts, n), F32), shape((experts, width), F32), shape((8, 128), F32)),
            in_specs=vmem(8), out_specs=tuple(vmem(4)),
            compiler_params=params(), cost_estimate=cost(gather_flops, 8 * n * width), name="combine",
        )(ids, mod, slot, logp, back_y, dy, x, stats)

        d_x = pl.pallas_call(
            functools.partial(token_grad_kernel, 4),
            out_shape=shape((n, width), BF16),
            in_specs=vmem(4), out_specs=vmem(1)[0],
            compiler_params=params(), cost_estimate=cost(gather_flops, 6 * n * width), name="token_grad",
        )(slot, d_log, d_back, router_t)

        small = jnp.concatenate([d_router_part, d_b_in.reshape(hid // width, width), d_b_out, jnp.zeros((3, width), F32)], axis=0)
        small = small_reduce(small, experts, 2)
        d_router = jnp.transpose(small[0:experts])
        d_b_in = small[experts:experts + hid // width].reshape(1, hid).astype(BF16)
        d_b_out = small[experts + hid // width:experts + hid // width + 1].astype(BF16)
        return out, loss[0, 0], d_x, d_router, d_w_in[None], d_b_in, d_w_out[None], d_b_out

    def split3_outside(a):
        hi = lax.reduce_precision(a, 8, 7)
        mid = lax.reduce_precision(a - hi, 8, 7)
        return hi.astype(BF16), mid.astype(BF16), (a - hi - mid).astype(BF16)

    return jax.shard_map(
        local_step,
        mesh=mesh,
        in_specs=(token_spec, token_spec, P(), token_spec, token_spec, expert_spec, expert_spec, expert_spec, expert_spec, token_spec),
        out_specs=(token_spec, P(), token_spec, P(), expert_spec, expert_spec, expert_spec, expert_spec),
        check_vma=False,
    )
```

```python
import functools

import jax
import jax.numpy as jnp
from jax import lax
from jax.experimental import pallas as pl
from jax.experimental.pallas import tpu as pltpu
from jax.sharding import PartitionSpec as P

ALL_AXES = ("dp", "ep")
MESH = pl.DeviceIdType.MESH
F32 = jnp.float32
BF16 = jnp.bfloat16
NOWHERE = -1.0
TILE = 256
CHUNK = 256


def col_of(row):
    return jnp.transpose(jnp.broadcast_to(row, (8, row.shape[1])))


def row_of(col):
    return jnp.transpose(jnp.broadcast_to(col, (col.shape[0], 8)))


def split3(a):
    hi = a.astype(BF16)
    rest = a - hi.astype(F32)
    mid = rest.astype(BF16)
    lo = (rest - mid.astype(F32)).astype(BF16)
    return hi, mid, lo


def nt(a, b):
    return lax.dot_general(a, b, (((1,), (1,)), ((), ())), preferred_element_type=F32)


def tn(a, b):
    return lax.dot_general(a, b, (((0,), (0,)), ((), ())), preferred_element_type=F32)


def nn(a, b):
    return jnp.dot(a, b, preferred_element_type=F32)


def wide(ref):
    v = ref[...].astype(F32)
    return jnp.concatenate([v[i:i + 1, :] for i in range(v.shape[0])], axis=1)


def greet(peers):
    barrier = pltpu.get_barrier_semaphore()
    for peer in peers:
        pl.semaphore_signal(barrier, inc=1, device_id=peer, device_id_type=MESH)
    return lambda: pl.semaphore_wait(barrier, len(peers))


def dispatch_kernel(
    ids_ref, prio_ref, mod_ref, x_ref, dy_ref, router3_ref, w_in, b_in_ref, w_out, b_out_ref,
    ids_row_ref, mod_row_ref, slot_ref, logp_ref, stats_ref, hidden_t, slope, rows_t_ref, y_ref, d_rows,
    keycol, dyt, out_x, out_d, rows, acc, ibuf, obuf, hbuf, sbuf,
    x_send, x_recv, d_send, d_recv, self_sem, load_sem, store_sem,
):
    dp = lax.axis_index("dp")
    ep = lax.axis_index("ep")
    x, core = ep // 2, lax.rem(ep, 2)
    experts, capacity, width = out_x.shape
    n = experts * capacity
    hid = hidden_t.shape[0]
    tiles = hid // TILE
    chunks = 4
    size = n // chunks

    enter = greet([(dp, lax.rem(ep + j, experts)) for j in range(1, experts)])

    def loads(i):
        slot = lax.rem(i, 2)
        at = pl.ds(pl.multiple_of(i * TILE, TILE), TILE)
        return (
            pltpu.make_async_copy(w_in.at[:, at], ibuf.at[slot], load_sem.at[slot, 0]),
            pltpu.make_async_copy(w_out.at[at], obuf.at[slot], load_sem.at[slot, 1]),
        )

    def stores(i):
        slot = lax.rem(i, 2)
        at = pl.ds(pl.multiple_of(i * TILE, TILE), TILE)
        return (
            pltpu.make_async_copy(hbuf.at[slot], hidden_t.at[at], store_sem.at[slot, 0]),
            pltpu.make_async_copy(sbuf.at[slot], slope.at[i], store_sem.at[slot, 1]),
        )

    for copy in loads(0):
        copy.start()

    ids = wide(ids_ref)
    key = ids * n + wide(prio_ref)
    low = ids * n
    keycol[...] = col_of(key)

    def count(j, total):
        col = keycol[pl.ds(pl.multiple_of(j * 128, 128), 128), :][:, 0:1]
        before = jnp.logical_and(col < key, col >= low)
        return total + jnp.sum(before.astype(F32), axis=0, keepdims=True)

    position = lax.fori_loop(0, n // 128, count, jnp.zeros((1, n), F32))
    slot_row = jnp.where(position < capacity, ids * capacity + position, NOWHERE)
    slot_ref[...] = jnp.broadcast_to(slot_row, slot_ref.shape)
    mod_row = wide(mod_ref)
    ids_row_ref[...] = jnp.broadcast_to(ids, ids_row_ref.shape)
    mod_row_ref[...] = jnp.broadcast_to(mod_row, mod_row_ref.shape)

    def target(j):
        return lax.rem(x + j // 2 + 1, 4) * 2 + lax.rem(core + 1 - lax.rem(j, 2), 2)

    def pick(e):
        index = (lax.broadcasted_iota(jnp.int32, (capacity, n), 0) + e * capacity).astype(F32)
        return (index == slot_ref[0:1, :]).astype(BF16)

    def send(j, src, dst, send_sems, recv_sems):
        to = target(j)
        return pltpu.make_async_remote_copy(
            src_ref=src.at[to], dst_ref=dst.at[ep], send_sem=send_sems.at[j], recv_sem=recv_sems.at[j],
            device_id=(dp, to), device_id_type=MESH)

    enter()

    def send_x(j, carry):
        out_x[target(j)] = nn(pick(target(j)), x_ref[...]).astype(BF16)
        send(j, out_x, rows, x_send, x_recv).start()
        return carry

    lax.fori_loop(0, experts - 1, send_x, 0)
    rows[ep] = nn(pick(ep), x_ref[...]).astype(BF16)

    logits3 = nt(router3_ref[...], x_ref[...])
    logits = logits3[0:experts] + logits3[experts:2 * experts] + logits3[2 * experts:3 * experts]
    shifted = logits - jnp.max(logits, axis=0, keepdims=True)
    logp = shifted - jnp.log(jnp.sum(jnp.exp(shifted), axis=0, keepdims=True))
    logp_ref[...] = logp
    probs = jnp.exp(logp)
    onehot = (lax.broadcasted_iota(jnp.int32, (experts, n), 0).astype(F32) == ids).astype(F32)
    gate = jnp.sum(probs * onehot, axis=0, keepdims=True)
    dyt[...] = (col_of(gate)[:, 0:1] * dy_ref[...].astype(F32)).astype(BF16)

    def send_cotangent(j, carry):
        out_d[target(j)] = nn(pick(target(j)), dyt[...]).astype(BF16)
        send(j, out_d, d_rows, d_send, d_recv).start()
        return carry

    lax.fori_loop(0, experts - 1, send_cotangent, 0)
    out_d[ep] = nn(pick(ep), dyt[...]).astype(BF16)
    keep_d = pltpu.make_async_copy(out_d.at[ep], d_rows.at[ep], self_sem)
    keep_d.start()

    entropy = -jnp.sum(probs * logp, axis=0, keepdims=True)
    for m in range(2):
        mask = (mod_row == m).astype(F32)
        stats_ref[24 * m:24 * m + 8, :] = jnp.broadcast_to(jnp.sum(probs * mask, axis=1, keepdims=True), (8, 128))
        stats_ref[24 * m + 8:24 * m + 16, :] = jnp.broadcast_to(jnp.sum(entropy * mask, axis=1, keepdims=True), (8, 128))
        stats_ref[24 * m + 16:24 * m + 24, :] = jnp.broadcast_to(jnp.sum(mask, axis=1, keepdims=True), (8, 128))
    acc[...] = jnp.broadcast_to(b_out_ref[...].astype(F32), acc.shape)

    def arrive(j, carry):
        send(j, out_x, rows, x_send, x_recv).wait_recv()
        return carry

    lax.fori_loop(0, experts - 1, arrive, 0)

    def tile(i, carry):
        slot = lax.rem(i, 2)
        for copy in loads(i):
            copy.wait()

        @pl.when(i + 1 < tiles)
        def _():
            for copy in loads(i + 1):
                copy.start()

        @pl.when(i >= 2)
        def _():
            for copy in stores(i - 2):
                copy.wait()

        bias = b_in_ref[:, pl.ds(pl.multiple_of(i * TILE, TILE), TILE)].astype(F32)
        for c in range(chunks):
            part = pl.ds(c * size, size)
            part_rows = rows[c * (experts // chunks):(c + 1) * (experts // chunks)].reshape(size, width)
            a = nn(part_rows, ibuf[slot]) + bias
            root = 0.7978845608028654
            sq = a * a
            t = jnp.tanh(root * (a + 0.044715 * (sq * a)))
            half = 0.5 * (1.0 + t)
            hidden = (a * half).astype(BF16)
            sbuf[slot, part, :] = half + (0.5 * root) * a * (1.0 - t * t) * (1.0 + (3 * 0.044715) * sq)
            hbuf[slot, :, part] = jnp.transpose(hidden)
            acc[part, :] += nn(hidden, obuf[slot])
        for copy in stores(i):
            copy.start()
        return carry

    lax.fori_loop(0, tiles, tile, 0)
    rows_t_ref[...] = jnp.transpose(rows[...].reshape(n, width))
    y_ref[...] = acc[...].astype(BF16).reshape(y_ref.shape)
    for i in (tiles - 2, tiles - 1):
        for copy in stores(jnp.int32(i)):
            copy.wait()
    keep_d.wait()

    def finish(j, carry):
        send(j, out_x, rows, x_send, x_recv).wait_send()
        send(j, out_d, d_rows, d_send, d_recv).wait()
        return carry

    lax.fori_loop(0, experts - 1, finish, 0)


def grads_kernel(
    hidden_t, slope, w_in, w_out, rows_t_in, d_in, y, x, dy, ids_row, mod_row, slot_row, logp_ref, stats_in,
    summed, back_y, back_d, out, d_log_ref, loss_ref, small_ref,
    part_sum, land_a, land_b, own, hbuf, sbuf, ibuf, obuf, act, acc, d_out, rows_t, tok, db_in, stage, stats_ref, d_router,
    stat_work, stat_bufs, small_work, small_bufs,
    send_sem, recv_sem, own_sem, load_sem, load2_sem, y_send, y_recv, d_send, d_recv, self_sem, tok_sem, out_sem,
    stat_send, stat_recv, small_send, small_recv,
):
    dp = lax.axis_index("dp")
    ep = lax.axis_index("ep")
    z, yy = dp // 4, lax.rem(dp, 4)
    tiles = part_sum.shape[0]
    units = tiles // 4
    half = tiles // 2
    experts = y.shape[0]
    n, width = acc.shape
    chunks = 4
    size = n // chunks

    def place(stream):
        way = 1 - 2 * lax.rem(stream, 2)
        first_z = stream // 2
        pa = yy * (1 - first_z) + z * first_z
        pb = z * (1 - first_z) + yy * first_z
        y_next, z_next = lax.rem(yy + way + 4, 4), lax.rem(z + way + 4, 4)
        along_y, along_z = z * 4 + y_next, z_next * 4 + yy
        next_a = along_y * (1 - first_z) + along_z * first_z
        next_b = along_z * (1 - first_z) + along_y * first_z
        return way, pa, pb, next_a, next_b

    def wrap(v):
        return lax.rem(v + 16, 4)

    def send(tile, k):
        way, pa, pb, next_a, next_b = place(lax.rem(tile, 4))
        if k < 3:
            src, dst, to = part_sum.at[tile, wrap(pa - way * (k + 1))], land_a.at[tile, k], next_a
        elif k < 6:
            src, dst, to = part_sum.at[tile, pa, wrap(pb - way * (k - 2))], land_b.at[tile, k - 3], next_b
        elif k == 6:
            src, dst, to = own.at[tile], summed.at[tile, pa, pb], next_b
        elif k < 9:
            src = summed.at[tile, pa, wrap(pb - way * (k - 6))]
            dst, to = src, next_b
        else:
            src = summed.at[tile, wrap(pa - way * (k - 9))]
            dst, to = src, next_a
        return pltpu.make_async_remote_copy(
            src_ref=src, dst_ref=dst, send_sem=send_sem.at[tile, k], recv_sem=recv_sem.at[tile, k],
            device_id=(to, ep), device_id_type=MESH)

    def keep(tile):
        way, pa, pb, _, _ = place(lax.rem(tile, 4))
        return pltpu.make_async_copy(own.at[tile], summed.at[tile, pa, pb], own_sem.at[tile])

    def advance(tile, k):
        way, pa, pb, _, _ = place(lax.rem(tile, 4))
        send(tile, k - 1).wait_recv()
        if k <= 3:
            block = wrap(pa - way * (k + 1))
            part_sum[tile, block] = part_sum[tile, block] + land_a[tile, k - 1]
        elif k <= 6:
            block = wrap(pb - way * (k - 2))
            total = part_sum[tile, pa, block] + land_b[tile, k - 4]
            if k < 6:
                part_sum[tile, pa, block] = total
            else:
                own[tile] = total.astype(BF16)
                keep(tile).start()
        elif k == 9:
            keep(tile).wait()
        if k < 12:
            send(tile, k).start()

    def wave(t, stream):
        for k in range(12, 0, -1):
            unit = t - k

            @pl.when(jnp.logical_and(unit >= 0, unit < units))
            def _():
                advance(unit * 4 + stream, k)

    def exchange(src, dst, send_sems, recv_sems):
        copies = []
        for j in range(1, experts):
            to = lax.rem(ep + j, experts)
            copies.append(pltpu.make_async_remote_copy(
                src_ref=src.at[to], dst_ref=dst.at[ep], send_sem=send_sems.at[j - 1], recv_sem=recv_sems.at[j - 1],
                device_id=(dp, to), device_id_type=MESH))
        return copies

    def load_hidden(i):
        slot = lax.rem(i, 2)
        return pltpu.make_async_copy(hidden_t.at[pl.ds(pl.multiple_of(i * TILE, TILE), TILE)], hbuf.at[slot], load_sem.at[slot])

    def load_rest(i):
        slot = lax.rem(i, 2)
        at = pl.ds(pl.multiple_of(i * TILE, TILE), TILE)
        return (
            pltpu.make_async_copy(slope.at[i], sbuf.at[slot], load2_sem.at[slot, 0]),
            pltpu.make_async_copy(w_in.at[:, at], ibuf.at[slot], load2_sem.at[slot, 1]),
            pltpu.make_async_copy(w_out.at[at], obuf.at[slot], load2_sem.at[slot, 2]),
        )

    load_hidden(0).start()
    for copy in load_rest(0):
        copy.start()

    load_rows = pltpu.make_async_copy(rows_t_in, rows_t, tok_sem.at[0])
    load_d = pltpu.make_async_copy(d_in, tok, tok_sem.at[1])
    load_rows.start()
    load_d.start()
    peers = [(z * 4 + wrap(yy + j), ep) for j in range(1, 4)] + [(wrap(z + j) * 4 + yy, ep) for j in range(1, 4)]
    peers += [(dp, lax.rem(ep + j, experts)) for j in range(1, experts)]
    greet(peers)()

    rings = (
        (ep // 2, [(dp, lax.rem(ep + 2 * j, experts)) for j in range(1, 4)]),
        (yy, peers[0:3]),
        (z, peers[3:6]),
    )
    partner = (dp, (ep // 2) * 2 + 1 - lax.rem(ep, 2))

    def small_sum(work, bufs, whole_rows, send_sems, recv_sems):
        rows = work.shape[1]
        head = pl.ds(0, whole_rows)

        def pair():
            return pltpu.make_async_remote_copy(
                src_ref=work.at[0, head], dst_ref=bufs.at[3, 0, head], send_sem=send_sems.at[3, 0], recv_sem=recv_sems.at[3, 0],
                device_id=partner, device_id_type=MESH)

        def ring(axis):
            me, others = rings[axis]
            at = head if axis == 0 else pl.ds(0, rows)
            return [
                pltpu.make_async_remote_copy(
                    src_ref=work.at[axis + 1, at], dst_ref=bufs.at[axis, me, at], send_sem=send_sems.at[axis, j],
                    recv_sem=recv_sems.at[axis, j], device_id=others[j], device_id_type=MESH)
                for j in range(3)
            ]

        def launch(axis):
            bufs[axis, rings[axis][0]] = work[axis + 1]
            for copy in ring(axis):
                copy.start()

        def total(axis, at):
            for copy in ring(axis):
                copy.wait()
            return bufs[axis, 0, at, :] + bufs[axis, 1, at, :] + bufs[axis, 2, at, :] + bufs[axis, 3, at, :]

        def step(k):
            if k == 0:
                pair().start()
            elif k == 1:
                pair().wait()
                work[1] = work[0]
                work[1, head, :] = work[0, head, :] + bufs[3, 0, head, :]
                launch(0)
            elif k < 4:
                at = head if k == 2 else pl.ds(0, rows)
                summed_rows = total(k - 2, at)
                work[k] = work[k - 1]
                work[k, at, :] = summed_rows
                launch(k - 1)
            else:
                return total(2, pl.ds(0, rows))

        return step

    stat_step = small_sum(stat_work, stat_bufs, 48, stat_send, stat_recv)
    small_step = small_sum(small_work, small_bufs, experts, small_send, small_recv)
    stat_work[0] = stats_in[...]
    stat_step(0)

    send_y = exchange(y, back_y, y_send, y_recv)
    for copy in send_y:
        copy.start()
    self_y = pltpu.make_async_copy(y.at[ep], back_y.at[ep], self_sem.at[0])
    self_y.start()
    acc[...] = jnp.zeros_like(acc)
    small_work[0] = jnp.zeros(small_work.shape[1:], F32)
    load_d.wait()

    def out_tile(i, carry):
        wave(i // 4, lax.rem(i, 4))
        slot = lax.rem(i, 2)
        load_hidden(i).wait()

        @pl.when(i + 1 < half)
        def _():
            load_hidden(i + 1).start()

        grad = nn(hbuf[slot], tok[...])
        part_sum[i] = grad.reshape(part_sum.shape[1:])
        send(i, 0).start()
        for k in (1, 2):
            @pl.when(i == 4 * k)
            def _():
                stat_step(k)

        return carry

    lax.fori_loop(0, half, out_tile, 0)

    def in_tile(i, carry):
        g = i + half
        wave(g // 4, lax.rem(g, 4))
        slot = lax.rem(i, 2)
        for copy in load_rest(i):
            copy.wait()

        @pl.when(i + 1 < half)
        def _():
            for copy in load_rest(i + 1):
                copy.start()

        total = jnp.zeros((1, TILE), F32)
        for c in range(chunks):
            part = pl.ds(c * size, size)
            d_hidden = nt(tok[part, :], obuf[slot]).astype(BF16)
            d_act = d_hidden.astype(F32) * sbuf[slot, part, :]
            total += jnp.sum(d_act, axis=0, keepdims=True)
            d_act_bf = d_act.astype(BF16)
            act[part, :] = d_act_bf
            acc[part, :] += nt(d_act_bf, ibuf[slot])
        db_in[:, pl.ds(pl.multiple_of(i * TILE, TILE), TILE)] = total
        rows = width // 4
        for a in range(4):
            grad = nn(rows_t[pl.ds(a * rows, rows), :], act[...])
            for b in range(4):
                for j in range(3):
                    at = b * (rows // 4) + j * 16
                    part_sum[g, a, b, :, j * TILE:(j + 1) * TILE] = grad[at:at + 16, :]
        send(g, 0).start()

        @pl.when(i == 0)
        def _():
            stat_step(3)

        @pl.when(i == 4)
        def _():
            stats_ref[...] = stat_step(4)

        return carry

    small_work[0, 12:13, :] = jnp.sum(tok[...].astype(F32), axis=0, keepdims=True)
    load_rows.wait()
    lax.fori_loop(0, half, in_tile, 0)

    d_out[...] = acc[...].astype(BF16).reshape(d_out.shape)
    send_d = exchange(d_out, back_d, d_send, d_recv)
    for copy in send_d:
        copy.start()
    self_d = pltpu.make_async_copy(d_out.at[ep], back_d.at[ep], self_sem.at[1])
    self_d.start()

    for copy in send_y:
        copy.wait_recv()
    self_y.wait()
    back = pltpu.make_async_copy(back_y, tok.reshape(back_y.shape), tok_sem.at[1])
    back.start()
    for i in range(4):
        small_work[0, 8 + i:9 + i, :] = db_in[:, i * width:(i + 1) * width]
    d_router[...] = jnp.zeros_like(d_router)
    loss, terms, inv = global_terms(stats_ref[...], experts)
    loss_ref[...] = jnp.broadcast_to(loss, loss_ref.shape)

    def token_loads(i):
        at = pl.ds(pl.multiple_of(i * CHUNK, CHUNK), CHUNK)
        return (
            pltpu.make_async_copy(dy.at[at], obuf.at[0], load2_sem.at[0, 2]),
            pltpu.make_async_copy(x.at[at], obuf.at[1], load2_sem.at[1, 2]),
        )

    def out_store(i):
        at = pl.ds(pl.multiple_of(i * CHUNK, CHUNK), CHUNK)
        return pltpu.make_async_copy(stage, out.at[at], out_sem)

    for copy in token_loads(jnp.int32(0)):
        copy.start()
    back.wait()
    pieces = n // CHUNK

    def combine(i):
        lanes = pl.ds(pl.multiple_of(i * CHUNK, CHUNK), CHUNK)
        slot_col = col_of(slot_row[0:1, lanes])[:, 0:1]
        pick = (lax.broadcasted_iota(jnp.int32, (CHUNK, n), 1).astype(F32) == slot_col).astype(BF16)
        y_tok = nn(pick, tok[...])
        logp = logp_ref[:, lanes]
        probs = jnp.exp(logp)
        onehot = (lax.broadcasted_iota(jnp.int32, (experts, CHUNK), 0).astype(F32) == ids_row[:, lanes]).astype(F32)
        gate = jnp.sum(probs * onehot, axis=0, keepdims=True)
        for copy in token_loads(i):
            copy.wait()

        @pl.when(i > 0)
        def _():
            out_store(i - 1).wait()

        stage[...] = (col_of(gate)[:, 0:1] * y_tok).astype(BF16)
        out_store(i).start()
        d_gate = row_of(jnp.sum(obuf[0].astype(F32) * y_tok, axis=1, keepdims=True))[0:1]
        is_text = mod_row[:, lanes] == 1.0
        global_part = jnp.where(is_text, terms[1][:, 0:1], terms[0][:, 0:1])
        inv_count = jnp.where(is_text, inv[1][:, 0:1], inv[0][:, 0:1])
        d_probs = onehot * d_gate + global_part - logp * inv_count
        d_log = probs * (d_probs - jnp.sum(d_probs * probs, axis=0, keepdims=True))
        d_log_ref[:, lanes] = d_log
        d_router[...] += nn(jnp.concatenate(split3(d_log), axis=0), obuf[1])

        @pl.when(i + 1 < pieces)
        def _():
            for copy in token_loads(i + 1):
                copy.start()

    def rest(t, carry):
        def streams(s, inner):
            wave(t, s)
            i = (t - units) * 2 + s // 2

            @pl.when(jnp.logical_and(lax.rem(s, 2) == 1, i < pieces))
            def _():
                combine(i)

            return inner

        return lax.fori_loop(0, 4, streams, carry)

    first = units + pieces // 2
    lax.fori_loop(units, first, rest, 0)
    out_store(jnp.int32(pieces - 1)).wait()
    small_work[0, 0:experts, :] = d_router[0:experts] + d_router[experts:2 * experts] + d_router[2 * experts:]

    def late(t, carry):
        def streams(s, inner):
            wave(t, s)
            return inner

        return lax.fori_loop(0, 4, streams, carry)

    small_step(0)
    for k in range(1, 5):
        lax.fori_loop(first + k - 1, first + k, late, 0)
        result = small_step(k)
    small_ref[...] = result
    lax.fori_loop(first + 4, units + 12, late, 0)

    def drain(tile, carry):
        for k in range(12):
            send(tile, k).wait_send()
        return carry

    lax.fori_loop(0, tiles, drain, 0)
    for copy in send_y:
        copy.wait_send()
    for copy in send_d:
        copy.wait()
    self_d.wait()


def global_terms(stats, experts):
    loss = jnp.zeros((1, 128), F32)
    terms = []
    inv = []
    for m in range(2):
        base = 24 * m
        count = stats[base + 16:base + 17]
        mean = stats[base:base + 8] / count
        log_mean = jnp.log(mean)
        loss = loss + stats[base + 8:base + 9] / count + jnp.sum(mean * log_mean, axis=0, keepdims=True)
        terms.append(log_mean / count)
        inv.append(1.0 / count)
    return loss, terms, inv


def final_kernel(slot_ref, d_log_ref, back_ref, router_ref, small_ref, loss_ref, sum_out_ref, sum_in_ref,
                 dx_ref, dw_in_ref, dw_out_ref, d_router_ref, db_in_ref, db_out_ref, aux_ref):
    step = pl.program_id(0)
    n = back_ref.shape[0]
    size, width = dx_ref.shape
    experts = d_log_ref.shape[0]

    @pl.when(step == 0)
    def _():
        d_router_ref[...] = small_ref[0:experts, :]
        for i in range(4):
            db_in_ref[:, i * width:(i + 1) * width] = small_ref[8 + i:9 + i, :].astype(BF16)
        db_out_ref[...] = small_ref[12:13, :].astype(BF16)
        aux_ref[0, 0] = loss_ref[0, 0]

    r = split3(router_ref[...])
    rights = jnp.concatenate([r[0], r[1], r[0], r[1], r[2], r[0]], axis=0)
    d = split3(d_log_ref[...])
    lefts = jnp.concatenate([d[0], d[0], d[1], d[1], d[0], d[2]], axis=0)
    routed = tn(lefts, rights).astype(BF16)
    slot_col = col_of(slot_ref[0:1, :])[:, 0:1]
    pick = (lax.broadcasted_iota(jnp.int32, (size, n), 1).astype(F32) == slot_col).astype(BF16)
    dx_ref[...] = (nn(pick, back_ref[...]) + routed.astype(F32)).astype(BF16)

    dw_out_ref[...] = sum_out_ref[...].reshape(dw_out_ref.shape)
    rows = width // 4
    for a in range(4):
        for b in range(4):
            for j in range(3):
                at = a * rows + b * (rows // 4) + j * 16
                dw_in_ref[at:at + 16, :] = sum_in_ref[0, a, b, :, j * TILE:(j + 1) * TILE]


def vmem(count):
    return [pl.BlockSpec(memory_space=pltpu.VMEM)] * count


def cost(flops, size):
    return pl.CostEstimate(flops=int(flops), bytes_accessed=int(size), transcendentals=0)


def solution(mesh):
    token_spec = P(ALL_AXES)
    expert_spec = P("ep")

    def local_step(x, modality, router, expert_ids, priority, w_in, b_in, w_out, b_out, dy):
        n, width = x.shape
        experts = router.shape[1]
        hid = w_in.shape[2]
        capacity = n // experts
        tiles = hid // TILE
        w_in, w_out = w_in[0], w_out[0]
        ids, prio, mod = (a.reshape(n // 128, 128) for a in (expert_ids, priority, modality))
        router_t = jnp.transpose(router)
        router3 = jnp.concatenate(split3_outside(router_t), axis=0)
        shape = jax.ShapeDtypeStruct
        anywhere = pl.BlockSpec(memory_space=pl.ANY)
        dma = pltpu.SemaphoreType.DMA
        slots = (experts, capacity, width)
        mm = 2 * n * width * hid

        ids_row, mod_row, slot, logp, stats, hidden_t, slope, rows_t, y, d_rows = pl.pallas_call(
            dispatch_kernel,
            out_shape=(
                shape((8, n), F32), shape((8, n), F32), shape((8, n), F32), shape((experts, n), F32), shape((48, 128), F32),
                shape((hid, n), BF16), shape((tiles, n, TILE), F32), shape((width, n), BF16), shape(slots, BF16), shape(slots, BF16),
            ),
            in_specs=vmem(6) + [anywhere] + vmem(1) + [anywhere] + vmem(1),
            out_specs=(*vmem(5), anywhere, anywhere, *vmem(2), anywhere),
            scratch_shapes=[
                pltpu.VMEM((n, 8), F32), pltpu.VMEM((n, width), BF16), pltpu.VMEM(slots, BF16), pltpu.VMEM(slots, BF16),
                pltpu.VMEM(slots, BF16), pltpu.VMEM((n, width), F32),
                pltpu.VMEM((2, width, TILE), BF16), pltpu.VMEM((2, TILE, width), BF16),
                pltpu.VMEM((2, TILE, n), BF16), pltpu.VMEM((2, n, TILE), F32),
                dma((experts - 1,)), dma((experts - 1,)), dma((experts - 1,)), dma((experts - 1,)), dma, dma((2, 2)), dma((2, 2)),
            ],
            compiler_params=pltpu.CompilerParams(collective_id=1, has_side_effects=True, vmem_limit_bytes=62_000_000),
            cost_estimate=cost(3 * mm, 6 * n * hid), name="dispatch",
        )(ids, prio, mod, x, dy, router3, w_in, b_in, w_out, b_out)

        summed, back_y, d_back, out, d_log, loss, small = pl.pallas_call(
            grads_kernel,
            out_shape=(
                shape((2 * tiles, 4, 4, 16, width), BF16), shape(slots, BF16), shape(slots, BF16), shape((n, width), BF16),
                shape((experts, n), F32), shape((8, 128), F32), shape((16, width), F32),
            ),
            in_specs=[anywhere] * 9 + vmem(5),
            out_specs=(*[anywhere] * 4, *vmem(3)),
            scratch_shapes=[
                pltpu.VMEM((2 * tiles, 4, 4, 16, width), F32),
                pltpu.VMEM((2 * tiles, 3, 4, 16, width), F32),
                pltpu.VMEM((2 * tiles, 3, 16, width), F32),
                pltpu.VMEM((2 * tiles, 16, width), BF16),
                pltpu.VMEM((2, TILE, n), BF16),
                pltpu.VMEM((2, n, TILE), F32),
                pltpu.VMEM((2, width, TILE), BF16),
                pltpu.VMEM((2, TILE, width), BF16),
                pltpu.VMEM((n, TILE), BF16),
                pltpu.VMEM((n, width), F32),
                pltpu.VMEM(slots, BF16),
                pltpu.VMEM((width, n), BF16),
                pltpu.VMEM((n, width), BF16),
                pltpu.VMEM((1, hid), F32),
                pltpu.VMEM((CHUNK, width), BF16),
                pltpu.VMEM((48, 128), F32),
                pltpu.VMEM((3 * experts, width), F32),
                pltpu.VMEM((4, 48, 128), F32), pltpu.VMEM((4, 4, 48, 128), F32),
                pltpu.VMEM((4, 16, width), F32), pltpu.VMEM((4, 4, 16, width), F32),
                dma((2 * tiles, 12)), dma((2 * tiles, 12)), dma((2 * tiles,)), dma((2,)), dma((2, 3)),
                dma((experts - 1,)), dma((experts - 1,)), dma((experts - 1,)), dma((experts - 1,)), dma((2,)), dma((2,)), dma,
                dma((4, 3)), dma((4, 3)), dma((4, 3)), dma((4, 3)),
            ],
            compiler_params=pltpu.CompilerParams(collective_id=3, has_side_effects=True, vmem_limit_bytes=67_000_000),
            cost_estimate=cost(4 * mm, 6 * n * hid), name="expert_grads",
        )(hidden_t, slope, w_in, w_out, rows_t, d_rows.reshape(n, width), y, x, dy, ids_row, mod_row, slot, logp, stats)

        size = n // tiles
        d_x, d_w_in, d_w_out, d_router, d_b_in, d_b_out, aux = pl.pallas_call(
            final_kernel,
            grid=(tiles,),
            out_shape=(
                shape((n, width), BF16), shape((width, hid), BF16), shape((hid, width), BF16), shape((experts, width), F32),
                shape((1, hid), BF16), shape((1, width), BF16), shape((1, 1), F32),
            ),
            in_specs=[
                pl.BlockSpec((8, size), lambda i: (0, i)),
                pl.BlockSpec((experts, size), lambda i: (0, i)),
                pl.BlockSpec((n, width), lambda i: (0, 0)),
                pl.BlockSpec((experts, width), lambda i: (0, 0)),
                pl.BlockSpec((16, width), lambda i: (0, 0)),
                pl.BlockSpec((8, 128), lambda i: (0, 0)),
                pl.BlockSpec((1, 4, 4, 16, width), lambda i: (i, 0, 0, 0, 0)),
                pl.BlockSpec((1, 4, 4, 16, width), lambda i: (i + tiles, 0, 0, 0, 0)),
            ],
            out_specs=(
                pl.BlockSpec((size, width), lambda i: (i, 0)),
                pl.BlockSpec((width, TILE), lambda i: (0, i)),
                pl.BlockSpec((TILE, width), lambda i: (i, 0)),
                pl.BlockSpec((experts, width), lambda i: (0, 0)),
                pl.BlockSpec((1, hid), lambda i: (0, 0)),
                pl.BlockSpec((1, width), lambda i: (0, 0)),
                pl.BlockSpec(memory_space=pltpu.SMEM),
            ),
            name="final",
        )(slot, d_log, d_back.reshape(n, width), router_t, small, loss, summed, summed)
        return out, aux[0, 0], d_x, jnp.transpose(d_router), d_w_in[None], d_b_in, d_w_out[None], d_b_out

    def split3_outside(a):
        hi = lax.reduce_precision(a, 8, 7)
        mid = lax.reduce_precision(a - hi, 8, 7)
        return hi.astype(BF16), mid.astype(BF16), (a - hi - mid).astype(BF16)

    return jax.shard_map(
        local_step,
        mesh=mesh,
        in_specs=(token_spec, token_spec, P(), token_spec, token_spec, expert_spec, expert_spec, expert_spec, expert_spec, token_spec),
        out_specs=(token_spec, P(), token_spec, P(), expert_spec, expert_spec, expert_spec, expert_spec),
        check_vma=False,
    )
```

```python
import functools

import jax
import jax.numpy as jnp
from jax import lax
from jax.experimental import pallas as pl
from jax.experimental.pallas import tpu as pltpu
from jax.sharding import PartitionSpec as P

ALL_AXES = ("dp", "ep")
MESH = pl.DeviceIdType.MESH
F32 = jnp.float32
BF16 = jnp.bfloat16
NOWHERE = -1.0
TILE = 256
CHUNK = 256


def col_of(row):
    return jnp.transpose(jnp.broadcast_to(row, (8, row.shape[1])))


def row_of(col):
    return jnp.transpose(jnp.broadcast_to(col, (col.shape[0], 8)))


def split3(a):
    hi = a.astype(BF16)
    rest = a - hi.astype(F32)
    mid = rest.astype(BF16)
    lo = (rest - mid.astype(F32)).astype(BF16)
    return hi, mid, lo


def nt(a, b):
    return lax.dot_general(a, b, (((1,), (1,)), ((), ())), preferred_element_type=F32)


def tn(a, b):
    return lax.dot_general(a, b, (((0,), (0,)), ((), ())), preferred_element_type=F32)


def nn(a, b):
    return jnp.dot(a, b, preferred_element_type=F32)


def wide(ref):
    v = ref[...].astype(F32)
    return jnp.concatenate([v[i:i + 1, :] for i in range(v.shape[0])], axis=1)


def greet(peers):
    barrier = pltpu.get_barrier_semaphore()
    for peer in peers:
        pl.semaphore_signal(barrier, inc=1, device_id=peer, device_id_type=MESH)
    return lambda: pl.semaphore_wait(barrier, len(peers))


ROOT = 0.7978845608028654
CUBIC = 0.044715


def block_kernel(
    ids_ref, prio_ref, mod_ref, x_any, dy_any, router_ref, w_in, b_in_ref, w_out, b_out_ref,
    summed, back_y, back_d, out, hidden_t, pre_act, slot_row, d_log_ref, loss_ref, small_ref,
    part_sum, land_a, land_b, own, x_buf, dy_buf, out_x, rows, rows_t, tok, acc, hidbuf, sbuf, ibuf, obuf, act, abuf, hbuf, stage,
    keycol, ids_row, mod_row, logp_ref, db_in, stats_ref, d_router, stat_work, stat_bufs, small_work, small_bufs,
    send_sem, recv_sem, own_sem, credit, x_send, x_recv, d_send, d_recv, y_send, y_recv, g_send, g_recv,
    self_sem, tok_sem, out_sem, i_sem, o_sem, a_sem, h_sem, hid_sem, s_sem, stat_send, stat_recv, small_send, small_recv,
):
    dp = lax.axis_index("dp")
    ep = lax.axis_index("ep")
    z, yy = dp // 4, lax.rem(dp, 4)
    xx, core = ep // 2, lax.rem(ep, 2)
    tiles = part_sum.shape[0]
    units = tiles // 4
    half = tiles // 2
    experts, capacity, width = out_x.shape
    n = experts * capacity
    pairs = experts // 2
    share = n // pairs
    steps = pairs * half
    others = experts - 1
    out_d = x_buf.reshape(out_x.shape)
    tok_slots = tok.reshape(out_x.shape)

    def wrap(v):
        return lax.rem(v + 16, 4)

    peers = [(z * 4 + wrap(yy + j), ep) for j in range(1, 4)] + [(wrap(z + j) * 4 + yy, ep) for j in range(1, 4)]
    enter = greet(peers + [(dp, lax.rem(ep + j, experts)) for j in range(1, experts)])
    load_x = pltpu.make_async_copy(x_any, x_buf, tok_sem.at[0])
    load_dy = pltpu.make_async_copy(dy_any, dy_buf, tok_sem.at[1])
    load_x.start()
    load_dy.start()

    rings = (
        (yy, peers[0:3]),
        (z, peers[3:6]),
        None,
        (xx, [(dp, lax.rem(ep + 2 * j, experts)) for j in range(1, 4)]),
    )
    partner = (dp, xx * 2 + 1 - core)

    def small_sum(work, bufs, whole_rows, send_sems, recv_sems):
        head = pl.ds(0, whole_rows)
        full = pl.ds(0, work.shape[1])

        def pair():
            return pltpu.make_async_remote_copy(
                src_ref=work.at[2, head], dst_ref=bufs.at[2, 0, head], send_sem=send_sems.at[2, 0], recv_sem=recv_sems.at[2, 0],
                device_id=partner, device_id_type=MESH)

        def ring(axis):
            me, ring_peers = rings[axis]
            at = head if axis == 3 else full
            return [
                pltpu.make_async_remote_copy(
                    src_ref=work.at[axis, at], dst_ref=bufs.at[axis, me, at], send_sem=send_sems.at[axis, j],
                    recv_sem=recv_sems.at[axis, j], device_id=ring_peers[j], device_id_type=MESH)
                for j in range(3)
            ]

        def launch(axis):
            bufs[axis, rings[axis][0]] = work[axis]
            for copy in ring(axis):
                copy.start()

        def total(axis, at):
            for copy in ring(axis):
                copy.wait()
            return bufs[axis, 0, at, :] + bufs[axis, 1, at, :] + bufs[axis, 2, at, :] + bufs[axis, 3, at, :]

        def step(k, dst=None):
            if k == 0:
                launch(0)
            elif k == 1:
                work[1] = total(0, full)
                launch(1)
            elif k == 2:
                work[2] = total(1, full)
                pair().start()
            elif k == 3:
                pair().wait()
                work[3] = work[2]
                work[3, head, :] = work[2, head, :] + bufs[2, 0, head, :]
                launch(3)
            else:
                dst[...] = work[2]
                dst[head, :] = total(3, head)

        return step

    stat_step = small_sum(stat_work, stat_bufs, 48, stat_send, stat_recv)
    small_step = small_sum(small_work, small_bufs, experts, small_send, small_recv)

    ids = wide(ids_ref)
    key = ids * n + wide(prio_ref)
    low = ids * n
    keycol[...] = col_of(key)

    def count(j, total):
        col = keycol[pl.ds(pl.multiple_of(j * 128, 128), 128), :][:, 0:1]
        before = jnp.logical_and(col < key, col >= low)
        return total + jnp.sum(before.astype(F32), axis=0, keepdims=True)

    position = lax.fori_loop(0, n // 128, count, jnp.zeros((1, n), F32))
    slot = jnp.where(position < capacity, ids * capacity + position, NOWHERE)
    slot_row[...] = jnp.broadcast_to(slot, slot_row.shape)
    mod = wide(mod_ref)
    ids_row[...] = jnp.broadcast_to(ids, ids_row.shape)
    mod_row[...] = jnp.broadcast_to(mod, mod_row.shape)

    def hops(q):
        return q + q // 2 - 2 * (q // 3)

    def target(j):
        return wrap(xx + hops((j + 1) // 2)) * 2 + lax.rem(core + 1 - lax.rem(j, 2), 2)

    def pick(e):
        index = (lax.broadcasted_iota(jnp.int32, (capacity, n), 0) + e * capacity).astype(F32)
        return (index == slot_row[0:1, :]).astype(BF16)

    def x_copy(j):
        to = target(j)
        return pltpu.make_async_remote_copy(
            src_ref=out_x.at[to], dst_ref=rows.at[ep], send_sem=x_send.at[j], recv_sem=x_recv.at[j],
            device_id=(dp, to), device_id_type=MESH)

    def d_copy(j, s):
        to = target(j)
        at = pl.ds(pl.multiple_of(s * TILE, TILE), TILE)
        return pltpu.make_async_remote_copy(
            src_ref=out_d.at[to, :, at], dst_ref=tok_slots.at[ep, :, at], send_sem=d_send.at[j, s], recv_sem=d_recv.at[j, s],
            device_id=(dp, to), device_id_type=MESH)

    def load_i(it):
        slot = lax.rem(it, 2)
        at = pl.ds(pl.multiple_of(lax.rem(it, half) * TILE, TILE), TILE)
        return pltpu.make_async_copy(w_in.at[:, at], ibuf.at[slot], i_sem.at[slot])

    def load_o(it):
        slot = lax.rem(it, 2)
        at = pl.ds(pl.multiple_of(lax.rem(it, half) * TILE, TILE), TILE)
        return pltpu.make_async_copy(w_out.at[at], obuf.at[slot], o_sem.at[slot])

    load_x.wait()
    enter()

    def send_x(j, carry):
        out_x[target(j)] = nn(pick(target(j)), x_buf[...]).astype(BF16)
        x_copy(j).start()
        return carry

    lax.fori_loop(0, others, send_x, 0)
    load_i(0).start()
    load_i(1).start()
    load_o(0).start()
    rows[ep] = nn(pick(ep), x_buf[...]).astype(BF16)

    router3 = jnp.concatenate(split3(router_ref[...]), axis=0)
    logits3 = nt(router3, x_buf[...])
    logits = logits3[0:experts] + logits3[experts:2 * experts] + logits3[2 * experts:3 * experts]
    shifted = logits - jnp.max(logits, axis=0, keepdims=True)
    logp = shifted - jnp.log(jnp.sum(jnp.exp(shifted), axis=0, keepdims=True))
    logp_ref[...] = logp
    probs = jnp.exp(logp)
    onehot = (lax.broadcasted_iota(jnp.int32, (experts, n), 0).astype(F32) == ids).astype(F32)
    gate = jnp.sum(probs * onehot, axis=0, keepdims=True)
    entropy = -jnp.sum(probs * logp, axis=0, keepdims=True)
    for m in range(2):
        mask = (mod == m).astype(F32)
        stat_work[0, 24 * m:24 * m + 8, :] = jnp.broadcast_to(jnp.sum(probs * mask, axis=1, keepdims=True), (8, 128))
        stat_work[0, 24 * m + 8:24 * m + 16, :] = jnp.broadcast_to(jnp.sum(entropy * mask, axis=1, keepdims=True), (8, 128))
        stat_work[0, 24 * m + 16:24 * m + 24, :] = jnp.broadcast_to(jnp.sum(mask, axis=1, keepdims=True), (8, 128))
    stat_step(0)
    load_dy.wait()
    dy_buf[...] = (col_of(gate)[:, 0:1] * dy_buf[...].astype(F32)).astype(BF16)

    def pick_cotangent(j, carry):
        out_d[target(j)] = nn(pick(target(j)), dy_buf[...]).astype(BF16)
        return carry

    lax.fori_loop(0, others, pick_cotangent, 0)
    tok_slots[ep] = nn(pick(ep), dy_buf[...]).astype(BF16)
    stat_step(1)
    acc[...] = jnp.broadcast_to(b_out_ref[...].astype(F32), acc.shape)
    small_work[0] = jnp.zeros(small_work.shape[1:], F32)

    def origin(it):
        return wrap(xx - hops(it // half))

    def store_a(it):
        slot = lax.rem(it, 3)
        at = pl.ds(pl.multiple_of(origin(it) * share, share), share)
        return pltpu.make_async_copy(abuf.at[slot], pre_act.at[lax.rem(it, half), at], a_sem.at[slot])

    def store_h(it):
        slot = lax.rem(it, 2)
        down = pl.ds(pl.multiple_of(lax.rem(it, half) * TILE, TILE), TILE)
        at = pl.ds(pl.multiple_of(origin(it) * share, share), share)
        return pltpu.make_async_copy(hbuf.at[slot], hidden_t.at[down, at], h_sem.at[slot])

    def first_matmul(it):
        at = pl.ds(pl.multiple_of(lax.rem(it, half) * TILE, TILE), TILE)
        chunk = rows[pl.ds(origin(it) * 2, 2)].reshape(share, width)
        abuf[lax.rem(it, 3)] = nn(chunk, ibuf[lax.rem(it, 2)]) + b_in_ref[:, at].astype(F32)

    def rest_of_step(it):
        a = abuf[lax.rem(it, 3)]
        t = jnp.tanh(ROOT * (a + CUBIC * (a * a * a)))
        hidden = (a * (0.5 * (1.0 + t))).astype(BF16)
        hbuf[lax.rem(it, 2)] = jnp.transpose(hidden)
        at = pl.ds(pl.multiple_of(origin(it) * share, share), share)
        acc[at, :] += nn(hidden, obuf[lax.rem(it, 2)])

    def forward(it, carry):
        nxt = it + 1
        store_a(it).start()
        load_o(it).wait()
        load_o(nxt).start()

        @pl.when(lax.rem(nxt, half) == 0)
        def _():
            q = nxt // half
            x_copy(2 * q - 1).wait_recv()
            x_copy(2 * q).wait_recv()

        load_i(nxt).wait()

        @pl.when(nxt + 1 < steps)
        def _():
            load_i(nxt + 1).start()

        @pl.when(it >= 2)
        def _():
            store_a(it - 2).wait()
            store_h(it - 2).wait()

        first_matmul(nxt)
        rest_of_step(it)
        store_h(it).start()
        for k, when in ((2, 4), (3, 8)):
            @pl.when(it == when)
            def _():
                stat_step(k)

        @pl.when(it == 9)
        def _():
            for s in range(3):
                for j in range(others):
                    d_copy(j, s).start()

        return carry

    x_copy(0).wait_recv()
    load_i(0).wait()
    first_matmul(jnp.int32(0))
    lax.fori_loop(0, steps - 1, forward, 0)
    last = jnp.int32(steps - 1)
    store_a(last).start()
    load_o(last).wait()
    store_a(last - 2).wait()
    store_h(last - 2).wait()
    rest_of_step(last)
    store_h(last).start()

    def place(stream):
        way = 1 - 2 * lax.rem(stream, 2)
        first_z = stream // 2
        pa = yy * (1 - first_z) + z * first_z
        pb = z * (1 - first_z) + yy * first_z

        def along(move):
            on_y = z * 4 + wrap(yy + move)
            on_z = wrap(z + move) * 4 + yy
            return on_y * (1 - first_z) + on_z * first_z, on_z * (1 - first_z) + on_y * first_z

        return way, pa, pb, along(way), along(-way)

    def send(tile, k):
        way, pa, pb, (next_a, next_b), _ = place(lax.rem(tile, 4))
        if k < 3:
            src, dst, to = part_sum.at[tile, wrap(pa - way * (k + 1))], land_a.at[lax.rem(tile, half), k], next_a
        elif k < 6:
            src, dst, to = part_sum.at[tile, pa, wrap(pb - way * (k - 2))], land_b.at[lax.rem(tile, half), k - 3], next_b
        elif k == 6:
            src, dst, to = own.at[tile], summed.at[tile, pa, pb], next_b
        elif k < 9:
            src = summed.at[tile, pa, wrap(pb - way * (k - 6))]
            dst, to = src, next_b
        else:
            src = summed.at[tile, wrap(pa - way * (k - 9))]
            dst, to = src, next_a
        return pltpu.make_async_remote_copy(
            src_ref=src, dst_ref=dst, send_sem=send_sem.at[tile, k], recv_sem=recv_sem.at[tile, k],
            device_id=(to, ep), device_id_type=MESH)

    def start(tile, k):
        if k < 6:
            @pl.when(tile >= half)
            def _():
                pl.semaphore_wait(credit.at[tile - half, k], 1)

        send(tile, k).start()

    def keep(tile):
        way, pa, pb, _, _ = place(lax.rem(tile, 4))
        return pltpu.make_async_copy(own.at[tile], summed.at[tile, pa, pb], own_sem.at[tile])

    def advance(tile, k):
        way, pa, pb, _, (prev_a, prev_b) = place(lax.rem(tile, 4))
        spot = lax.rem(tile, half)
        send(tile, k - 1).wait_recv()
        if k <= 3:
            block = wrap(pa - way * (k + 1))
            part_sum[tile, block] = part_sum[tile, block] + land_a[spot, k - 1]
        elif k <= 6:
            block = wrap(pb - way * (k - 2))
            total = part_sum[tile, pa, block] + land_b[spot, k - 4]
            if k < 6:
                part_sum[tile, pa, block] = total
            else:
                own[tile] = total.astype(BF16)
                keep(tile).start()
        elif k == 9:
            keep(tile).wait()
        if k <= 6:
            back_to = prev_a if k <= 3 else prev_b

            @pl.when(tile < half)
            def _():
                pl.semaphore_signal(credit.at[tile, k - 1], inc=1, device_id=(back_to, ep), device_id_type=MESH)

        if k < 12:
            start(tile, k)

    def wave(t, stream):
        for k in range(12, 0, -1):
            unit = t - k

            @pl.when(jnp.logical_and(unit >= 0, unit < units))
            def _():
                advance(unit * 4 + stream, k)

    def exchange(src, dst, send_sems, recv_sems):
        copies = []
        for j in range(1, experts):
            to = lax.rem(ep + j, experts)
            copies.append(pltpu.make_async_remote_copy(
                src_ref=src.at[to], dst_ref=dst.at[ep], send_sem=send_sems.at[j - 1], recv_sem=recv_sems.at[j - 1],
                device_id=(dp, to), device_id_type=MESH))
        return copies

    def place_tile(tile, a, grad):
        for b in range(4):
            for j in range(3):
                at = b * (width // 16) + j * 16
                part_sum[tile, a, b, :, j * TILE:(j + 1) * TILE] = grad[at:at + 16, :]

    def load_hid(i):
        slot = lax.rem(i, 2)
        at = pl.ds(pl.multiple_of(lax.rem(i, 8) * (width // 2), width // 2), width // 2)
        return pltpu.make_async_copy(hidden_t.at[at], hidbuf.at[slot], hid_sem.at[slot])

    def load_s(i):
        slot = lax.rem(i, 2)
        return pltpu.make_async_copy(pre_act.at[i], sbuf.at[slot], s_sem.at[slot])

    store_a(last - 1).wait()
    store_a(last).wait()
    store_h(last - 1).wait()
    store_h(last).wait()
    load_hid(jnp.int32(0)).start()
    load_s(jnp.int32(0)).start()
    load_i(0).start()
    load_o(0).start()
    for j in range(others):
        x_copy(j).wait_send()
    out_x[...] = acc[...].astype(BF16).reshape(out_x.shape)

    def out_tile(i, carry):
        unit, stream = i // 4, lax.rem(i, 4)
        wave(unit, stream)

        @pl.when(stream == 0)
        def _():
            for j in range(others):
                d_copy(j, unit).wait_recv()

        at = pl.ds(pl.multiple_of(unit * TILE, TILE), TILE)
        for piece in range(2):
            load_hid(2 * i + piece).wait()

            @pl.when(2 * i + piece + 1 < 2 * half)
            def _():
                load_hid(2 * i + piece + 1).start()

            grad = nn(hidbuf[piece], tok[:, at])
            for a in range(2):
                place_tile(i, 2 * piece + a, grad[a * (width // 4):(a + 1) * (width // 4)])
        start(i, 0)
        return carry

    lax.fori_loop(0, half, out_tile, 0)
    stat_step(4, stats_ref)
    send_y = exchange(out_x, back_y, y_send, y_recv)
    for copy in send_y:
        copy.start()
    self_y = pltpu.make_async_copy(out_x.at[ep], back_y.at[ep], self_sem.at[0])
    self_y.start()
    small_work[0, 12:13, :] = jnp.sum(tok[...].astype(F32), axis=0, keepdims=True)
    rows_t[...] = jnp.transpose(rows[...].reshape(n, width))
    acc[...] = jnp.zeros_like(acc)
    chunks = 4
    size = n // chunks

    def in_tile(i, carry):
        g = i + half
        wave(g // 4, lax.rem(g, 4))
        slot = lax.rem(i, 2)
        for load in (load_s, load_i, load_o):
            load(i).wait()

        @pl.when(i + 1 < half)
        def _():
            for load in (load_s, load_i, load_o):
                load(i + 1).start()

        total = jnp.zeros((1, TILE), F32)
        for c in range(chunks):
            part = pl.ds(c * size, size)
            d_hidden = nt(tok[part, :], obuf[slot]).astype(BF16)
            a = sbuf[slot, part, :]
            sq = a * a
            t = jnp.tanh(ROOT * (a + CUBIC * (sq * a)))
            slope = 0.5 * (1.0 + t) + (0.5 * ROOT) * a * (1.0 - t * t) * (1.0 + (3 * CUBIC) * sq)
            d_act = d_hidden.astype(F32) * slope
            total += jnp.sum(d_act, axis=0, keepdims=True)
            d_act_bf = d_act.astype(BF16)
            act[part, :] = d_act_bf
            acc[part, :] += nt(d_act_bf, ibuf[slot])
        db_in[:, pl.ds(pl.multiple_of(i * TILE, TILE), TILE)] = total
        for a in range(4):
            place_tile(g, a, nn(rows_t[pl.ds(a * (width // 4), width // 4), :], act[...]))
        start(g, 0)
        return carry

    lax.fori_loop(0, half, in_tile, 0)

    rows[...] = acc[...].astype(BF16).reshape(rows.shape)
    send_g = exchange(rows, back_d, g_send, g_recv)
    for copy in send_g:
        copy.start()
    self_g = pltpu.make_async_copy(rows.at[ep], back_d.at[ep], self_sem.at[1])
    self_g.start()

    for copy in send_y:
        copy.wait_recv()
    self_y.wait()
    back = pltpu.make_async_copy(back_y, dy_buf.reshape(back_y.shape), tok_sem.at[1])
    back.start()
    for i in range(4):
        small_work[0, 8 + i:9 + i, :] = db_in[:, i * width:(i + 1) * width]
    d_router[...] = jnp.zeros_like(d_router)
    loss, terms, inv = global_terms(stats_ref[...], experts)
    loss_ref[...] = jnp.broadcast_to(loss, loss_ref.shape)

    def token_loads(i):
        at = pl.ds(pl.multiple_of(i * CHUNK, CHUNK), CHUNK)
        return (
            pltpu.make_async_copy(dy_any.at[at], obuf.at[0], o_sem.at[0]),
            pltpu.make_async_copy(x_any.at[at], obuf.at[1], o_sem.at[1]),
        )

    def out_store(i):
        at = pl.ds(pl.multiple_of(i * CHUNK, CHUNK), CHUNK)
        return pltpu.make_async_copy(stage, out.at[at], out_sem)

    for copy in token_loads(jnp.int32(0)):
        copy.start()
    back.wait()
    pieces = n // CHUNK

    def combine(i):
        lanes = pl.ds(pl.multiple_of(i * CHUNK, CHUNK), CHUNK)
        slot_col = col_of(slot_row[0:1, lanes])[:, 0:1]
        chosen = (lax.broadcasted_iota(jnp.int32, (CHUNK, n), 1).astype(F32) == slot_col).astype(BF16)
        y_tok = nn(chosen, dy_buf[...])
        logp = logp_ref[:, lanes]
        probs = jnp.exp(logp)
        onehot = (lax.broadcasted_iota(jnp.int32, (experts, CHUNK), 0).astype(F32) == ids_row[:, lanes]).astype(F32)
        gate = jnp.sum(probs * onehot, axis=0, keepdims=True)
        for copy in token_loads(i):
            copy.wait()

        @pl.when(i > 0)
        def _():
            out_store(i - 1).wait()

        stage[...] = (col_of(gate)[:, 0:1] * y_tok).astype(BF16)
        out_store(i).start()
        d_gate = row_of(jnp.sum(obuf[0].astype(F32) * y_tok, axis=1, keepdims=True))[0:1]
        is_text = mod_row[:, lanes] == 1.0
        global_part = jnp.where(is_text, terms[1][:, 0:1], terms[0][:, 0:1])
        inv_count = jnp.where(is_text, inv[1][:, 0:1], inv[0][:, 0:1])
        d_probs = onehot * d_gate + global_part - logp * inv_count
        d_log = probs * (d_probs - jnp.sum(d_probs * probs, axis=0, keepdims=True))
        d_log_ref[:, lanes] = d_log
        d_router[...] += nn(jnp.concatenate(split3(d_log), axis=0), obuf[1])

        @pl.when(i + 1 < pieces)
        def _():
            for copy in token_loads(i + 1):
                copy.start()

    def rest(t, carry):
        def streams(s, inner):
            wave(t, s)

            @pl.when(s == 1)
            def _():
                combine(t - units)

            return inner

        return lax.fori_loop(0, 4, streams, carry)

    first = units + pieces
    lax.fori_loop(units, first, rest, 0)
    out_store(jnp.int32(pieces - 1)).wait()
    small_work[0, 0:experts, :] = d_router[0:experts] + d_router[experts:2 * experts] + d_router[2 * experts:]

    def late(t, carry):
        def streams(s, inner):
            wave(t, s)
            return inner

        return lax.fori_loop(0, 4, streams, carry)

    small_step(0)
    for k in range(1, 4):
        lax.fori_loop(first + k - 1, first + k, late, 0)
        small_step(k)
    lax.fori_loop(first + 3, units + 12, late, 0)
    small_step(4, small_ref)

    def drain(tile, carry):
        for k in range(12):
            send(tile, k).wait_send()
        return carry

    lax.fori_loop(0, tiles, drain, 0)
    for s in range(3):
        for j in range(others):
            d_copy(j, s).wait_send()
    for copy in send_y:
        copy.wait_send()
    for copy in send_g:
        copy.wait()
    self_g.wait()


def global_terms(stats, experts):
    loss = jnp.zeros((1, 128), F32)
    terms = []
    inv = []
    for m in range(2):
        base = 24 * m
        count = stats[base + 16:base + 17]
        mean = stats[base:base + 8] / count
        log_mean = jnp.log(mean)
        loss = loss + stats[base + 8:base + 9] / count + jnp.sum(mean * log_mean, axis=0, keepdims=True)
        terms.append(log_mean / count)
        inv.append(1.0 / count)
    return loss, terms, inv


def final_kernel(slot_ref, d_log_ref, back_any, router_ref, small_ref, loss_ref, summed, out_any,
                 dx, dw_in, dw_out, out, d_router_ref, db_in_ref, db_out_ref, aux_ref,
                 buf, back, out_buf, dx_buf, load_sem, store_sem, back_sem, out_sem, dx_sem):
    n, width = dx.shape
    tiles = buf.shape[0]
    half = tiles // 2
    units = tiles // 4
    experts = d_log_ref.shape[0]
    pieces = n // CHUNK

    load_back = pltpu.make_async_copy(back_any, back, back_sem)
    load_back.start()

    def loads(t):
        return [
            pltpu.make_async_copy(summed.at[t, :, :, :, pl.ds(j * TILE, TILE)], buf.at[t, :, :, j], load_sem.at[t, j])
            for j in range(3)
        ]

    def store(t):
        tile = buf.at[t].reshape(width, TILE)
        if t < half:
            unit, stream = t // 4, t % 4
            dst = dw_out.at[pl.ds(stream * width, width), pl.ds(unit * TILE, TILE)]
        else:
            dst = dw_in.at[:, pl.ds((t - half) * TILE, TILE)]
        return pltpu.make_async_copy(tile, dst, store_sem.at[t])

    for t in range(tiles):
        for copy in loads(t):
            copy.start()
    load_out = pltpu.make_async_copy(out_any, out_buf, out_sem.at[0])
    load_out.start()

    d_router_ref[...] = small_ref[0:experts, :]
    for i in range(4):
        db_in_ref[:, i * width:(i + 1) * width] = small_ref[8 + i:9 + i, :].astype(BF16)
    db_out_ref[...] = small_ref[12:13, :].astype(BF16)
    aux_ref[0, 0] = loss_ref[0, 0]
    r = split3(router_ref[...])
    rights = jnp.concatenate([r[0], r[1], r[0], r[1], r[2], r[0]], axis=0)
    load_back.wait()

    def dx_store(i):
        at = pl.ds(i * CHUNK, CHUNK)
        return pltpu.make_async_copy(dx_buf.at[at], dx.at[at], dx_sem.at[i])

    per_piece = tiles // pieces
    for i in range(pieces):
        lanes = pl.ds(i * CHUNK, CHUNK)
        d = split3(d_log_ref[:, lanes])
        lefts = jnp.concatenate([d[0], d[0], d[1], d[1], d[0], d[2]], axis=0)
        routed = tn(lefts, rights).astype(BF16)
        slot_col = col_of(slot_ref[0:1, lanes])[:, 0:1]
        chosen = (lax.broadcasted_iota(jnp.int32, (CHUNK, n), 1).astype(F32) == slot_col).astype(BF16)
        dx_buf[lanes, :] = (nn(chosen, back[...]) + routed.astype(F32)).astype(BF16)
        dx_store(i).start()
        for t in range(i * per_piece, (i + 1) * per_piece):
            for copy in loads(t):
                copy.wait()
            store(t).start()
    load_out.wait()
    store_out = pltpu.make_async_copy(out_buf, out, out_sem.at[1])
    store_out.start()
    for t in range(tiles):
        store(t).wait()
    for i in range(pieces):
        dx_store(i).wait()
    store_out.wait()


def vmem(count):
    return [pl.BlockSpec(memory_space=pltpu.VMEM)] * count


def cost(flops, size):
    return pl.CostEstimate(flops=int(flops), bytes_accessed=int(size), transcendentals=0)


def solution(mesh):
    token_spec = P(ALL_AXES)
    expert_spec = P("ep")

    def local_step(x, modality, router, expert_ids, priority, w_in, b_in, w_out, b_out, dy):
        n, width = x.shape
        experts = router.shape[1]
        hid = w_in.shape[2]
        capacity = n // experts
        tiles = hid // TILE
        share = n // (experts // 2)
        w_in, w_out = w_in[0], w_out[0]
        ids, prio, mod = (a.reshape(n // 128, 128) for a in (expert_ids, priority, modality))
        router_t = jnp.transpose(router)
        shape = jax.ShapeDtypeStruct
        anywhere = pl.BlockSpec(memory_space=pl.ANY)
        dma = pltpu.SemaphoreType.DMA
        slots = (experts, capacity, width)
        mm = 2 * n * width * hid
        others = experts - 1

        summed, back_y, d_back, out, _, _, slot, d_log, loss, small = pl.pallas_call(
            block_kernel,
            out_shape=(
                shape((2 * tiles, 4, 4, 16, width), BF16), shape(slots, BF16), shape(slots, BF16), shape((n, width), BF16),
                shape((hid, n), BF16), shape((tiles, n, TILE), F32),
                shape((8, n), F32), shape((experts, n), F32), shape((8, 128), F32), shape((16, width), F32),
            ),
            in_specs=vmem(3) + [anywhere] * 2 + vmem(1) + [anywhere] + vmem(1) + [anywhere] + vmem(1),
            out_specs=(*[anywhere] * 6, *vmem(4)),
            scratch_shapes=[
                pltpu.VMEM((2 * tiles, 4, 4, 16, width), F32),
                pltpu.VMEM((tiles, 3, 4, 16, width), F32),
                pltpu.VMEM((tiles, 3, 16, width), F32),
                pltpu.VMEM((2 * tiles, 16, width), BF16),
                pltpu.VMEM((n, width), BF16),
                pltpu.VMEM((n, width), BF16),
                pltpu.VMEM(slots, BF16),
                pltpu.VMEM(slots, BF16),
                pltpu.VMEM((width, n), BF16),
                pltpu.VMEM((n, width), BF16),
                pltpu.VMEM((n, width), F32),
                pltpu.VMEM((2, width // 2, n), BF16),
                pltpu.VMEM((2, n, TILE), F32),
                pltpu.VMEM((2, width, TILE), BF16),
                pltpu.VMEM((2, TILE, width), BF16),
                pltpu.VMEM((n, TILE), BF16),
                pltpu.VMEM((3, share, TILE), F32),
                pltpu.VMEM((2, TILE, share), BF16),
                pltpu.VMEM((CHUNK, width), BF16),
                pltpu.VMEM((n, 8), F32),
                pltpu.VMEM((8, n), F32),
                pltpu.VMEM((8, n), F32),
                pltpu.VMEM((experts, n), F32),
                pltpu.VMEM((1, hid), F32),
                pltpu.VMEM((48, 128), F32),
                pltpu.VMEM((3 * experts, width), F32),
                pltpu.VMEM((4, 48, 128), F32), pltpu.VMEM((4, 4, 48, 128), F32),
                pltpu.VMEM((4, 16, width), F32), pltpu.VMEM((4, 4, 16, width), F32),
                dma((2 * tiles, 12)), dma((2 * tiles, 12)), dma((2 * tiles,)), pltpu.SemaphoreType.REGULAR((tiles, 6)),
                dma((others,)), dma((others,)), dma((others, 3)), dma((others, 3)),
                dma((others,)), dma((others,)), dma((others,)), dma((others,)),
                dma((2,)), dma((2,)), dma, dma((2,)), dma((2,)), dma((3,)), dma((2,)), dma((2,)), dma((2,)),
                dma((4, 3)), dma((4, 3)), dma((4, 3)), dma((4, 3)),
            ],
            compiler_params=pltpu.CompilerParams(collective_id=1, has_side_effects=True, vmem_limit_bytes=67_000_000),
            cost_estimate=cost(6 * mm, 6 * n * hid), name="block",
        )(ids, prio, mod, x, dy, router_t, w_in, b_in, w_out, b_out)

        d_x, d_w_in, d_w_out, out, d_router, d_b_in, d_b_out, aux = pl.pallas_call(
            final_kernel,
            out_shape=(
                shape((n, width), BF16), shape((width, hid), BF16), shape((hid, width), BF16), shape((n, width), BF16),
                shape((experts, width), F32), shape((1, hid), BF16), shape((1, width), BF16), shape((1, 1), F32),
            ),
            in_specs=vmem(2) + [anywhere] + vmem(3) + [anywhere] * 2,
            out_specs=(*[anywhere] * 4, *vmem(3), pl.BlockSpec(memory_space=pltpu.SMEM)),
            scratch_shapes=[
                pltpu.VMEM((2 * tiles, 4, 4, 3, 16, TILE), BF16),
                pltpu.VMEM((n, width), BF16), pltpu.VMEM((n, width), BF16), pltpu.VMEM((n, width), BF16),
                dma((2 * tiles, 3)), dma((2 * tiles,)), dma, dma((2,)), dma((n // CHUNK,)),
            ],
            compiler_params=pltpu.CompilerParams(vmem_limit_bytes=40_000_000),
            cost_estimate=cost(2 * n * n * width, 8 * width * hid), name="final",
        )(slot, d_log, d_back.reshape(n, width), router_t, small, loss, summed, out)
        return out, aux[0, 0], d_x, jnp.transpose(d_router), d_w_in[None], d_b_in, d_w_out[None], d_b_out

    return jax.shard_map(
        local_step,
        mesh=mesh,
        in_specs=(token_spec, token_spec, P(), token_spec, token_spec, expert_spec, expert_spec, expert_spec, expert_spec, token_spec),
        out_specs=(token_spec, P(), token_spec, P(), expert_spec, expert_spec, expert_spec, expert_spec),
        check_vma=False,
    )
```

```python
import functools

import jax
import jax.numpy as jnp
from jax import lax
from jax.experimental import pallas as pl
from jax.experimental.pallas import tpu as pltpu
from jax.sharding import PartitionSpec as P

ALL_AXES = ("dp", "ep")
MESH = pl.DeviceIdType.MESH
F32 = jnp.float32
BF16 = jnp.bfloat16
NOWHERE = -1.0
TILE = 256
CHUNK = 256
WIDE = 768


def col_of(row):
    return jnp.transpose(jnp.broadcast_to(row, (8, row.shape[1])))


def row_of(col):
    return jnp.transpose(jnp.broadcast_to(col, (col.shape[0], 8)))


def split3(a):
    hi = a.astype(BF16)
    rest = a - hi.astype(F32)
    mid = rest.astype(BF16)
    lo = (rest - mid.astype(F32)).astype(BF16)
    return hi, mid, lo


def nt(a, b):
    return lax.dot_general(a, b, (((1,), (1,)), ((), ())), preferred_element_type=F32)


def tn(a, b):
    return lax.dot_general(a, b, (((0,), (0,)), ((), ())), preferred_element_type=F32)


def nn(a, b):
    return jnp.dot(a, b, preferred_element_type=F32)


def wide(ref):
    v = ref[...].astype(F32)
    return jnp.concatenate([v[i:i + 1, :] for i in range(v.shape[0])], axis=1)


def greet(peers):
    barrier = pltpu.get_barrier_semaphore()
    for peer in peers:
        pl.semaphore_signal(barrier, inc=1, device_id=peer, device_id_type=MESH)
    return lambda: pl.semaphore_wait(barrier, len(peers))


ROOT = 0.7978845608028654
CUBIC = 0.044715


def block_kernel(
    ids_ref, prio_ref, mod_ref, x_any, dy_any, router_ref, w_in, b_in_ref, w_out, b_out_ref,
    summed, back_y, back_d, out, hidden_t, pre_act, slot_row, d_log_ref, loss_ref, small_ref,
    part_sum, land_a, land_b, own, x_buf, dy_buf, out_x, rows, rows_t, tok, acc, wbuf, sbuf, act, hbuf, stage, late,
    keycol, ids_row, mod_row, logp_ref, db_in, stats_ref, d_router, stat_work, stat_bufs, small_work, small_bufs,
    send_sem, recv_sem, own_sem, credit, x_send, x_recv, d_send, d_recv, y_send, y_recv, g_send, g_recv,
    self_sem, tok_sem, out_sem, i_sem, o_sem, a_sem, h_sem, hid_sem, s_sem, late_sem, stat_send, stat_recv, small_send, small_recv,
):
    dp = lax.axis_index("dp")
    ep = lax.axis_index("ep")
    z, yy = dp // 4, lax.rem(dp, 4)
    xx, core = ep // 2, lax.rem(ep, 2)
    tiles = part_sum.shape[0]
    units = tiles // 4
    half = tiles // 2
    experts, capacity, width = out_x.shape
    n = experts * capacity
    pairs = experts // 2
    share = n // pairs
    fwd_tiles = hidden_t.shape[1] // WIDE
    steps = pairs * fwd_tiles
    groups = part_sum.reshape(tiles * 16, 16, width)
    late_from = tiles - late.shape[0]
    others = experts - 1
    out_d = x_buf.reshape(out_x.shape)
    tok_slots = tok.reshape(out_x.shape)

    def wrap(v):
        return lax.rem(v + 16, 4)

    peers = [(z * 4 + wrap(yy + j), ep) for j in range(1, 4)] + [(wrap(z + j) * 4 + yy, ep) for j in range(1, 4)]
    enter = greet(peers + [(dp, lax.rem(ep + j, experts)) for j in range(1, experts)])
    load_x = pltpu.make_async_copy(x_any, x_buf, tok_sem.at[0])
    load_dy = pltpu.make_async_copy(dy_any, dy_buf, tok_sem.at[1])
    load_x.start()
    load_dy.start()

    rings = (
        (yy, peers[0:3]),
        (z, peers[3:6]),
        None,
        (xx, [(dp, lax.rem(ep + 2 * j, experts)) for j in range(1, 4)]),
    )
    partner = (dp, xx * 2 + 1 - core)

    def small_sum(work, bufs, whole_rows, send_sems, recv_sems):
        head = pl.ds(0, whole_rows)
        full = pl.ds(0, work.shape[1])

        def pair():
            return pltpu.make_async_remote_copy(
                src_ref=work.at[2, head], dst_ref=bufs.at[2, 0, head], send_sem=send_sems.at[2, 0], recv_sem=recv_sems.at[2, 0],
                device_id=partner, device_id_type=MESH)

        def ring(axis):
            me, ring_peers = rings[axis]
            at = head if axis == 3 else full
            return [
                pltpu.make_async_remote_copy(
                    src_ref=work.at[axis, at], dst_ref=bufs.at[axis, me, at], send_sem=send_sems.at[axis, j],
                    recv_sem=recv_sems.at[axis, j], device_id=ring_peers[j], device_id_type=MESH)
                for j in range(3)
            ]

        def launch(axis):
            bufs[axis, rings[axis][0]] = work[axis]
            for copy in ring(axis):
                copy.start()

        def total(axis, at):
            for copy in ring(axis):
                copy.wait()
            return bufs[axis, 0, at, :] + bufs[axis, 1, at, :] + bufs[axis, 2, at, :] + bufs[axis, 3, at, :]

        def step(k, dst=None):
            if k == 0:
                launch(0)
            elif k == 1:
                work[1] = total(0, full)
                launch(1)
            elif k == 2:
                work[2] = total(1, full)
                pair().start()
            elif k == 3:
                pair().wait()
                work[3] = work[2]
                work[3, head, :] = work[2, head, :] + bufs[2, 0, head, :]
                launch(3)
            else:
                dst[...] = work[2]
                dst[head, :] = total(3, head)

        return step

    stat_step = small_sum(stat_work, stat_bufs, 48, stat_send, stat_recv)
    small_step = small_sum(small_work, small_bufs, experts, small_send, small_recv)

    ids = wide(ids_ref)
    key = ids * n + wide(prio_ref)
    low = ids * n
    keycol[...] = col_of(key)

    def count(j, total):
        col = keycol[pl.ds(pl.multiple_of(j * 128, 128), 128), :][:, 0:1]
        before = jnp.logical_and(col < key, col >= low)
        return total + jnp.sum(before.astype(F32), axis=0, keepdims=True)

    position = lax.fori_loop(0, n // 128, count, jnp.zeros((1, n), F32))
    slot = jnp.where(position < capacity, ids * capacity + position, NOWHERE)
    slot_row[...] = jnp.broadcast_to(slot, slot_row.shape)
    mod = wide(mod_ref)
    ids_row[...] = jnp.broadcast_to(ids, ids_row.shape)
    mod_row[...] = jnp.broadcast_to(mod, mod_row.shape)

    def hops(q):
        return q + q // 2 - 2 * (q // 3)

    def target(j):
        return wrap(xx + hops((j + 1) // 2)) * 2 + lax.rem(core + 1 - lax.rem(j, 2), 2)

    def pick(e):
        index = (lax.broadcasted_iota(jnp.int32, (capacity, n), 0) + e * capacity).astype(F32)
        return (index == slot_row[0:1, :]).astype(BF16)

    def x_copy(j):
        to = target(j)
        return pltpu.make_async_remote_copy(
            src_ref=out_x.at[to], dst_ref=rows.at[ep], send_sem=x_send.at[j], recv_sem=x_recv.at[j],
            device_id=(dp, to), device_id_type=MESH)

    def d_copy(j, s):
        to = target(j)
        at = pl.ds(pl.multiple_of(s * TILE, TILE), TILE)
        return pltpu.make_async_remote_copy(
            src_ref=out_d.at[to, :, at], dst_ref=tok_slots.at[ep, :, at], send_sem=d_send.at[j, s], recv_sem=d_recv.at[j, s],
            device_id=(dp, to), device_id_type=MESH)

    def load_i(it):
        slot = lax.rem(it, 2)
        at = pl.ds(pl.multiple_of(lax.rem(it, fwd_tiles) * WIDE, WIDE), WIDE)
        return pltpu.make_async_copy(w_in.at[:, at], wbuf.at[slot], i_sem.at[slot])

    def load_o(it):
        slot = lax.rem(it, 2)
        at = pl.ds(pl.multiple_of(lax.rem(it, fwd_tiles) * WIDE, WIDE), WIDE)
        return pltpu.make_async_copy(w_out.at[at], wbuf.at[2 + slot], o_sem.at[slot])

    load_x.wait()
    enter()

    def send_x(j, carry):
        out_x[target(j)] = nn(pick(target(j)), x_buf[...]).astype(BF16)
        x_copy(j).start()
        return carry

    lax.fori_loop(0, others, send_x, 0)
    load_i(0).start()
    load_i(1).start()
    load_o(0).start()
    rows[ep] = nn(pick(ep), x_buf[...]).astype(BF16)

    router3 = jnp.concatenate(split3(router_ref[...]), axis=0)
    logits3 = nt(router3, x_buf[...])
    logits = logits3[0:experts] + logits3[experts:2 * experts] + logits3[2 * experts:3 * experts]
    shifted = logits - jnp.max(logits, axis=0, keepdims=True)
    logp = shifted - jnp.log(jnp.sum(jnp.exp(shifted), axis=0, keepdims=True))
    logp_ref[...] = logp
    probs = jnp.exp(logp)
    onehot = (lax.broadcasted_iota(jnp.int32, (experts, n), 0).astype(F32) == ids).astype(F32)
    gate = jnp.sum(probs * onehot, axis=0, keepdims=True)
    entropy = -jnp.sum(probs * logp, axis=0, keepdims=True)
    for m in range(2):
        mask = (mod == m).astype(F32)
        stat_work[0, 24 * m:24 * m + 8, :] = jnp.broadcast_to(jnp.sum(probs * mask, axis=1, keepdims=True), (8, 128))
        stat_work[0, 24 * m + 8:24 * m + 16, :] = jnp.broadcast_to(jnp.sum(entropy * mask, axis=1, keepdims=True), (8, 128))
        stat_work[0, 24 * m + 16:24 * m + 24, :] = jnp.broadcast_to(jnp.sum(mask, axis=1, keepdims=True), (8, 128))
    stat_step(0)
    load_dy.wait()
    dy_buf[...] = (col_of(gate)[:, 0:1] * dy_buf[...].astype(F32)).astype(BF16)

    def pick_cotangent(j, carry):
        out_d[target(j)] = nn(pick(target(j)), dy_buf[...]).astype(BF16)
        return carry

    lax.fori_loop(0, others, pick_cotangent, 0)
    tok_slots[ep] = nn(pick(ep), dy_buf[...]).astype(BF16)
    stat_step(1)
    acc[...] = jnp.broadcast_to(b_out_ref[...].astype(F32), acc.shape)
    small_work[0] = jnp.zeros(small_work.shape[1:], F32)

    def origin(it):
        return wrap(xx - hops(it // fwd_tiles))

    def store_a(it):
        slot = lax.rem(it, 3)
        at = pl.ds(pl.multiple_of(origin(it) * (share // 16), share // 16), share // 16)
        return pltpu.make_async_copy(
            groups.at[pl.ds(slot * (share // 16), share // 16)], pre_act.at[lax.rem(it, fwd_tiles), at], a_sem.at[slot])

    def store_h(it):
        slot = lax.rem(it, 2)
        down = pl.ds(pl.multiple_of(lax.rem(it, fwd_tiles) * WIDE, WIDE), WIDE)
        at = pl.ds(pl.multiple_of(lax.rem(origin(it), 2) * share, share), share)
        return pltpu.make_async_copy(hbuf.at[slot], hidden_t.at[origin(it) // 2, down, at], h_sem.at[slot])

    def first_matmul(it):
        at = pl.ds(pl.multiple_of(lax.rem(it, fwd_tiles) * WIDE, WIDE), WIDE)
        chunk = rows[pl.ds(origin(it) * 2, 2)].reshape(share, width)
        a = nn(chunk, wbuf[lax.rem(it, 2)]) + b_in_ref[:, at].astype(F32)
        groups[pl.ds(lax.rem(it, 3) * (share // 16), share // 16)] = a.reshape(share // 16, 16, WIDE)

    def rest_of_step(it):
        a = groups[pl.ds(lax.rem(it, 3) * (share // 16), share // 16)].reshape(share, WIDE)
        t = jnp.tanh(ROOT * (a + CUBIC * (a * a * a)))
        hidden = (a * (0.5 * (1.0 + t))).astype(BF16)
        hbuf[lax.rem(it, 2)] = jnp.transpose(hidden)
        at = pl.ds(pl.multiple_of(origin(it) * share, share), share)
        acc[at, :] += nn(hidden, wbuf[2 + lax.rem(it, 2)])

    def forward(it, carry):
        nxt = it + 1
        store_a(it).start()
        load_o(it).wait()
        load_o(nxt).start()

        @pl.when(lax.rem(nxt, fwd_tiles) == 0)
        def _():
            q = nxt // fwd_tiles
            x_copy(2 * q - 1).wait_recv()
            x_copy(2 * q).wait_recv()

        load_i(nxt).wait()

        @pl.when(nxt + 1 < steps)
        def _():
            load_i(nxt + 1).start()

        @pl.when(it >= 2)
        def _():
            store_a(it - 2).wait()
            store_h(it - 2).wait()

        rest_of_step(it)
        first_matmul(nxt)
        store_h(it).start()
        for k, when in ((2, 1), (3, 2)):
            @pl.when(it == when)
            def _():
                stat_step(k)

        @pl.when(it == 3)
        def _():
            for s in range(3):
                for j in range(others):
                    d_copy(j, s).start()

        return carry

    x_copy(0).wait_recv()
    load_i(0).wait()
    first_matmul(jnp.int32(0))
    lax.fori_loop(0, steps - 1, forward, 0)
    last = jnp.int32(steps - 1)
    store_a(last).start()
    load_o(last).wait()
    store_a(last - 2).wait()
    store_h(last - 2).wait()
    rest_of_step(last)
    store_h(last).start()

    def place(stream):
        way = 1 - 2 * lax.rem(stream, 2)
        first_z = stream // 2
        pa = yy * (1 - first_z) + z * first_z
        pb = z * (1 - first_z) + yy * first_z

        def along(move):
            on_y = z * 4 + wrap(yy + move)
            on_z = wrap(z + move) * 4 + yy
            return on_y * (1 - first_z) + on_z * first_z, on_z * (1 - first_z) + on_y * first_z

        return way, pa, pb, along(way), along(-way)

    def send(tile, k, end=False):
        way, pa, pb, (next_a, next_b), _ = place(lax.rem(tile, 4))
        whole = late.at[tile - late_from] if end else summed.at[tile]
        if k < 3:
            src, dst, to = part_sum.at[tile, wrap(pa - way * (k + 1))], land_a.at[lax.rem(tile, half), k], next_a
        elif k < 6:
            src, dst, to = part_sum.at[tile, pa, wrap(pb - way * (k - 2))], land_b.at[lax.rem(tile, half), k - 3], next_b
        elif k < 9:
            src = whole.at[pa, wrap(pb - way * (k - 6))]
            dst, to = src, next_b
            if k == 6 and not end:
                src = own.at[tile]
        else:
            src = whole.at[wrap(pa - way * (k - 9))]
            dst, to = src, next_a
        return pltpu.make_async_remote_copy(
            src_ref=src, dst_ref=dst, send_sem=send_sem.at[tile, k], recv_sem=recv_sem.at[tile, k],
            device_id=(to, ep), device_id_type=MESH)

    def act_on(tile, k, action):
        if k < 6:
            action(send(tile, k))
        else:
            @pl.when(tile < late_from)
            def _():
                action(send(tile, k))

            @pl.when(tile >= late_from)
            def _():
                action(send(tile, k, True))

    def start(tile, k):
        if k < 6:
            @pl.when(tile >= half)
            def _():
                pl.semaphore_wait(credit.at[tile - half, k], 1)

        act_on(tile, k, lambda copy: copy.start())

    def keep(tile):
        way, pa, pb, _, _ = place(lax.rem(tile, 4))
        return pltpu.make_async_copy(own.at[tile], summed.at[tile, pa, pb], own_sem.at[tile])

    def keep_late(tile):
        spot = tile - late_from
        return pltpu.make_async_copy(late.at[spot], summed.at[tile], late_sem.at[spot])

    def advance(tile, k):
        way, pa, pb, _, (prev_a, prev_b) = place(lax.rem(tile, 4))
        spot = lax.rem(tile, half)
        act_on(tile, k - 1, lambda copy: copy.wait_recv())
        if k <= 3:
            block = wrap(pa - way * (k + 1))
            part_sum[tile, block] = part_sum[tile, block] + land_a[spot, k - 1]
        elif k <= 6:
            block = wrap(pb - way * (k - 2))
            total = part_sum[tile, pa, block] + land_b[spot, k - 4]
            if k < 6:
                part_sum[tile, pa, block] = total
            else:
                @pl.when(tile < late_from)
                def _():
                    own[tile] = total.astype(BF16)
                    keep(tile).start()

                @pl.when(tile >= late_from)
                def _():
                    late[tile - late_from, pa, pb] = total.astype(BF16)
        elif k == 9:
            @pl.when(tile < late_from)
            def _():
                keep(tile).wait()
        elif k == 12:
            @pl.when(tile >= late_from)
            def _():
                keep_late(tile).start()
        if k <= 6:
            back_to = prev_a if k <= 3 else prev_b

            @pl.when(tile < half)
            def _():
                pl.semaphore_signal(credit.at[tile, k - 1], inc=1, device_id=(back_to, ep), device_id_type=MESH)

        if k < 12:
            start(tile, k)

    def wave(t, stream):
        for k in range(12, 0, -1):
            unit = t - k

            @pl.when(jnp.logical_and(unit >= 0, unit < units))
            def _():
                advance(unit * 4 + stream, k)

    def exchange(src, dst, send_sems, recv_sems):
        copies = []
        for j in range(1, experts):
            to = lax.rem(ep + j, experts)
            copies.append(pltpu.make_async_remote_copy(
                src_ref=src.at[to], dst_ref=dst.at[ep], send_sem=send_sems.at[j - 1], recv_sem=recv_sems.at[j - 1],
                device_id=(dp, to), device_id_type=MESH))
        return copies

    def place_tile(tile, a, grad):
        for b in range(4):
            for j in range(3):
                at = b * (width // 16) + j * 16
                part_sum[tile, a, b, :, j * TILE:(j + 1) * TILE] = grad[at:at + 16, :]

    def load_hid(i):
        base = 2 * lax.rem(i, 2)
        at = pl.ds(pl.multiple_of(lax.rem(i, 4) * WIDE, WIDE), WIDE)
        return [pltpu.make_async_copy(hidden_t.at[h, at], wbuf.at[base + h], hid_sem.at[base + h]) for h in range(2)]

    def load_rest(i):
        slot = lax.rem(i, 2)
        at = pl.ds(pl.multiple_of(i * TILE, TILE), TILE)
        lanes = pl.ds(pl.multiple_of(lax.rem(i, WIDE // TILE) * TILE, TILE), TILE)
        return (
            pltpu.make_async_copy(pre_act.at[i // (WIDE // TILE), :, :, lanes], sbuf.at[slot], s_sem.at[slot]),
            pltpu.make_async_copy(w_in.at[:, at], wbuf.at[slot, :, pl.ds(0, TILE)], i_sem.at[slot]),
            pltpu.make_async_copy(w_out.at[at], wbuf.at[2 + slot, pl.ds(0, TILE)], o_sem.at[slot]),
        )

    store_a(last - 1).wait()
    store_a(last).wait()
    store_h(last - 1).wait()
    store_h(last).wait()
    for copy in load_hid(jnp.int32(0)):
        copy.start()
    for j in range(others):
        x_copy(j).wait_send()
    out_x[...] = acc[...].astype(BF16).reshape(out_x.shape)

    def out_tile(i, carry):
        unit, stream = i // 4, lax.rem(i, 4)
        wave(unit, stream)

        @pl.when(stream == 0)
        def _():
            for j in range(others):
                d_copy(j, unit).wait_recv()

        at = pl.ds(pl.multiple_of(unit * TILE, TILE), TILE)
        for copy in load_hid(i):
            copy.wait()

        @pl.when(i + 1 < half)
        def _():
            for copy in load_hid(i + 1):
                copy.start()

        base = 2 * lax.rem(i, 2)
        for a in range(2):
            part = slice(a * (WIDE // 2), (a + 1) * (WIDE // 2))
            grad = nn(wbuf[base, part, :], tok[0:WIDE, at]) + nn(wbuf[base + 1, part, :], tok[WIDE:, at])
            for b in range(2):
                place_tile(i, 2 * a + b, grad[b * (width // 4):(b + 1) * (width // 4)])
        start(i, 0)
        return carry

    lax.fori_loop(0, half, out_tile, 0)
    for copy in load_rest(jnp.int32(0)):
        copy.start()
    stat_step(4, stats_ref)
    send_y = exchange(out_x, back_y, y_send, y_recv)
    for copy in send_y:
        copy.start()
    self_y = pltpu.make_async_copy(out_x.at[ep], back_y.at[ep], self_sem.at[0])
    self_y.start()
    small_work[0, 12:13, :] = jnp.sum(tok[...].astype(F32), axis=0, keepdims=True)
    rows_t[...] = jnp.transpose(rows[...].reshape(n, width))
    acc[...] = jnp.zeros_like(acc)
    chunks = 4
    size = n // chunks

    def in_tile(i, carry):
        g = i + half
        wave(g // 4, lax.rem(g, 4))
        slot = lax.rem(i, 2)
        for copy in load_rest(i):
            copy.wait()

        @pl.when(i + 1 < half)
        def _():
            for copy in load_rest(i + 1):
                copy.start()

        total = jnp.zeros((1, TILE), F32)
        for c in range(chunks):
            part = pl.ds(c * size, size)
            d_hidden = nt(tok[part, :], wbuf[2 + slot, 0:TILE, :]).astype(BF16)
            a = sbuf[slot, c * (size // 16):(c + 1) * (size // 16)].reshape(size, TILE)
            sq = a * a
            t = jnp.tanh(ROOT * (a + CUBIC * (sq * a)))
            slope = 0.5 * (1.0 + t) + (0.5 * ROOT) * a * (1.0 - t * t) * (1.0 + (3 * CUBIC) * sq)
            d_act = d_hidden.astype(F32) * slope
            total += jnp.sum(d_act, axis=0, keepdims=True)
            d_act_bf = d_act.astype(BF16)
            act[part, :] = d_act_bf
            acc[part, :] += nt(d_act_bf, wbuf[slot, :, 0:TILE])
        db_in[:, pl.ds(pl.multiple_of(i * TILE, TILE), TILE)] = total
        for a in range(4):
            place_tile(g, a, nn(rows_t[pl.ds(a * (width // 4), width // 4), :], act[...]))
        start(g, 0)
        return carry

    lax.fori_loop(0, half, in_tile, 0)

    rows[...] = acc[...].astype(BF16).reshape(rows.shape)
    send_g = exchange(rows, back_d, g_send, g_recv)
    for copy in send_g:
        copy.start()
    self_g = pltpu.make_async_copy(rows.at[ep], back_d.at[ep], self_sem.at[1])
    self_g.start()

    for copy in send_y:
        copy.wait_recv()
    self_y.wait()
    back = pltpu.make_async_copy(back_y, dy_buf.reshape(back_y.shape), tok_sem.at[1])
    back.start()
    for i in range(4):
        small_work[0, 8 + i:9 + i, :] = db_in[:, i * width:(i + 1) * width]
    d_router[...] = jnp.zeros_like(d_router)
    loss, terms, inv = global_terms(stats_ref[...], experts)
    loss_ref[...] = jnp.broadcast_to(loss, loss_ref.shape)

    def token_loads(i):
        at = pl.ds(pl.multiple_of(i * CHUNK, CHUNK), CHUNK)
        return (
            pltpu.make_async_copy(dy_any.at[at], wbuf.at[2, pl.ds(0, CHUNK)], o_sem.at[0]),
            pltpu.make_async_copy(x_any.at[at], wbuf.at[3, pl.ds(0, CHUNK)], o_sem.at[1]),
        )

    def out_store(i):
        at = pl.ds(pl.multiple_of(i * CHUNK, CHUNK), CHUNK)
        return pltpu.make_async_copy(stage, out.at[at], out_sem)

    for copy in token_loads(jnp.int32(0)):
        copy.start()
    back.wait()
    pieces = n // CHUNK

    def combine(i):
        lanes = pl.ds(pl.multiple_of(i * CHUNK, CHUNK), CHUNK)
        slot_col = col_of(slot_row[0:1, lanes])[:, 0:1]
        chosen = (lax.broadcasted_iota(jnp.int32, (CHUNK, n), 1).astype(F32) == slot_col).astype(BF16)
        y_tok = nn(chosen, dy_buf[...])
        logp = logp_ref[:, lanes]
        probs = jnp.exp(logp)
        onehot = (lax.broadcasted_iota(jnp.int32, (experts, CHUNK), 0).astype(F32) == ids_row[:, lanes]).astype(F32)
        gate = jnp.sum(probs * onehot, axis=0, keepdims=True)
        for copy in token_loads(i):
            copy.wait()

        @pl.when(i > 0)
        def _():
            out_store(i - 1).wait()

        stage[...] = (col_of(gate)[:, 0:1] * y_tok).astype(BF16)
        out_store(i).start()
        d_gate = row_of(jnp.sum(wbuf[2, 0:CHUNK, :].astype(F32) * y_tok, axis=1, keepdims=True))[0:1]
        is_text = mod_row[:, lanes] == 1.0
        global_part = jnp.where(is_text, terms[1][:, 0:1], terms[0][:, 0:1])
        inv_count = jnp.where(is_text, inv[1][:, 0:1], inv[0][:, 0:1])
        d_probs = onehot * d_gate + global_part - logp * inv_count
        d_log = probs * (d_probs - jnp.sum(d_probs * probs, axis=0, keepdims=True))
        d_log_ref[:, lanes] = d_log
        d_router[...] += nn(jnp.concatenate(split3(d_log), axis=0), wbuf[3, 0:CHUNK, :])

        @pl.when(i + 1 < pieces)
        def _():
            for copy in token_loads(i + 1):
                copy.start()

    def rest(t, carry):
        def streams(s, inner):
            wave(t, s)

            @pl.when(s == 1)
            def _():
                combine(t - units)

            return inner

        return lax.fori_loop(0, 4, streams, carry)

    first = units + pieces
    lax.fori_loop(units, first, rest, 0)
    out_store(jnp.int32(pieces - 1)).wait()
    small_work[0, 0:experts, :] = d_router[0:experts] + d_router[experts:2 * experts] + d_router[2 * experts:]

    def tail(t, carry):
        def streams(s, inner):
            wave(t, s)
            return inner

        return lax.fori_loop(0, 4, streams, carry)

    small_step(0)
    for k in range(1, 4):
        lax.fori_loop(first + k - 1, first + k, tail, 0)
        small_step(k)
    lax.fori_loop(first + 3, units + 12, tail, 0)
    small_step(4, small_ref)

    def drain(tile, carry):
        for k in range(12):
            act_on(tile, k, lambda copy: copy.wait_send())
        return carry

    lax.fori_loop(0, tiles, drain, 0)
    for s in range(3):
        for j in range(others):
            d_copy(j, s).wait_send()
    for copy in send_y:
        copy.wait_send()
    for copy in send_g:
        copy.wait()
    self_g.wait()
    for i in range(late.shape[0]):
        keep_late(jnp.int32(late_from + i)).wait()


def global_terms(stats, experts):
    loss = jnp.zeros((1, 128), F32)
    terms = []
    inv = []
    for m in range(2):
        base = 24 * m
        count = stats[base + 16:base + 17]
        mean = stats[base:base + 8] / count
        log_mean = jnp.log(mean)
        loss = loss + stats[base + 8:base + 9] / count + jnp.sum(mean * log_mean, axis=0, keepdims=True)
        terms.append(log_mean / count)
        inv.append(1.0 / count)
    return loss, terms, inv


def final_kernel(slot_ref, d_log_ref, back_any, router_ref, small_ref, loss_ref, summed, out_any,
                 dx, dw_in, dw_out, out, d_router_ref, db_in_ref, db_out_ref, aux_ref,
                 buf, back, out_buf, dx_buf, load_sem, store_sem, back_sem, out_sem, dx_sem):
    n, width = dx.shape
    tiles = buf.shape[0]
    half = tiles // 2
    units = tiles // 4
    experts = d_log_ref.shape[0]
    pieces = n // CHUNK

    load_back = pltpu.make_async_copy(back_any, back, back_sem)
    load_back.start()

    def loads(t):
        return [
            pltpu.make_async_copy(summed.at[t, :, :, :, pl.ds(j * TILE, TILE)], buf.at[t, :, :, j], load_sem.at[t, j])
            for j in range(3)
        ]

    def store(t):
        tile = buf.at[t].reshape(width, TILE)
        if t < half:
            unit, stream = t // 4, t % 4
            dst = dw_out.at[pl.ds(stream * width, width), pl.ds(unit * TILE, TILE)]
        else:
            dst = dw_in.at[:, pl.ds((t - half) * TILE, TILE)]
        return pltpu.make_async_copy(tile, dst, store_sem.at[t])

    for t in range(tiles):
        for copy in loads(t):
            copy.start()
    load_out = pltpu.make_async_copy(out_any, out_buf, out_sem.at[0])
    load_out.start()

    d_router_ref[...] = small_ref[0:experts, :]
    for i in range(4):
        db_in_ref[:, i * width:(i + 1) * width] = small_ref[8 + i:9 + i, :].astype(BF16)
    db_out_ref[...] = small_ref[12:13, :].astype(BF16)
    aux_ref[0, 0] = loss_ref[0, 0]
    r = split3(router_ref[...])
    rights = jnp.concatenate([r[0], r[1], r[0], r[1], r[2], r[0]], axis=0)
    load_back.wait()

    def dx_store(i):
        at = pl.ds(i * CHUNK, CHUNK)
        return pltpu.make_async_copy(dx_buf.at[at], dx.at[at], dx_sem.at[i])

    per_piece = tiles // pieces
    for i in range(pieces):
        lanes = pl.ds(i * CHUNK, CHUNK)
        d = split3(d_log_ref[:, lanes])
        lefts = jnp.concatenate([d[0], d[0], d[1], d[1], d[0], d[2]], axis=0)
        routed = tn(lefts, rights).astype(BF16)
        slot_col = col_of(slot_ref[0:1, lanes])[:, 0:1]
        chosen = (lax.broadcasted_iota(jnp.int32, (CHUNK, n), 1).astype(F32) == slot_col).astype(BF16)
        dx_buf[lanes, :] = (nn(chosen, back[...]) + routed.astype(F32)).astype(BF16)
        dx_store(i).start()
        for t in range(i * per_piece, (i + 1) * per_piece):
            for copy in loads(t):
                copy.wait()
            store(t).start()
    load_out.wait()
    store_out = pltpu.make_async_copy(out_buf, out, out_sem.at[1])
    store_out.start()
    for t in range(tiles):
        store(t).wait()
    for i in range(pieces):
        dx_store(i).wait()
    store_out.wait()


def vmem(count):
    return [pl.BlockSpec(memory_space=pltpu.VMEM)] * count


def cost(flops, size):
    return pl.CostEstimate(flops=int(flops), bytes_accessed=int(size), transcendentals=0)


def solution(mesh):
    token_spec = P(ALL_AXES)
    expert_spec = P("ep")

    def local_step(x, modality, router, expert_ids, priority, w_in, b_in, w_out, b_out, dy):
        n, width = x.shape
        experts = router.shape[1]
        hid = w_in.shape[2]
        capacity = n // experts
        tiles = hid // TILE
        share = n // (experts // 2)
        w_in, w_out = w_in[0], w_out[0]
        ids, prio, mod = (a.reshape(n // 128, 128) for a in (expert_ids, priority, modality))
        router_t = jnp.transpose(router)
        shape = jax.ShapeDtypeStruct
        anywhere = pl.BlockSpec(memory_space=pl.ANY)
        dma = pltpu.SemaphoreType.DMA
        slots = (experts, capacity, width)
        mm = 2 * n * width * hid
        others = experts - 1

        summed, back_y, d_back, out, _, _, slot, d_log, loss, small = pl.pallas_call(
            block_kernel,
            out_shape=(
                shape((2 * tiles, 4, 4, 16, width), BF16), shape(slots, BF16), shape(slots, BF16), shape((n, width), BF16),
                shape((n // WIDE, hid, WIDE), BF16), shape((hid // WIDE, n // 16, 16, WIDE), F32),
                shape((8, n), F32), shape((experts, n), F32), shape((8, 128), F32), shape((16, width), F32),
            ),
            in_specs=vmem(3) + [anywhere] * 2 + vmem(1) + [anywhere] + vmem(1) + [anywhere] + vmem(1),
            out_specs=(*[anywhere] * 6, *vmem(4)),
            scratch_shapes=[
                pltpu.VMEM((2 * tiles, 4, 4, 16, width), F32),
                pltpu.VMEM((tiles, 3, 4, 16, width), F32),
                pltpu.VMEM((tiles, 3, 16, width), F32),
                pltpu.VMEM((2 * tiles, 16, width), BF16),
                pltpu.VMEM((n, width), BF16),
                pltpu.VMEM((n, width), BF16),
                pltpu.VMEM(slots, BF16),
                pltpu.VMEM(slots, BF16),
                pltpu.VMEM((width, n), BF16),
                pltpu.VMEM((n, width), BF16),
                pltpu.VMEM((n, width), F32),
                pltpu.VMEM((4, WIDE, WIDE), BF16),
                pltpu.VMEM((2, n // 16, 16, TILE), F32),
                pltpu.VMEM((n, TILE), BF16),
                pltpu.VMEM((2, WIDE, share), BF16),
                pltpu.VMEM((CHUNK, width), BF16),
                pltpu.VMEM((4, 4, 4, 16, width), BF16),
                pltpu.VMEM((n, 8), F32),
                pltpu.VMEM((8, n), F32),
                pltpu.VMEM((8, n), F32),
                pltpu.VMEM((experts, n), F32),
                pltpu.VMEM((1, hid), F32),
                pltpu.VMEM((48, 128), F32),
                pltpu.VMEM((3 * experts, width), F32),
                pltpu.VMEM((4, 48, 128), F32), pltpu.VMEM((4, 4, 48, 128), F32),
                pltpu.VMEM((4, 16, width), F32), pltpu.VMEM((4, 4, 16, width), F32),
                dma((2 * tiles, 12)), dma((2 * tiles, 12)), dma((2 * tiles,)), pltpu.SemaphoreType.REGULAR((tiles, 6)),
                dma((others,)), dma((others,)), dma((others, 3)), dma((others, 3)),
                dma((others,)), dma((others,)), dma((others,)), dma((others,)),
                dma((2,)), dma((2,)), dma, dma((2,)), dma((2,)), dma((3,)), dma((2,)), dma((4,)), dma((2,)), dma((4,)),
                dma((4, 3)), dma((4, 3)), dma((4, 3)), dma((4, 3)),
            ],
            compiler_params=pltpu.CompilerParams(collective_id=1, has_side_effects=True, vmem_limit_bytes=67_000_000),
            cost_estimate=cost(6 * mm, 6 * n * hid), name="block",
        )(ids, prio, mod, x, dy, router_t, w_in, b_in, w_out, b_out)

        d_x, d_w_in, d_w_out, out, d_router, d_b_in, d_b_out, aux = pl.pallas_call(
            final_kernel,
            out_shape=(
                shape((n, width), BF16), shape((width, hid), BF16), shape((hid, width), BF16), shape((n, width), BF16),
                shape((experts, width), F32), shape((1, hid), BF16), shape((1, width), BF16), shape((1, 1), F32),
            ),
            in_specs=vmem(2) + [anywhere] + vmem(3) + [anywhere] * 2,
            out_specs=(*[anywhere] * 4, *vmem(3), pl.BlockSpec(memory_space=pltpu.SMEM)),
            scratch_shapes=[
                pltpu.VMEM((2 * tiles, 4, 4, 3, 16, TILE), BF16),
                pltpu.VMEM((n, width), BF16), pltpu.VMEM((n, width), BF16), pltpu.VMEM((n, width), BF16),
                dma((2 * tiles, 3)), dma((2 * tiles,)), dma, dma((2,)), dma((n // CHUNK,)),
            ],
            compiler_params=pltpu.CompilerParams(vmem_limit_bytes=66_000_000),
            cost_estimate=cost(2 * n * n * width, 8 * width * hid), name="final",
        )(slot, d_log, d_back.reshape(n, width), router_t, small, loss, summed, out)
        return out, aux[0, 0], d_x, jnp.transpose(d_router), d_w_in[None], d_b_in, d_w_out[None], d_b_out

    return jax.shard_map(
        local_step,
        mesh=mesh,
        in_specs=(token_spec, token_spec, P(), token_spec, token_spec, expert_spec, expert_spec, expert_spec, expert_spec, token_spec),
        out_specs=(token_spec, P(), token_spec, P(), expert_spec, expert_spec, expert_spec, expert_spec),
        check_vma=False,
    )
```

```python
import functools

import jax
import jax.numpy as jnp
from jax import lax
from jax.experimental import pallas as pl
from jax.experimental.pallas import tpu as pltpu
from jax.sharding import PartitionSpec as P

ALL_AXES = ("dp", "ep")
MESH = pl.DeviceIdType.MESH
F32 = jnp.float32
BF16 = jnp.bfloat16
NOWHERE = -1.0
TILE = 256
CHUNK = 256
WIDE = 768


def col_of(row):
    return jnp.transpose(jnp.broadcast_to(row, (8, row.shape[1])))


def row_of(col):
    return jnp.transpose(jnp.broadcast_to(col, (col.shape[0], 8)))


def split3(a):
    hi = a.astype(BF16)
    rest = a - hi.astype(F32)
    mid = rest.astype(BF16)
    lo = (rest - mid.astype(F32)).astype(BF16)
    return hi, mid, lo


def nt(a, b):
    return lax.dot_general(a, b, (((1,), (1,)), ((), ())), preferred_element_type=F32)


def tn(a, b):
    return lax.dot_general(a, b, (((0,), (0,)), ((), ())), preferred_element_type=F32)


def nn(a, b):
    return jnp.dot(a, b, preferred_element_type=F32)


def wide(ref):
    v = ref[...].astype(F32)
    return jnp.concatenate([v[i:i + 1, :] for i in range(v.shape[0])], axis=1)


def greet(peers):
    barrier = pltpu.get_barrier_semaphore()
    for peer in peers:
        pl.semaphore_signal(barrier, inc=1, device_id=peer, device_id_type=MESH)
    return lambda: pl.semaphore_wait(barrier, len(peers))


ROOT = 0.7978845608028654
CUBIC = 0.044715


def block_kernel(
    ids_ref, prio_ref, mod_ref, x_any, dy_any, router_ref, w_in, b_in_ref, w_out, b_out_ref,
    summed, back_y, back_d, out, hidden_t, pre_act, slot_row, d_log_ref, loss_ref, small_ref,
    part_sum, land_a, land_b, own, x_buf, dy_buf, out_x, rows, rows_t, tok, acc, wbuf, sbuf, act, hbuf, stage, late,
    keycol, ids_row, mod_row, logp_ref, db_in, stats_ref, d_router, stat_work, stat_bufs, small_work, small_bufs,
    send_sem, sum_sem, recv_sem, own_sem, credit, x_send, x_recv, d_send, d_recv, y_send, y_recv, g_send, g_recv,
    self_sem, tok_sem, out_sem, i_sem, o_sem, a_sem, h_sem, hid_sem, s_sem, late_sem, stat_send, stat_recv,
):
    dp = lax.axis_index("dp")
    ep = lax.axis_index("ep")
    z, yy = dp // 4, lax.rem(dp, 4)
    xx, core = ep // 2, lax.rem(ep, 2)
    tiles = part_sum.shape[0]
    units = tiles // 4
    half = tiles // 2
    experts, capacity, width = out_x.shape
    n = experts * capacity
    pairs = experts // 2
    share = n // pairs
    fwd_tiles = hidden_t.shape[1] // WIDE
    steps = pairs * fwd_tiles
    groups = part_sum.reshape(tiles * 16, 16, width)
    late_from = tiles - late.shape[0]
    others = experts - 1
    out_d = x_buf.reshape(out_x.shape)
    tok_slots = tok.reshape(out_x.shape)

    def wrap(v):
        return lax.rem(v + 16, 4)

    peers = [(z * 4 + wrap(yy + j), ep) for j in range(1, 4)] + [(wrap(z + j) * 4 + yy, ep) for j in range(1, 4)]
    enter = greet(peers + [(dp, lax.rem(ep + j, experts)) for j in range(1, experts)])
    load_x = pltpu.make_async_copy(x_any, x_buf, tok_sem.at[0])
    load_dy = pltpu.make_async_copy(dy_any, dy_buf, tok_sem.at[1])
    load_x.start()
    load_dy.start()

    rings = (
        (yy, peers[0:3]),
        (z, peers[3:6]),
        None,
        (xx, [(dp, lax.rem(ep + 2 * j, experts)) for j in range(1, 4)]),
    )
    partner = (dp, xx * 2 + 1 - core)

    def small_sum(work, bufs, whole_rows, send_sems, recv_sems):
        head = pl.ds(0, whole_rows)
        full = pl.ds(0, work.shape[1])

        def pair():
            return pltpu.make_async_remote_copy(
                src_ref=work.at[2, head], dst_ref=bufs.at[2, 0, head], send_sem=send_sems.at[2, 0], recv_sem=recv_sems.at[2, 0],
                device_id=partner, device_id_type=MESH)

        def ring(axis):
            me, ring_peers = rings[axis]
            at = head if axis == 3 else full
            return [
                pltpu.make_async_remote_copy(
                    src_ref=work.at[axis, at], dst_ref=bufs.at[axis, me, at], send_sem=send_sems.at[axis, j],
                    recv_sem=recv_sems.at[axis, j], device_id=ring_peers[j], device_id_type=MESH)
                for j in range(3)
            ]

        def launch(axis):
            bufs[axis, rings[axis][0]] = work[axis]
            for copy in ring(axis):
                copy.start()

        def total(axis, at):
            for copy in ring(axis):
                copy.wait()
            return bufs[axis, 0, at, :] + bufs[axis, 1, at, :] + bufs[axis, 2, at, :] + bufs[axis, 3, at, :]

        def step(k, dst=None):
            if k == 0:
                launch(0)
            elif k == 1:
                work[1] = total(0, full)
                launch(1)
            elif k == 2:
                work[2] = total(1, full)
                pair().start()
            elif k == 3:
                pair().wait()
                work[3] = work[2]
                work[3, head, :] = work[2, head, :] + bufs[2, 0, head, :]
                launch(3)
            else:
                dst[...] = work[2]
                dst[head, :] = total(3, head)

        return step

    stat_step = small_sum(stat_work, stat_bufs, 48, stat_send, stat_recv)
    small_step = small_sum(small_work, small_bufs, experts, stat_send, stat_recv)

    ids = wide(ids_ref)
    key = ids * n + wide(prio_ref)
    low = ids * n
    keycol[...] = col_of(key)

    def count(j, total):
        col = keycol[pl.ds(pl.multiple_of(j * 128, 128), 128), :][:, 0:1]
        before = jnp.logical_and(col < key, col >= low)
        return total + jnp.sum(before.astype(F32), axis=0, keepdims=True)

    position = lax.fori_loop(0, n // 128, count, jnp.zeros((1, n), F32))
    slot = jnp.where(position < capacity, ids * capacity + position, NOWHERE)
    slot_row[...] = jnp.broadcast_to(slot, slot_row.shape)
    mod = wide(mod_ref)
    ids_row[...] = jnp.broadcast_to(ids, ids_row.shape)
    mod_row[...] = jnp.broadcast_to(mod, mod_row.shape)

    def hops(q):
        return q + q // 2 - 2 * (q // 3)

    def target(j):
        return wrap(xx + hops((j + 1) // 2)) * 2 + lax.rem(core + 1 - lax.rem(j, 2), 2)

    def pick(e):
        index = (lax.broadcasted_iota(jnp.int32, (capacity, n), 0) + e * capacity).astype(F32)
        return (index == slot_row[0:1, :]).astype(BF16)

    def x_copy(j):
        to = target(j)
        return pltpu.make_async_remote_copy(
            src_ref=out_x.at[to], dst_ref=rows.at[ep], send_sem=x_send, recv_sem=x_recv.at[j],
            device_id=(dp, to), device_id_type=MESH)

    def d_copy(j, s):
        to = target(j)
        at = pl.ds(pl.multiple_of(s * TILE, TILE), TILE)
        return pltpu.make_async_remote_copy(
            src_ref=out_d.at[to, :, at], dst_ref=tok_slots.at[ep, :, at], send_sem=d_send, recv_sem=d_recv.at[j, s],
            device_id=(dp, to), device_id_type=MESH)

    def load_i(it):
        slot = lax.rem(it, 2)
        at = pl.ds(pl.multiple_of(lax.rem(it, fwd_tiles) * WIDE, WIDE), WIDE)
        return pltpu.make_async_copy(w_in.at[:, at], wbuf.at[slot], i_sem.at[slot])

    def load_o(it):
        slot = lax.rem(it, 2)
        at = pl.ds(pl.multiple_of(lax.rem(it, fwd_tiles) * WIDE, WIDE), WIDE)
        return pltpu.make_async_copy(w_out.at[at], wbuf.at[2 + slot], o_sem.at[slot])

    def all_sent(sem):
        pltpu.make_async_copy(out_x.at[pl.ds(0, others)], out_x.at[pl.ds(0, others)], sem).wait()

    load_x.wait()
    enter()

    def send_x(j, carry):
        out_x[target(j)] = nn(pick(target(j)), x_buf[...]).astype(BF16)
        x_copy(j).start()
        return carry

    lax.fori_loop(0, others, send_x, 0)
    load_i(0).start()
    load_i(1).start()
    load_o(0).start()
    rows[ep] = nn(pick(ep), x_buf[...]).astype(BF16)

    router3 = jnp.concatenate(split3(router_ref[...]), axis=0)
    logits3 = nt(router3, x_buf[...])
    logits = logits3[0:experts] + logits3[experts:2 * experts] + logits3[2 * experts:3 * experts]
    shifted = logits - jnp.max(logits, axis=0, keepdims=True)
    logp = shifted - jnp.log(jnp.sum(jnp.exp(shifted), axis=0, keepdims=True))
    logp_ref[...] = logp
    probs = jnp.exp(logp)
    onehot = (lax.broadcasted_iota(jnp.int32, (experts, n), 0).astype(F32) == ids).astype(F32)
    gate = jnp.sum(probs * onehot, axis=0, keepdims=True)
    entropy = -jnp.sum(probs * logp, axis=0, keepdims=True)
    for m in range(2):
        mask = (mod == m).astype(F32)
        stat_work[0, 24 * m:24 * m + 8, :] = jnp.broadcast_to(jnp.sum(probs * mask, axis=1, keepdims=True), (8, 128))
        stat_work[0, 24 * m + 8:24 * m + 16, :] = jnp.broadcast_to(jnp.sum(entropy * mask, axis=1, keepdims=True), (8, 128))
        stat_work[0, 24 * m + 16:24 * m + 24, :] = jnp.broadcast_to(jnp.sum(mask, axis=1, keepdims=True), (8, 128))
    stat_step(0)
    load_dy.wait()
    dy_buf[...] = (col_of(gate)[:, 0:1] * dy_buf[...].astype(F32)).astype(BF16)

    def pick_cotangent(j, carry):
        out_d[target(j)] = nn(pick(target(j)), dy_buf[...]).astype(BF16)
        return carry

    lax.fori_loop(0, others, pick_cotangent, 0)
    tok_slots[ep] = nn(pick(ep), dy_buf[...]).astype(BF16)
    stat_step(1)
    acc[...] = jnp.broadcast_to(b_out_ref[...].astype(F32), acc.shape)
    small_work[0] = jnp.zeros(small_work.shape[1:], F32)

    def origin(it):
        return wrap(xx - hops(it // fwd_tiles))

    def store_a(it):
        slot = lax.rem(it, 3)
        at = pl.ds(pl.multiple_of(origin(it) * (share // 16), share // 16), share // 16)
        return pltpu.make_async_copy(
            groups.at[pl.ds(slot * (share // 16), share // 16)], pre_act.at[lax.rem(it, fwd_tiles), at], a_sem.at[slot])

    def store_h(it):
        slot = lax.rem(it, 2)
        down = pl.ds(pl.multiple_of(lax.rem(it, fwd_tiles) * WIDE, WIDE), WIDE)
        at = pl.ds(pl.multiple_of(lax.rem(origin(it), 2) * share, share), share)
        return pltpu.make_async_copy(hbuf.at[slot], hidden_t.at[origin(it) // 2, down, at], h_sem.at[slot])

    def first_matmul(it):
        at = pl.ds(pl.multiple_of(lax.rem(it, fwd_tiles) * WIDE, WIDE), WIDE)
        chunk = rows[pl.ds(origin(it) * 2, 2)].reshape(share, width)
        a = nn(chunk, wbuf[lax.rem(it, 2)]) + b_in_ref[:, at].astype(F32)
        groups[pl.ds(lax.rem(it, 3) * (share // 16), share // 16)] = a.reshape(share // 16, 16, WIDE)

    def rest_of_step(it):
        a = groups[pl.ds(lax.rem(it, 3) * (share // 16), share // 16)].reshape(share, WIDE)
        t = jnp.tanh(ROOT * (a + CUBIC * (a * a * a)))
        hidden = (a * (0.5 * (1.0 + t))).astype(BF16)
        hbuf[lax.rem(it, 2)] = jnp.transpose(hidden)
        at = pl.ds(pl.multiple_of(origin(it) * share, share), share)
        acc[at, :] += nn(hidden, wbuf[2 + lax.rem(it, 2)])

    def forward(it, carry):
        nxt = it + 1
        store_a(it).start()
        load_o(it).wait()
        load_o(nxt).start()

        @pl.when(lax.rem(nxt, fwd_tiles) == 0)
        def _():
            q = nxt // fwd_tiles
            x_copy(2 * q - 1).wait_recv()
            x_copy(2 * q).wait_recv()

        load_i(nxt).wait()

        @pl.when(nxt + 1 < steps)
        def _():
            load_i(nxt + 1).start()

        @pl.when(it >= 2)
        def _():
            store_a(it - 2).wait()
            store_h(it - 2).wait()

        rest_of_step(it)
        first_matmul(nxt)
        store_h(it).start()
        for k, when in ((2, 1), (3, 2)):
            @pl.when(it == when)
            def _():
                stat_step(k)

        @pl.when(it == 3)
        def _():
            for s in range(3):
                for j in range(others):
                    d_copy(j, s).start()

        return carry

    x_copy(0).wait_recv()
    load_i(0).wait()
    first_matmul(jnp.int32(0))
    lax.fori_loop(0, steps - 1, forward, 0)
    last = jnp.int32(steps - 1)
    store_a(last).start()
    load_o(last).wait()
    store_a(last - 2).wait()
    store_h(last - 2).wait()
    rest_of_step(last)
    store_h(last).start()

    def place(stream):
        way = 1 - 2 * lax.rem(stream, 2)
        first_z = stream // 2
        pa = yy * (1 - first_z) + z * first_z
        pb = z * (1 - first_z) + yy * first_z

        def along(move):
            on_y = z * 4 + wrap(yy + move)
            on_z = wrap(z + move) * 4 + yy
            return on_y * (1 - first_z) + on_z * first_z, on_z * (1 - first_z) + on_y * first_z

        return way, pa, pb, along(way), along(-way)

    def send(tile, k, end=False):
        way, pa, pb, (next_a, next_b), _ = place(lax.rem(tile, 4))
        whole = late.at[tile - late_from] if end else summed.at[tile]
        if k < 3:
            src, dst, to = part_sum.at[tile, wrap(pa - way * (k + 1))], land_a.at[lax.rem(tile, half), k], next_a
        elif k < 6:
            src, dst, to = part_sum.at[tile, pa, wrap(pb - way * (k - 2))], land_b.at[lax.rem(tile, half), k - 3], next_b
        elif k < 9:
            src = whole.at[pa, wrap(pb - way * (k - 6))]
            dst, to = src, next_b
            if k == 6 and not end:
                src = own.at[tile]
        else:
            src = whole.at[wrap(pa - way * (k - 9))]
            dst, to = src, next_a
        return pltpu.make_async_remote_copy(
            src_ref=src, dst_ref=dst, send_sem=send_sem.at[tile],
            recv_sem=sum_sem.at[lax.rem(tile, half), k] if k < 6 else recv_sem.at[tile, k - 6],
            device_id=(to, ep), device_id_type=MESH)

    def sent(tile):
        count = 3 * (5 * 16 + 5 * 8)
        return pltpu.make_async_copy(acc.at[pl.ds(0, count)], acc.at[pl.ds(count, count)], send_sem.at[tile])

    def act_on(tile, k, action):
        if k < 6:
            action(send(tile, k))
        else:
            @pl.when(tile < late_from)
            def _():
                action(send(tile, k))

            @pl.when(tile >= late_from)
            def _():
                action(send(tile, k, True))

    def start(tile, k):
        if k < 6:
            @pl.when(tile >= half)
            def _():
                pl.semaphore_wait(credit.at[tile - half, k // 3], 1)

        act_on(tile, k, lambda copy: copy.start())

    def keep(tile):
        way, pa, pb, _, _ = place(lax.rem(tile, 4))
        return pltpu.make_async_copy(own.at[tile], summed.at[tile, pa, pb], own_sem.at[lax.rem(tile, half)])

    def keep_late(tile):
        spot = tile - late_from
        return pltpu.make_async_copy(late.at[spot], summed.at[tile], late_sem.at[spot])

    def advance(tile, k):
        way, pa, pb, _, (prev_a, prev_b) = place(lax.rem(tile, 4))
        spot = lax.rem(tile, half)
        act_on(tile, k - 1, lambda copy: copy.wait_recv())
        if k <= 3:
            block = wrap(pa - way * (k + 1))
            part_sum[tile, block] = part_sum[tile, block] + land_a[spot, k - 1]
        elif k <= 6:
            block = wrap(pb - way * (k - 2))
            total = part_sum[tile, pa, block] + land_b[spot, k - 4]
            if k < 6:
                part_sum[tile, pa, block] = total
            else:
                @pl.when(tile < late_from)
                def _():
                    own[tile] = total.astype(BF16)
                    keep(tile).start()

                @pl.when(tile >= late_from)
                def _():
                    late[tile - late_from, pa, pb] = total.astype(BF16)
        elif k == 9:
            @pl.when(tile < late_from)
            def _():
                keep(tile).wait()
        elif k == 12:
            @pl.when(tile >= late_from)
            def _():
                keep_late(tile).start()
        if k <= 6:
            back_to = prev_a if k <= 3 else prev_b

            @pl.when(tile < half)
            def _():
                pl.semaphore_signal(credit.at[tile, (k - 1) // 3], inc=1, device_id=(back_to, ep), device_id_type=MESH)

        if k < 12:
            start(tile, k)

    def wave(t, ages):
        for k in ages:
            unit = t - k

            @pl.when(jnp.logical_and(unit >= 0, unit < units))
            def _():
                def streams(stream, carry):
                    advance(unit * 4 + stream, k)
                    return carry

                lax.fori_loop(0, 4, streams, 0)

    def quarter(t, stream):
        for p, ages in enumerate(((6, 5), (4, 3), (2,), (1,))):
            @pl.when(stream == p)
            def _():
                wave(t, ages)

    def exchange(src, dst, send_sems, recv_sems):
        copies = []
        for j in range(1, experts):
            to = lax.rem(ep + j, experts)
            copies.append(pltpu.make_async_remote_copy(
                src_ref=src.at[to], dst_ref=dst.at[ep], send_sem=send_sems, recv_sem=recv_sems.at[j - 1],
                device_id=(dp, to), device_id_type=MESH))
        return copies

    def place_tile(tile, a, grad):
        for b in range(4):
            for j in range(3):
                at = b * (width // 16) + j * 16
                part_sum[tile, a, b, :, j * TILE:(j + 1) * TILE] = grad[at:at + 16, :]

    def load_hid(i):
        base = 2 * lax.rem(i, 2)
        at = pl.ds(pl.multiple_of(lax.rem(i, 4) * WIDE, WIDE), WIDE)
        return [pltpu.make_async_copy(hidden_t.at[h, at], wbuf.at[base + h], hid_sem.at[base + h]) for h in range(2)]

    def load_rest(i):
        slot = lax.rem(i, 2)
        at = pl.ds(pl.multiple_of(i * TILE, TILE), TILE)
        lanes = pl.ds(pl.multiple_of(lax.rem(i, WIDE // TILE) * TILE, TILE), TILE)
        return (
            pltpu.make_async_copy(pre_act.at[i // (WIDE // TILE), :, :, lanes], sbuf.at[slot], s_sem.at[slot]),
            pltpu.make_async_copy(w_in.at[:, at], wbuf.at[slot, :, pl.ds(0, TILE)], i_sem.at[slot]),
            pltpu.make_async_copy(w_out.at[at], wbuf.at[2 + slot, pl.ds(0, TILE)], o_sem.at[slot]),
        )

    store_a(last - 1).wait()
    store_a(last).wait()
    store_h(last - 1).wait()
    store_h(last).wait()
    for copy in load_hid(jnp.int32(0)):
        copy.start()
    all_sent(x_send)
    out_x[...] = acc[...].astype(BF16).reshape(out_x.shape)

    def out_tile(i, carry):
        unit, stream = i // 4, lax.rem(i, 4)
        quarter(unit, stream)

        @pl.when(stream == 0)
        def _():
            for j in range(others):
                d_copy(j, unit).wait_recv()

        at = pl.ds(pl.multiple_of(unit * TILE, TILE), TILE)
        for copy in load_hid(i):
            copy.wait()

        @pl.when(i + 1 < half)
        def _():
            for copy in load_hid(i + 1):
                copy.start()

        base = 2 * lax.rem(i, 2)
        grad = nn(wbuf[base], tok[0:WIDE, at]) + nn(wbuf[base + 1], tok[WIDE:, at])
        for a in range(4):
            place_tile(i, a, grad[a * (width // 4):(a + 1) * (width // 4)])
        start(i, 0)
        return carry

    lax.fori_loop(0, half, out_tile, 0)
    for copy in load_rest(jnp.int32(0)):
        copy.start()
    stat_step(4, stats_ref)
    send_y = exchange(out_x, back_y, y_send, y_recv)
    for copy in send_y:
        copy.start()
    self_y = pltpu.make_async_copy(out_x.at[ep], back_y.at[ep], self_sem.at[0])
    self_y.start()
    small_work[0, 12:13, :] = jnp.sum(tok[...].astype(F32), axis=0, keepdims=True)
    rows_t[...] = jnp.transpose(rows[...].reshape(n, width))
    acc[...] = jnp.zeros_like(acc)
    chunks = 4
    size = n // chunks

    def in_tile(i, carry):
        g = i + half
        quarter(g // 4, lax.rem(g, 4))
        slot = lax.rem(i, 2)
        for copy in load_rest(i):
            copy.wait()

        @pl.when(i + 1 < half)
        def _():
            for copy in load_rest(i + 1):
                copy.start()

        total = jnp.zeros((1, TILE), F32)
        for c in range(chunks):
            part = pl.ds(c * size, size)
            d_hidden = nt(tok[part, :], wbuf[2 + slot, 0:TILE, :]).astype(BF16)
            a = sbuf[slot, c * (size // 16):(c + 1) * (size // 16)].reshape(size, TILE)
            sq = a * a
            t = jnp.tanh(ROOT * (a + CUBIC * (sq * a)))
            slope = 0.5 * (1.0 + t) + (0.5 * ROOT) * a * (1.0 - t * t) * (1.0 + (3 * CUBIC) * sq)
            d_act = d_hidden.astype(F32) * slope
            total += jnp.sum(d_act, axis=0, keepdims=True)
            d_act_bf = d_act.astype(BF16)
            act[part, :] = d_act_bf
            acc[part, :] += nt(d_act_bf, wbuf[slot, :, 0:TILE])
        db_in[:, pl.ds(pl.multiple_of(i * TILE, TILE), TILE)] = total
        grad = nn(rows_t[...], act[...])
        for a in range(4):
            place_tile(g, a, grad[a * (width // 4):(a + 1) * (width // 4)])
        start(g, 0)
        return carry

    lax.fori_loop(0, half, in_tile, 0)

    rows[...] = acc[...].astype(BF16).reshape(rows.shape)
    send_g = exchange(rows, back_d, g_send, g_recv)
    for copy in send_g:
        copy.start()
    self_g = pltpu.make_async_copy(rows.at[ep], back_d.at[ep], self_sem.at[1])
    self_g.start()

    for copy in send_y:
        copy.wait_recv()
    self_y.wait()
    back = pltpu.make_async_copy(back_y, dy_buf.reshape(back_y.shape), tok_sem.at[1])
    back.start()
    for i in range(4):
        small_work[0, 8 + i:9 + i, :] = db_in[:, i * width:(i + 1) * width]
    d_router[...] = jnp.zeros_like(d_router)
    loss, terms, inv = global_terms(stats_ref[...], experts)
    loss_ref[...] = jnp.broadcast_to(loss, loss_ref.shape)

    def token_loads(i):
        at = pl.ds(pl.multiple_of(i * CHUNK, CHUNK), CHUNK)
        return (
            pltpu.make_async_copy(dy_any.at[at], wbuf.at[2, pl.ds(0, CHUNK)], o_sem.at[0]),
            pltpu.make_async_copy(x_any.at[at], wbuf.at[3, pl.ds(0, CHUNK)], o_sem.at[1]),
        )

    def out_store(i):
        at = pl.ds(pl.multiple_of(i * CHUNK, CHUNK), CHUNK)
        return pltpu.make_async_copy(stage, out.at[at], out_sem)

    for copy in token_loads(jnp.int32(0)):
        copy.start()
    back.wait()
    pieces = n // CHUNK

    def combine(i):
        lanes = pl.ds(pl.multiple_of(i * CHUNK, CHUNK), CHUNK)
        slot_col = col_of(slot_row[0:1, lanes])[:, 0:1]
        chosen = (lax.broadcasted_iota(jnp.int32, (CHUNK, n), 1).astype(F32) == slot_col).astype(BF16)
        y_tok = nn(chosen, dy_buf[...])
        logp = logp_ref[:, lanes]
        probs = jnp.exp(logp)
        onehot = (lax.broadcasted_iota(jnp.int32, (experts, CHUNK), 0).astype(F32) == ids_row[:, lanes]).astype(F32)
        gate = jnp.sum(probs * onehot, axis=0, keepdims=True)
        for copy in token_loads(i):
            copy.wait()

        @pl.when(i > 0)
        def _():
            out_store(i - 1).wait()

        stage[...] = (col_of(gate)[:, 0:1] * y_tok).astype(BF16)
        out_store(i).start()
        d_gate = row_of(jnp.sum(wbuf[2, 0:CHUNK, :].astype(F32) * y_tok, axis=1, keepdims=True))[0:1]
        is_text = mod_row[:, lanes] == 1.0
        global_part = jnp.where(is_text, terms[1][:, 0:1], terms[0][:, 0:1])
        inv_count = jnp.where(is_text, inv[1][:, 0:1], inv[0][:, 0:1])
        d_probs = onehot * d_gate + global_part - logp * inv_count
        d_log = probs * (d_probs - jnp.sum(d_probs * probs, axis=0, keepdims=True))
        d_log_ref[:, lanes] = d_log
        d_router[...] += nn(jnp.concatenate(split3(d_log), axis=0), wbuf[3, 0:CHUNK, :])

        @pl.when(i + 1 < pieces)
        def _():
            for copy in token_loads(i + 1):
                copy.start()

    def rest(t, carry):
        wave(t, range(12, 4, -1))
        combine(t - units)
        wave(t, range(4, 0, -1))
        return carry

    first = units + pieces
    lax.fori_loop(units, first, rest, 0)
    out_store(jnp.int32(pieces - 1)).wait()
    small_work[0, 0:experts, :] = d_router[0:experts] + d_router[experts:2 * experts] + d_router[2 * experts:]

    small_step(0)
    for k in range(1, 5):
        wave(first + k - 1, range(12, 8, -1))
        small_step(k, small_ref)
        wave(first + k - 1, range(8, 0, -1))

    def tail(t, carry):
        wave(t, range(12, 0, -1))
        return carry

    lax.fori_loop(first + 4, units + 12, tail, 0)

    def drain(tile, carry):
        sent(tile).wait()
        return carry

    lax.fori_loop(0, tiles, drain, 0)
    for sem in (d_send, y_send, g_send):
        all_sent(sem)
    for copy in send_g:
        copy.wait_recv()
    self_g.wait()
    for i in range(late.shape[0]):
        keep_late(jnp.int32(late_from + i)).wait()


def global_terms(stats, experts):
    loss = jnp.zeros((1, 128), F32)
    terms = []
    inv = []
    for m in range(2):
        base = 24 * m
        count = stats[base + 16:base + 17]
        mean = stats[base:base + 8] / count
        log_mean = jnp.log(mean)
        loss = loss + stats[base + 8:base + 9] / count + jnp.sum(mean * log_mean, axis=0, keepdims=True)
        terms.append(log_mean / count)
        inv.append(1.0 / count)
    return loss, terms, inv


def final_kernel(slot_ref, d_log_ref, back_any, router_ref, small_ref, loss_ref, summed, out_any,
                 dx, dw_in, dw_out, out, d_router_ref, db_in_ref, db_out_ref, aux_ref,
                 buf, back, out_buf, dx_buf, load_sem, store_sem, back_sem, out_sem, dx_sem):
    n, width = dx.shape
    tiles = buf.shape[0]
    half = tiles // 2
    units = tiles // 4
    experts = d_log_ref.shape[0]
    pieces = n // CHUNK
    per_piece = tiles // pieces

    load_back = pltpu.make_async_copy(back_any, back, back_sem)

    def loads(t):
        return [
            pltpu.make_async_copy(summed.at[t, :, :, :, pl.ds(j * TILE, TILE)], buf.at[t, :, :, j], load_sem.at[t])
            for j in range(3)
        ]

    def store(t):
        tile = buf.at[t].reshape(width, TILE)
        if t < half:
            unit, stream = t // 4, t % 4
            dst = dw_out.at[pl.ds(stream * width, width), pl.ds(unit * TILE, TILE)]
        else:
            dst = dw_in.at[:, pl.ds((t - half) * TILE, TILE)]
        return pltpu.make_async_copy(tile, dst, store_sem.at[t])

    for t in range(tiles):
        if t == per_piece:
            load_back.start()
        for copy in loads(t):
            copy.start()
    load_out = pltpu.make_async_copy(out_any, out_buf, out_sem.at[0])
    load_out.start()

    d_router_ref[...] = small_ref[0:experts, :]
    for i in range(4):
        db_in_ref[:, i * width:(i + 1) * width] = small_ref[8 + i:9 + i, :].astype(BF16)
    db_out_ref[...] = small_ref[12:13, :].astype(BF16)
    aux_ref[0, 0] = loss_ref[0, 0]
    r = split3(router_ref[...])
    rights = jnp.concatenate([r[0], r[1], r[0], r[1], r[2], r[0]], axis=0)

    def dx_store(i):
        at = pl.ds(i * CHUNK, CHUNK)
        return pltpu.make_async_copy(dx_buf.at[at], dx.at[at], dx_sem.at[i])

    def move(i):
        for t in range(i * per_piece, (i + 1) * per_piece):
            pltpu.make_async_copy(buf.at[t], buf.at[t], load_sem.at[t]).wait()
            store(t).start()

    move(0)
    load_back.wait()
    for i in range(pieces):
        lanes = pl.ds(i * CHUNK, CHUNK)
        d = split3(d_log_ref[:, lanes])
        lefts = jnp.concatenate([d[0], d[0], d[1], d[1], d[0], d[2]], axis=0)
        routed = tn(lefts, rights).astype(BF16)
        slot_col = col_of(slot_ref[0:1, lanes])[:, 0:1]
        chosen = (lax.broadcasted_iota(jnp.int32, (CHUNK, n), 1).astype(F32) == slot_col).astype(BF16)
        dx_buf[lanes, :] = (nn(chosen, back[...]) + routed.astype(F32)).astype(BF16)
        dx_store(i).start()
        for piece in (2 * i + 1, 2 * i + 2):
            if piece < pieces:
                move(piece)
    load_out.wait()
    store_out = pltpu.make_async_copy(out_buf, out, out_sem.at[1])
    store_out.start()
    for t in range(tiles):
        store(t).wait()
    for i in range(pieces):
        dx_store(i).wait()
    store_out.wait()


def vmem(count):
    return [pl.BlockSpec(memory_space=pltpu.VMEM)] * count


def cost(flops, size):
    return pl.CostEstimate(flops=int(flops), bytes_accessed=int(size), transcendentals=0)


def solution(mesh):
    token_spec = P(ALL_AXES)
    expert_spec = P("ep")

    def local_step(x, modality, router, expert_ids, priority, w_in, b_in, w_out, b_out, dy):
        n, width = x.shape
        experts = router.shape[1]
        hid = w_in.shape[2]
        capacity = n // experts
        tiles = hid // TILE
        share = n // (experts // 2)
        w_in, w_out = w_in[0], w_out[0]
        ids, prio, mod = (a.reshape(n // 128, 128) for a in (expert_ids, priority, modality))
        router_t = jnp.transpose(router)
        shape = jax.ShapeDtypeStruct
        anywhere = pl.BlockSpec(memory_space=pl.ANY)
        dma = pltpu.SemaphoreType.DMA
        slots = (experts, capacity, width)
        mm = 2 * n * width * hid
        others = experts - 1

        summed, back_y, d_back, out, _, _, slot, d_log, loss, small = pl.pallas_call(
            block_kernel,
            out_shape=(
                shape((2 * tiles, 4, 4, 16, width), BF16), shape(slots, BF16), shape(slots, BF16), shape((n, width), BF16),
                shape((n // WIDE, hid, WIDE), BF16), shape((hid // WIDE, n // 16, 16, WIDE), F32),
                shape((8, n), F32), shape((experts, n), F32), shape((8, 128), F32), shape((16, width), F32),
            ),
            in_specs=vmem(3) + [anywhere] * 2 + vmem(1) + [anywhere] + vmem(1) + [anywhere] + vmem(1),
            out_specs=(*[anywhere] * 6, *vmem(4)),
            scratch_shapes=[
                pltpu.VMEM((2 * tiles, 4, 4, 16, width), F32),
                pltpu.VMEM((tiles, 3, 4, 16, width), F32),
                pltpu.VMEM((tiles, 3, 16, width), F32),
                pltpu.VMEM((2 * tiles, 16, width), BF16),
                pltpu.VMEM((n, width), BF16),
                pltpu.VMEM((n, width), BF16),
                pltpu.VMEM(slots, BF16),
                pltpu.VMEM(slots, BF16),
                pltpu.VMEM((width, n), BF16),
                pltpu.VMEM((n, width), BF16),
                pltpu.VMEM((n, width), F32),
                pltpu.VMEM((4, WIDE, WIDE), BF16),
                pltpu.VMEM((2, n // 16, 16, TILE), F32),
                pltpu.VMEM((n, TILE), BF16),
                pltpu.VMEM((2, WIDE, share), BF16),
                pltpu.VMEM((CHUNK, width), BF16),
                pltpu.VMEM((4, 4, 4, 16, width), BF16),
                pltpu.VMEM((n, 8), F32),
                pltpu.VMEM((8, n), F32),
                pltpu.VMEM((8, n), F32),
                pltpu.VMEM((experts, n), F32),
                pltpu.VMEM((1, hid), F32),
                pltpu.VMEM((48, 128), F32),
                pltpu.VMEM((3 * experts, width), F32),
                pltpu.VMEM((4, 48, 128), F32), pltpu.VMEM((4, 4, 48, 128), F32),
                pltpu.VMEM((4, 16, width), F32), pltpu.VMEM((4, 4, 16, width), F32),
                dma((2 * tiles,)), dma((tiles, 6)), dma((2 * tiles, 6)), dma((tiles,)), pltpu.SemaphoreType.REGULAR((tiles, 2)),
                dma, dma((others,)), dma, dma((others, 3)), dma, dma((others,)), dma, dma((others,)),
                dma((2,)), dma((2,)), dma, dma((2,)), dma((2,)), dma((3,)), dma((2,)), dma((4,)), dma((2,)), dma((4,)),
                dma((4, 3)), dma((4, 3)),
            ],
            compiler_params=pltpu.CompilerParams(collective_id=1, has_side_effects=True, vmem_limit_bytes=67_000_000),
            cost_estimate=cost(6 * mm, 6 * n * hid), name="block",
        )(ids, prio, mod, x, dy, router_t, w_in, b_in, w_out, b_out)

        d_x, d_w_in, d_w_out, out, d_router, d_b_in, d_b_out, aux = pl.pallas_call(
            final_kernel,
            out_shape=(
                shape((n, width), BF16), shape((width, hid), BF16), shape((hid, width), BF16), shape((n, width), BF16),
                shape((experts, width), F32), shape((1, hid), BF16), shape((1, width), BF16), shape((1, 1), F32),
            ),
            in_specs=vmem(2) + [anywhere] + vmem(3) + [anywhere] * 2,
            out_specs=(*[anywhere] * 4, *vmem(3), pl.BlockSpec(memory_space=pltpu.SMEM)),
            scratch_shapes=[
                pltpu.VMEM((2 * tiles, 4, 4, 3, 16, TILE), BF16),
                pltpu.VMEM((n, width), BF16), pltpu.VMEM((n, width), BF16), pltpu.VMEM((n, width), BF16),
                dma((2 * tiles,)), dma((2 * tiles,)), dma, dma((2,)), dma((n // CHUNK,)),
            ],
            compiler_params=pltpu.CompilerParams(vmem_limit_bytes=66_000_000),
            cost_estimate=cost(2 * n * n * width, 8 * width * hid), name="final",
        )(slot, d_log, d_back.reshape(n, width), router_t, small, loss, summed, out)
        return out, aux[0, 0], d_x, jnp.transpose(d_router), d_w_in[None], d_b_in, d_w_out[None], d_b_out

    return jax.shard_map(
        local_step,
        mesh=mesh,
        in_specs=(token_spec, token_spec, P(), token_spec, token_spec, expert_spec, expert_spec, expert_spec, expert_spec, token_spec),
        out_specs=(token_spec, P(), token_spec, P(), expert_spec, expert_spec, expert_spec, expert_spec),
        check_vma=False,
    )
```

```python
import functools

import jax
import jax.numpy as jnp
from jax import lax
from jax.experimental import pallas as pl
from jax.experimental.pallas import tpu as pltpu
from jax.sharding import PartitionSpec as P

ALL_AXES = ("dp", "ep")
MESH = pl.DeviceIdType.MESH
F32 = jnp.float32
BF16 = jnp.bfloat16
NOWHERE = -1.0
TILE = 256
CHUNK = 256
WIDE = 768


def col_of(row):
    return jnp.transpose(jnp.broadcast_to(row, (8, row.shape[1])))


def row_of(col):
    return jnp.transpose(jnp.broadcast_to(col, (col.shape[0], 8)))


def split3(a):
    hi = a.astype(BF16)
    rest = a - hi.astype(F32)
    mid = rest.astype(BF16)
    lo = (rest - mid.astype(F32)).astype(BF16)
    return hi, mid, lo


def nt(a, b):
    return lax.dot_general(a, b, (((1,), (1,)), ((), ())), preferred_element_type=F32)


def tn(a, b):
    return lax.dot_general(a, b, (((0,), (0,)), ((), ())), preferred_element_type=F32)


def nn(a, b):
    return jnp.dot(a, b, preferred_element_type=F32)


def wide(ref):
    v = ref[...].astype(F32)
    return jnp.concatenate([v[i:i + 1, :] for i in range(v.shape[0])], axis=1)


def greet(peers):
    barrier = pltpu.get_barrier_semaphore()
    for peer in peers:
        pl.semaphore_signal(barrier, inc=1, device_id=peer, device_id_type=MESH)
    return lambda: pl.semaphore_wait(barrier, len(peers))


ROOT = 0.7978845608028654
CUBIC = 0.044715


def block_kernel(
    ids_ref, prio_ref, mod_ref, x_any, dy_any, router_ref, w_in, b_in_ref, w_out, b_out_ref,
    summed, back_y, back_d, out, hidden_t, pre_act, slot_row, d_log_ref, loss_ref, small_ref,
    part_sum, land_a, land_b, own, x_buf, dy_buf, out_x, rows, rows_t, tok, acc, wbuf, sbuf, act, hbuf, stage, late,
    keycol, ids_row, mod_row, logp_ref, db_in, stats_ref, d_router, stat_work, stat_bufs, small_work, small_bufs,
    send_sem, sum_sem, recv_sem, own_sem, credit, x_send, x_recv, d_send, d_recv, y_send, y_recv, g_send, g_recv,
    self_sem, tok_sem, out_sem, i_sem, o_sem, a_sem, h_sem, hid_sem, s_sem, late_sem, stat_send, stat_recv,
):
    dp = lax.axis_index("dp")
    ep = lax.axis_index("ep")
    z, yy = dp // 4, lax.rem(dp, 4)
    xx, core = ep // 2, lax.rem(ep, 2)
    tiles = part_sum.shape[0]
    units = tiles // 4
    half = tiles // 2
    experts, capacity, width = out_x.shape
    n = experts * capacity
    pairs = experts // 2
    share = n // pairs
    fwd_tiles = hidden_t.shape[1] // WIDE
    steps = pairs * fwd_tiles
    groups = part_sum.reshape(tiles * 16, 16, width)
    late_from = tiles - late.shape[0]
    others = experts - 1
    out_d = x_buf.reshape(out_x.shape)
    tok_slots = tok.reshape(out_x.shape)

    def wrap(v):
        return lax.rem(v + 16, 4)

    peers = [(z * 4 + wrap(yy + j), ep) for j in range(1, 4)] + [(wrap(z + j) * 4 + yy, ep) for j in range(1, 4)]
    enter = greet(peers + [(dp, lax.rem(ep + j, experts)) for j in range(1, experts)])
    load_x = pltpu.make_async_copy(x_any, x_buf, tok_sem.at[0])
    load_dy = pltpu.make_async_copy(dy_any, dy_buf, tok_sem.at[1])
    load_x.start()
    load_dy.start()

    rings = (
        (yy, peers[0:3]),
        (z, peers[3:6]),
        None,
        (xx, [(dp, lax.rem(ep + 2 * j, experts)) for j in range(1, 4)]),
    )
    partner = (dp, xx * 2 + 1 - core)

    def small_sum(work, bufs, whole_rows, send_sems, recv_sems):
        head = pl.ds(0, whole_rows)
        full = pl.ds(0, work.shape[1])

        def pair():
            return pltpu.make_async_remote_copy(
                src_ref=work.at[2, head], dst_ref=bufs.at[2, 0, head], send_sem=send_sems.at[2, 0], recv_sem=recv_sems.at[2, 0],
                device_id=partner, device_id_type=MESH)

        def ring(axis):
            me, ring_peers = rings[axis]
            at = head if axis == 3 else full
            return [
                pltpu.make_async_remote_copy(
                    src_ref=work.at[axis, at], dst_ref=bufs.at[axis, me, at], send_sem=send_sems.at[axis, j],
                    recv_sem=recv_sems.at[axis, j], device_id=ring_peers[j], device_id_type=MESH)
                for j in range(3)
            ]

        def launch(axis):
            bufs[axis, rings[axis][0]] = work[axis]
            for copy in ring(axis):
                copy.start()

        def total(axis, at):
            for copy in ring(axis):
                copy.wait()
            return bufs[axis, 0, at, :] + bufs[axis, 1, at, :] + bufs[axis, 2, at, :] + bufs[axis, 3, at, :]

        def step(k, dst=None):
            if k == 0:
                launch(0)
            elif k == 1:
                work[1] = total(0, full)
                launch(1)
            elif k == 2:
                work[2] = total(1, full)
                pair().start()
            elif k == 3:
                pair().wait()
                work[3] = work[2]
                work[3, head, :] = work[2, head, :] + bufs[2, 0, head, :]
                launch(3)
            else:
                dst[...] = work[2]
                dst[head, :] = total(3, head)

        return step

    stat_step = small_sum(stat_work, stat_bufs, 48, stat_send, stat_recv)
    small_step = small_sum(small_work, small_bufs, experts, stat_send, stat_recv)

    ids = wide(ids_ref)
    key = ids * n + wide(prio_ref)
    low = ids * n
    keycol[...] = col_of(key)

    def count(j, total):
        col = keycol[pl.ds(pl.multiple_of(j * 128, 128), 128), :][:, 0:1]
        before = jnp.logical_and(col < key, col >= low)
        return total + jnp.sum(before.astype(F32), axis=0, keepdims=True)

    position = lax.fori_loop(0, n // 128, count, jnp.zeros((1, n), F32))
    slot = jnp.where(position < capacity, ids * capacity + position, NOWHERE)
    slot_row[...] = jnp.broadcast_to(slot, slot_row.shape)
    mod = wide(mod_ref)
    ids_row[...] = jnp.broadcast_to(ids, ids_row.shape)
    mod_row[...] = jnp.broadcast_to(mod, mod_row.shape)

    def hops(q):
        return q + q // 2 - 2 * (q // 3)

    def target(j):
        return wrap(xx + hops((j + 1) // 2)) * 2 + lax.rem(core + 1 - lax.rem(j, 2), 2)

    def pick(e):
        index = (lax.broadcasted_iota(jnp.int32, (capacity, n), 0) + e * capacity).astype(F32)
        return (index == slot_row[0:1, :]).astype(BF16)

    def x_copy(j):
        to = target(j)
        return pltpu.make_async_remote_copy(
            src_ref=out_x.at[to], dst_ref=rows.at[ep], send_sem=x_send, recv_sem=x_recv.at[j],
            device_id=(dp, to), device_id_type=MESH)

    def d_copy(j, s):
        to = target(j)
        at = pl.ds(pl.multiple_of(s * TILE, TILE), TILE)
        return pltpu.make_async_remote_copy(
            src_ref=out_d.at[to, :, at], dst_ref=tok_slots.at[ep, :, at], send_sem=d_send, recv_sem=d_recv.at[j, s],
            device_id=(dp, to), device_id_type=MESH)

    def load_i(it):
        slot = lax.rem(it, 2)
        at = pl.ds(pl.multiple_of(lax.rem(it, fwd_tiles) * WIDE, WIDE), WIDE)
        return pltpu.make_async_copy(w_in.at[:, at], wbuf.at[slot], i_sem.at[slot])

    def load_o(it):
        slot = lax.rem(it, 2)
        at = pl.ds(pl.multiple_of(lax.rem(it, fwd_tiles) * WIDE, WIDE), WIDE)
        return pltpu.make_async_copy(w_out.at[at], wbuf.at[2 + slot], o_sem.at[slot])

    def all_sent(sem):
        pltpu.make_async_copy(out_x.at[pl.ds(0, others)], out_x.at[pl.ds(0, others)], sem).wait()

    load_x.wait()
    enter()

    def send_x(j, carry):
        out_x[target(j)] = nn(pick(target(j)), x_buf[...]).astype(BF16)
        x_copy(j).start()
        return carry

    lax.fori_loop(0, others, send_x, 0)
    load_i(0).start()
    load_i(1).start()
    load_o(0).start()
    rows[ep] = nn(pick(ep), x_buf[...]).astype(BF16)

    router3 = jnp.concatenate(split3(router_ref[...]), axis=0)
    logits3 = nt(router3, x_buf[...])
    logits = logits3[0:experts] + logits3[experts:2 * experts] + logits3[2 * experts:3 * experts]
    shifted = logits - jnp.max(logits, axis=0, keepdims=True)
    logp = shifted - jnp.log(jnp.sum(jnp.exp(shifted), axis=0, keepdims=True))
    logp_ref[...] = logp
    probs = jnp.exp(logp)
    onehot = (lax.broadcasted_iota(jnp.int32, (experts, n), 0).astype(F32) == ids).astype(F32)
    gate = jnp.sum(probs * onehot, axis=0, keepdims=True)
    entropy = -jnp.sum(probs * logp, axis=0, keepdims=True)
    for m in range(2):
        mask = (mod == m).astype(F32)
        stat_work[0, 24 * m:24 * m + 8, :] = jnp.broadcast_to(jnp.sum(probs * mask, axis=1, keepdims=True), (8, 128))
        stat_work[0, 24 * m + 8:24 * m + 16, :] = jnp.broadcast_to(jnp.sum(entropy * mask, axis=1, keepdims=True), (8, 128))
        stat_work[0, 24 * m + 16:24 * m + 24, :] = jnp.broadcast_to(jnp.sum(mask, axis=1, keepdims=True), (8, 128))
    stat_step(0)
    load_dy.wait()
    dy_buf[...] = (col_of(gate)[:, 0:1] * dy_buf[...].astype(F32)).astype(BF16)

    def pick_cotangent(j, carry):
        out_d[target(j)] = nn(pick(target(j)), dy_buf[...]).astype(BF16)
        return carry

    lax.fori_loop(0, others, pick_cotangent, 0)
    tok_slots[ep] = nn(pick(ep), dy_buf[...]).astype(BF16)
    stat_step(1)
    acc[...] = jnp.broadcast_to(b_out_ref[...].astype(F32), acc.shape)
    small_work[0] = jnp.zeros(small_work.shape[1:], F32)

    def origin(it):
        return wrap(xx - hops(it // fwd_tiles))

    def store_a(it):
        slot = lax.rem(it, 3)
        at = pl.ds(pl.multiple_of(origin(it) * (share // 16), share // 16), share // 16)
        return pltpu.make_async_copy(
            groups.at[pl.ds(slot * (share // 16), share // 16)], pre_act.at[lax.rem(it, fwd_tiles), at], a_sem.at[slot])

    def store_h(it):
        slot = lax.rem(it, 2)
        down = pl.ds(pl.multiple_of(lax.rem(it, fwd_tiles) * WIDE, WIDE), WIDE)
        at = pl.ds(pl.multiple_of(lax.rem(origin(it), 2) * share, share), share)
        return pltpu.make_async_copy(hbuf.at[slot], hidden_t.at[origin(it) // 2, down, at], h_sem.at[slot])

    def first_matmul(it):
        at = pl.ds(pl.multiple_of(lax.rem(it, fwd_tiles) * WIDE, WIDE), WIDE)
        chunk = rows[pl.ds(origin(it) * 2, 2)].reshape(share, width)
        a = nn(chunk, wbuf[lax.rem(it, 2)]) + b_in_ref[:, at].astype(F32)
        groups[pl.ds(lax.rem(it, 3) * (share // 16), share // 16)] = a.reshape(share // 16, 16, WIDE)

    def rest_of_step(it):
        a = groups[pl.ds(lax.rem(it, 3) * (share // 16), share // 16)].reshape(share, WIDE)
        t = jnp.tanh(ROOT * (a + CUBIC * (a * a * a)))
        hidden = (a * (0.5 * (1.0 + t))).astype(BF16)
        hbuf[lax.rem(it, 2)] = jnp.transpose(hidden)
        at = pl.ds(pl.multiple_of(origin(it) * share, share), share)
        acc[at, :] += nn(hidden, wbuf[2 + lax.rem(it, 2)])

    def forward(it, carry):
        nxt = it + 1
        store_a(it).start()
        load_o(it).wait()
        load_o(nxt).start()

        @pl.when(lax.rem(nxt, fwd_tiles) == 0)
        def _():
            q = nxt // fwd_tiles
            x_copy(2 * q - 1).wait_recv()
            x_copy(2 * q).wait_recv()

        load_i(nxt).wait()

        @pl.when(nxt + 1 < steps)
        def _():
            load_i(nxt + 1).start()

        @pl.when(it >= 2)
        def _():
            store_a(it - 2).wait()
            store_h(it - 2).wait()

        rest_of_step(it)
        first_matmul(nxt)
        store_h(it).start()
        for k, when in ((2, 1), (3, 2)):
            @pl.when(it == when)
            def _():
                stat_step(k)

        @pl.when(it == 3)
        def _():
            for s in range(3):
                for j in range(others):
                    d_copy(j, s).start()

        return carry

    x_copy(0).wait_recv()
    load_i(0).wait()
    first_matmul(jnp.int32(0))
    lax.fori_loop(0, steps - 1, forward, 0)
    last = jnp.int32(steps - 1)
    store_a(last).start()
    load_o(last).wait()
    store_a(last - 2).wait()
    store_h(last - 2).wait()
    rest_of_step(last)
    store_h(last).start()

    def place(stream):
        way = 1 - 2 * lax.rem(stream, 2)
        first_z = stream // 2
        pa = yy * (1 - first_z) + z * first_z
        pb = z * (1 - first_z) + yy * first_z

        def along(move):
            on_y = z * 4 + wrap(yy + move)
            on_z = wrap(z + move) * 4 + yy
            return on_y * (1 - first_z) + on_z * first_z, on_z * (1 - first_z) + on_y * first_z

        return way, pa, pb, along(way), along(-way)

    def send(tile, k, end=False):
        way, pa, pb, (next_a, next_b), _ = place(lax.rem(tile, 4))
        whole = late.at[tile - late_from] if end else summed.at[tile]
        if k < 3:
            src, dst, to = part_sum.at[tile, wrap(pa - way * (k + 1))], land_a.at[lax.rem(tile, half), k], next_a
        elif k < 6:
            src, dst, to = part_sum.at[tile, pa, wrap(pb - way * (k - 2))], land_b.at[lax.rem(tile, half), k - 3], next_b
        elif k < 9:
            src = whole.at[pa, wrap(pb - way * (k - 6))]
            dst, to = src, next_b
            if k == 6 and not end:
                src = own.at[tile]
        else:
            src = whole.at[wrap(pa - way * (k - 9))]
            dst, to = src, next_a
        return pltpu.make_async_remote_copy(
            src_ref=src, dst_ref=dst, send_sem=send_sem.at[tile],
            recv_sem=sum_sem.at[lax.rem(tile, half), k] if k < 6 else recv_sem.at[tile, k - 6],
            device_id=(to, ep), device_id_type=MESH)

    def sent(tile):
        count = 3 * (5 * 16 + 5 * 8)
        return pltpu.make_async_copy(acc.at[pl.ds(0, count)], acc.at[pl.ds(count, count)], send_sem.at[tile])

    def direct(tile):
        way, pa, _, _, _ = place(lax.rem(tile, 4))
        first_z = lax.rem(tile, 4) // 2
        row = late.at[tile - late_from, pa]
        copies = []
        for m, move in enumerate((way, -way, 2 * way)):
            to = (z * 4 + wrap(yy + move)) * (1 - first_z) + (wrap(z + move) * 4 + yy) * first_z
            copies.append(pltpu.make_async_remote_copy(
                src_ref=row, dst_ref=row, send_sem=send_sem.at[tile], recv_sem=recv_sem.at[tile, 3 + m],
                device_id=(to, ep), device_id_type=MESH))
        return copies

    def act_on(tile, k, action):
        if k < 6:
            action(send(tile, k))
        else:
            @pl.when(tile < late_from)
            def _():
                action(send(tile, k))

            @pl.when(tile >= late_from)
            def _():
                action(send(tile, k, True))

    def start(tile, k):
        if k < 6:
            @pl.when(tile >= half)
            def _():
                pl.semaphore_wait(credit.at[tile - half, k // 3], 1)

        act_on(tile, k, lambda copy: copy.start())

    def keep(tile):
        way, pa, pb, _, _ = place(lax.rem(tile, 4))
        return pltpu.make_async_copy(own.at[tile], summed.at[tile, pa, pb], own_sem.at[lax.rem(tile, half)])

    def keep_late(tile):
        spot = tile - late_from
        return pltpu.make_async_copy(late.at[spot], summed.at[tile], late_sem.at[spot])

    def advance(tile, k):
        way, pa, pb, _, (prev_a, prev_b) = place(lax.rem(tile, 4))
        spot = lax.rem(tile, half)
        if k >= 10:
            @pl.when(tile < late_from)
            def _():
                send(tile, k - 1).wait_recv()
                if k < 12:
                    send(tile, k).start()

            if k == 10:
                @pl.when(tile >= late_from)
                def _():
                    for copy in direct(tile):
                        copy.wait_recv()
                    keep_late(tile).start()

            return

        act_on(tile, k - 1, lambda copy: copy.wait_recv())
        if k <= 3:
            block = wrap(pa - way * (k + 1))
            part_sum[tile, block] = part_sum[tile, block] + land_a[spot, k - 1]
        elif k <= 6:
            block = wrap(pb - way * (k - 2))
            total = part_sum[tile, pa, block] + land_b[spot, k - 4]
            if k < 6:
                part_sum[tile, pa, block] = total
            else:
                @pl.when(tile < late_from)
                def _():
                    own[tile] = total.astype(BF16)
                    keep(tile).start()

                @pl.when(tile >= late_from)
                def _():
                    late[tile - late_from, pa, pb] = total.astype(BF16)
        elif k == 9:
            @pl.when(tile < late_from)
            def _():
                keep(tile).wait()
                send(tile, 9).start()

            @pl.when(tile >= late_from)
            def _():
                for copy in direct(tile):
                    copy.start()
        if k <= 6:
            back_to = prev_a if k <= 3 else prev_b

            @pl.when(tile < half)
            def _():
                pl.semaphore_signal(credit.at[tile, (k - 1) // 3], inc=1, device_id=(back_to, ep), device_id_type=MESH)

        if k < 9:
            start(tile, k)

    def wave(t, ages):
        for k in ages:
            unit = t - k

            @pl.when(jnp.logical_and(unit >= 0, unit < units))
            def _():
                def streams(stream, carry):
                    advance(unit * 4 + stream, k)
                    return carry

                lax.fori_loop(0, 4, streams, 0)

    def quarter(t, stream):
        for p, ages in enumerate(((6, 5), (4, 3), (2,), (1,))):
            @pl.when(stream == p)
            def _():
                wave(t, ages)

    def exchange(src, dst, send_sems, recv_sems):
        copies = []
        for j in range(1, experts):
            to = lax.rem(ep + j, experts)
            copies.append(pltpu.make_async_remote_copy(
                src_ref=src.at[to], dst_ref=dst.at[ep], send_sem=send_sems, recv_sem=recv_sems.at[j - 1],
                device_id=(dp, to), device_id_type=MESH))
        return copies

    def place_tile(tile, a, grad):
        for b in range(4):
            for j in range(3):
                at = b * (width // 16) + j * 16
                part_sum[tile, a, b, :, j * TILE:(j + 1) * TILE] = grad[at:at + 16, :]

    def load_hid(i):
        base = 2 * lax.rem(i, 2)
        at = pl.ds(pl.multiple_of(lax.rem(i, 4) * WIDE, WIDE), WIDE)
        return [pltpu.make_async_copy(hidden_t.at[h, at], wbuf.at[base + h], hid_sem.at[base + h]) for h in range(2)]

    def load_rest(i):
        slot = lax.rem(i, 2)
        at = pl.ds(pl.multiple_of(i * TILE, TILE), TILE)
        lanes = pl.ds(pl.multiple_of(lax.rem(i, WIDE // TILE) * TILE, TILE), TILE)
        return (
            pltpu.make_async_copy(pre_act.at[i // (WIDE // TILE), :, :, lanes], sbuf.at[slot], s_sem.at[slot]),
            pltpu.make_async_copy(w_in.at[:, at], wbuf.at[slot, :, pl.ds(0, TILE)], i_sem.at[slot]),
            pltpu.make_async_copy(w_out.at[at], wbuf.at[2 + slot, pl.ds(0, TILE)], o_sem.at[slot]),
        )

    store_a(last - 1).wait()
    store_a(last).wait()
    store_h(last - 1).wait()
    store_h(last).wait()
    for copy in load_hid(jnp.int32(0)):
        copy.start()
    all_sent(x_send)
    out_x[...] = acc[...].astype(BF16).reshape(out_x.shape)

    def out_tile(i, carry):
        unit, stream = i // 4, lax.rem(i, 4)
        quarter(unit, stream)

        @pl.when(stream == 0)
        def _():
            for j in range(others):
                d_copy(j, unit).wait_recv()

        at = pl.ds(pl.multiple_of(unit * TILE, TILE), TILE)
        for copy in load_hid(i):
            copy.wait()

        @pl.when(i + 1 < half)
        def _():
            for copy in load_hid(i + 1):
                copy.start()

        base = 2 * lax.rem(i, 2)
        grad = nn(wbuf[base], tok[0:WIDE, at]) + nn(wbuf[base + 1], tok[WIDE:, at])
        for a in range(4):
            place_tile(i, a, grad[a * (width // 4):(a + 1) * (width // 4)])
        start(i, 0)
        return carry

    lax.fori_loop(0, half, out_tile, 0)
    for copy in load_rest(jnp.int32(0)):
        copy.start()
    stat_step(4, stats_ref)
    send_y = exchange(out_x, back_y, y_send, y_recv)
    for copy in send_y:
        copy.start()
    self_y = pltpu.make_async_copy(out_x.at[ep], back_y.at[ep], self_sem.at[0])
    self_y.start()
    small_work[0, 12:13, :] = jnp.sum(tok[...].astype(F32), axis=0, keepdims=True)
    rows_t[...] = jnp.transpose(rows[...].reshape(n, width))
    acc[...] = jnp.zeros_like(acc)
    chunks = 4
    size = n // chunks

    def in_tile(i, carry):
        g = i + half
        quarter(g // 4, lax.rem(g, 4))
        slot = lax.rem(i, 2)
        for copy in load_rest(i):
            copy.wait()

        @pl.when(i + 1 < half)
        def _():
            for copy in load_rest(i + 1):
                copy.start()

        total = jnp.zeros((1, TILE), F32)
        for c in range(chunks):
            part = pl.ds(c * size, size)
            d_hidden = nt(tok[part, :], wbuf[2 + slot, 0:TILE, :]).astype(BF16)
            a = sbuf[slot, c * (size // 16):(c + 1) * (size // 16)].reshape(size, TILE)
            sq = a * a
            t = jnp.tanh(ROOT * (a + CUBIC * (sq * a)))
            slope = 0.5 * (1.0 + t) + (0.5 * ROOT) * a * (1.0 - t * t) * (1.0 + (3 * CUBIC) * sq)
            d_act = d_hidden.astype(F32) * slope
            total += jnp.sum(d_act, axis=0, keepdims=True)
            d_act_bf = d_act.astype(BF16)
            act[part, :] = d_act_bf
            acc[part, :] += nt(d_act_bf, wbuf[slot, :, 0:TILE])
        db_in[:, pl.ds(pl.multiple_of(i * TILE, TILE), TILE)] = total
        grad = nn(rows_t[...], act[...])
        for a in range(4):
            place_tile(g, a, grad[a * (width // 4):(a + 1) * (width // 4)])
        start(g, 0)

        @pl.when(i == half - 2)
        def _():
            for copy in send_y:
                copy.wait_recv()
            self_y.wait()
            back.start()

        return carry

    back = pltpu.make_async_copy(back_y, dy_buf.reshape(back_y.shape), tok_sem.at[1])
    lax.fori_loop(0, half, in_tile, 0)

    rows[...] = acc[...].astype(BF16).reshape(rows.shape)
    send_g = exchange(rows, back_d, g_send, g_recv)
    for copy in send_g:
        copy.start()
    self_g = pltpu.make_async_copy(rows.at[ep], back_d.at[ep], self_sem.at[1])
    self_g.start()

    for i in range(4):
        small_work[0, 8 + i:9 + i, :] = db_in[:, i * width:(i + 1) * width]
    d_router[...] = jnp.zeros_like(d_router)
    loss, terms, inv = global_terms(stats_ref[...], experts)
    loss_ref[...] = jnp.broadcast_to(loss, loss_ref.shape)

    def token_loads(i):
        at = pl.ds(pl.multiple_of(i * CHUNK, CHUNK), CHUNK)
        return (
            pltpu.make_async_copy(dy_any.at[at], wbuf.at[2, pl.ds(0, CHUNK)], o_sem.at[0]),
            pltpu.make_async_copy(x_any.at[at], wbuf.at[3, pl.ds(0, CHUNK)], o_sem.at[1]),
        )

    def out_store(i):
        at = pl.ds(pl.multiple_of(i * CHUNK, CHUNK), CHUNK)
        return pltpu.make_async_copy(stage, out.at[at], out_sem)

    for copy in token_loads(jnp.int32(0)):
        copy.start()
    back.wait()
    pieces = n // CHUNK

    def combine(i):
        lanes = pl.ds(pl.multiple_of(i * CHUNK, CHUNK), CHUNK)
        slot_col = col_of(slot_row[0:1, lanes])[:, 0:1]
        chosen = (lax.broadcasted_iota(jnp.int32, (CHUNK, n), 1).astype(F32) == slot_col).astype(BF16)
        y_tok = nn(chosen, dy_buf[...])
        logp = logp_ref[:, lanes]
        probs = jnp.exp(logp)
        onehot = (lax.broadcasted_iota(jnp.int32, (experts, CHUNK), 0).astype(F32) == ids_row[:, lanes]).astype(F32)
        gate = jnp.sum(probs * onehot, axis=0, keepdims=True)
        for copy in token_loads(i):
            copy.wait()

        @pl.when(i > 0)
        def _():
            out_store(i - 1).wait()

        stage[...] = (col_of(gate)[:, 0:1] * y_tok).astype(BF16)
        out_store(i).start()
        d_gate = row_of(jnp.sum(wbuf[2, 0:CHUNK, :].astype(F32) * y_tok, axis=1, keepdims=True))[0:1]
        is_text = mod_row[:, lanes] == 1.0
        global_part = jnp.where(is_text, terms[1][:, 0:1], terms[0][:, 0:1])
        inv_count = jnp.where(is_text, inv[1][:, 0:1], inv[0][:, 0:1])
        d_probs = onehot * d_gate + global_part - logp * inv_count
        d_log = probs * (d_probs - jnp.sum(d_probs * probs, axis=0, keepdims=True))
        d_log_ref[:, lanes] = d_log
        d_router[...] += nn(jnp.concatenate(split3(d_log), axis=0), wbuf[3, 0:CHUNK, :])

        @pl.when(i + 1 < pieces)
        def _():
            for copy in token_loads(i + 1):
                copy.start()

    def rest(t, carry):
        wave(t, range(12, 4, -1))
        combine(t - units)
        wave(t, range(4, 0, -1))
        return carry

    first = units + pieces
    lax.fori_loop(units, first, rest, 0)
    out_store(jnp.int32(pieces - 1)).wait()
    small_work[0, 0:experts, :] = d_router[0:experts] + d_router[experts:2 * experts] + d_router[2 * experts:]

    small_step(0)
    for k in range(1, 5):
        wave(first + k - 1, range(12, 8, -1))
        small_step(k, small_ref)
        wave(first + k - 1, range(8, 0, -1))

    def tail(t, carry):
        wave(t, range(12, 0, -1))
        return carry

    lax.fori_loop(first + 4, units + 11, tail, 0)

    def drain(tile, carry):
        sent(tile).wait()
        return carry

    lax.fori_loop(0, tiles, drain, 0)
    for sem in (d_send, y_send, g_send):
        all_sent(sem)
    for copy in send_g:
        copy.wait_recv()
    self_g.wait()
    for i in range(late.shape[0]):
        keep_late(jnp.int32(late_from + i)).wait()


def global_terms(stats, experts):
    loss = jnp.zeros((1, 128), F32)
    terms = []
    inv = []
    for m in range(2):
        base = 24 * m
        count = stats[base + 16:base + 17]
        mean = stats[base:base + 8] / count
        log_mean = jnp.log(mean)
        loss = loss + stats[base + 8:base + 9] / count + jnp.sum(mean * log_mean, axis=0, keepdims=True)
        terms.append(log_mean / count)
        inv.append(1.0 / count)
    return loss, terms, inv


def final_kernel(slot_ref, d_log_ref, back_any, router_ref, small_ref, loss_ref, summed, out_any,
                 dx, dw_in, dw_out, out, d_router_ref, db_in_ref, db_out_ref, aux_ref,
                 buf, back, out_buf, dx_buf, load_sem, store_sem, back_sem, out_sem, dx_sem):
    n, width = dx.shape
    tiles = buf.shape[0]
    half = tiles // 2
    units = tiles // 4
    experts = d_log_ref.shape[0]
    chunk = 2 * CHUNK
    pieces = n // chunk
    per_piece = tiles // (2 * pieces)

    load_back = pltpu.make_async_copy(back_any, back, back_sem)
    load_back.start()

    def loads(t):
        return [
            pltpu.make_async_copy(summed.at[t, :, :, :, pl.ds(j * TILE, TILE)], buf.at[t, :, :, j], load_sem.at[t])
            for j in range(3)
        ]

    def store(t):
        tile = buf.at[t].reshape(width, TILE)
        if t < half:
            unit, stream = t // 4, t % 4
            dst = dw_out.at[pl.ds(stream * width, width), pl.ds(unit * TILE, TILE)]
        else:
            dst = dw_in.at[:, pl.ds((t - half) * TILE, TILE)]
        return pltpu.make_async_copy(tile, dst, store_sem.at[t])

    for t in range(tiles):
        for copy in loads(t):
            copy.start()
    load_out = pltpu.make_async_copy(out_any, out_buf, out_sem.at[0])
    load_out.start()

    d_router_ref[...] = small_ref[0:experts, :]
    for i in range(4):
        db_in_ref[:, i * width:(i + 1) * width] = small_ref[8 + i:9 + i, :].astype(BF16)
    db_out_ref[...] = small_ref[12:13, :].astype(BF16)
    aux_ref[0, 0] = loss_ref[0, 0]
    r = split3(router_ref[...])
    rights = jnp.concatenate([r[0], r[1], r[0], r[1], r[2], r[0]], axis=0)

    def dx_store(i):
        at = pl.ds(i * chunk, chunk)
        return pltpu.make_async_copy(dx_buf.at[at], dx.at[at], dx_sem.at[i])

    def move(i):
        for t in range(i * per_piece, (i + 1) * per_piece):
            pltpu.make_async_copy(buf.at[t], buf.at[t], load_sem.at[t]).wait()
            store(t).start()

    load_back.wait()
    for i in range(pieces):
        lanes = pl.ds(i * chunk, chunk)
        d = split3(d_log_ref[:, lanes])
        lefts = jnp.concatenate([d[0], d[0], d[1], d[1], d[0], d[2]], axis=0)
        routed = tn(lefts, rights).astype(BF16)
        slot_col = col_of(slot_ref[0:1, lanes])[:, 0:1]
        chosen = (lax.broadcasted_iota(jnp.int32, (chunk, n), 1).astype(F32) == slot_col).astype(BF16)
        dx_buf[lanes, :] = (nn(chosen, back[...]) + routed.astype(F32)).astype(BF16)
        dx_store(i).start()
        move(2 * i)
        move(2 * i + 1)
    load_out.wait()
    store_out = pltpu.make_async_copy(out_buf, out, out_sem.at[1])
    store_out.start()
    for t in range(tiles):
        store(t).wait()
    for i in range(pieces):
        dx_store(i).wait()
    store_out.wait()


def vmem(count):
    return [pl.BlockSpec(memory_space=pltpu.VMEM)] * count


def cost(flops, size):
    return pl.CostEstimate(flops=int(flops), bytes_accessed=int(size), transcendentals=0)


def solution(mesh):
    token_spec = P(ALL_AXES)
    expert_spec = P("ep")

    def local_step(x, modality, router, expert_ids, priority, w_in, b_in, w_out, b_out, dy):
        n, width = x.shape
        experts = router.shape[1]
        hid = w_in.shape[2]
        capacity = n // experts
        tiles = hid // TILE
        share = n // (experts // 2)
        w_in, w_out = w_in[0], w_out[0]
        ids, prio, mod = (a.reshape(n // 128, 128) for a in (expert_ids, priority, modality))
        router_t = jnp.transpose(router)
        shape = jax.ShapeDtypeStruct
        anywhere = pl.BlockSpec(memory_space=pl.ANY)
        dma = pltpu.SemaphoreType.DMA
        slots = (experts, capacity, width)
        mm = 2 * n * width * hid
        others = experts - 1

        summed, back_y, d_back, out, _, _, slot, d_log, loss, small = pl.pallas_call(
            block_kernel,
            out_shape=(
                shape((2 * tiles, 4, 4, 16, width), BF16), shape(slots, BF16), shape(slots, BF16), shape((n, width), BF16),
                shape((n // WIDE, hid, WIDE), BF16), shape((hid // WIDE, n // 16, 16, WIDE), F32),
                shape((8, n), F32), shape((experts, n), F32), shape((8, 128), F32), shape((16, width), F32),
            ),
            in_specs=vmem(3) + [anywhere] * 2 + vmem(1) + [anywhere] + vmem(1) + [anywhere] + vmem(1),
            out_specs=(*[anywhere] * 6, *vmem(4)),
            scratch_shapes=[
                pltpu.VMEM((2 * tiles, 4, 4, 16, width), F32),
                pltpu.VMEM((tiles, 3, 4, 16, width), F32),
                pltpu.VMEM((tiles, 3, 16, width), F32),
                pltpu.VMEM((2 * tiles, 16, width), BF16),
                pltpu.VMEM((n, width), BF16),
                pltpu.VMEM((n, width), BF16),
                pltpu.VMEM(slots, BF16),
                pltpu.VMEM(slots, BF16),
                pltpu.VMEM((width, n), BF16),
                pltpu.VMEM((n, width), BF16),
                pltpu.VMEM((n, width), F32),
                pltpu.VMEM((4, WIDE, WIDE), BF16),
                pltpu.VMEM((2, n // 16, 16, TILE), F32),
                pltpu.VMEM((n, TILE), BF16),
                pltpu.VMEM((2, WIDE, share), BF16),
                pltpu.VMEM((CHUNK, width), BF16),
                pltpu.VMEM((4, 4, 4, 16, width), BF16),
                pltpu.VMEM((n, 8), F32),
                pltpu.VMEM((8, n), F32),
                pltpu.VMEM((8, n), F32),
                pltpu.VMEM((experts, n), F32),
                pltpu.VMEM((1, hid), F32),
                pltpu.VMEM((48, 128), F32),
                pltpu.VMEM((3 * experts, width), F32),
                pltpu.VMEM((4, 48, 128), F32), pltpu.VMEM((4, 4, 48, 128), F32),
                pltpu.VMEM((4, 16, width), F32), pltpu.VMEM((4, 4, 16, width), F32),
                dma((2 * tiles,)), dma((tiles, 6)), dma((2 * tiles, 6)), dma((tiles,)), pltpu.SemaphoreType.REGULAR((tiles, 2)),
                dma, dma((others,)), dma, dma((others, 3)), dma, dma((others,)), dma, dma((others,)),
                dma((2,)), dma((2,)), dma, dma((2,)), dma((2,)), dma((3,)), dma((2,)), dma((4,)), dma((2,)), dma((4,)),
                dma((4, 3)), dma((4, 3)),
            ],
            compiler_params=pltpu.CompilerParams(collective_id=1, has_side_effects=True, vmem_limit_bytes=67_000_000),
            cost_estimate=cost(6 * mm, 6 * n * hid), name="block",
        )(ids, prio, mod, x, dy, router_t, w_in, b_in, w_out, b_out)

        d_x, d_w_in, d_w_out, out, d_router, d_b_in, d_b_out, aux = pl.pallas_call(
            final_kernel,
            out_shape=(
                shape((n, width), BF16), shape((width, hid), BF16), shape((hid, width), BF16), shape((n, width), BF16),
                shape((experts, width), F32), shape((1, hid), BF16), shape((1, width), BF16), shape((1, 1), F32),
            ),
            in_specs=vmem(2) + [anywhere] + vmem(3) + [anywhere] * 2,
            out_specs=(*[anywhere] * 4, *vmem(3), pl.BlockSpec(memory_space=pltpu.SMEM)),
            scratch_shapes=[
                pltpu.VMEM((2 * tiles, 4, 4, 3, 16, TILE), BF16),
                pltpu.VMEM((n, width), BF16), pltpu.VMEM((n, width), BF16), pltpu.VMEM((n, width), BF16),
                dma((2 * tiles,)), dma((2 * tiles,)), dma, dma((2,)), dma((n // (2 * CHUNK),)),
            ],
            compiler_params=pltpu.CompilerParams(vmem_limit_bytes=66_000_000),
            cost_estimate=cost(2 * n * n * width, 8 * width * hid), name="final",
        )(slot, d_log, d_back.reshape(n, width), router_t, small, loss, summed, out)
        return out, aux[0, 0], d_x, jnp.transpose(d_router), d_w_in[None], d_b_in, d_w_out[None], d_b_out

    return jax.shard_map(
        local_step,
        mesh=mesh,
        in_specs=(token_spec, token_spec, P(), token_spec, token_spec, expert_spec, expert_spec, expert_spec, expert_spec, token_spec),
        out_specs=(token_spec, P(), token_spec, P(), expert_spec, expert_spec, expert_spec, expert_spec),
        check_vma=False,
    )
```

```python
import functools

import jax
import jax.numpy as jnp
from jax import lax
from jax.experimental import pallas as pl
from jax.experimental.pallas import tpu as pltpu
from jax.sharding import PartitionSpec as P

ALL_AXES = ("dp", "ep")
MESH = pl.DeviceIdType.MESH
F32 = jnp.float32
BF16 = jnp.bfloat16
NOWHERE = -1.0
TILE = 256
CHUNK = 256
WIDE = 768


def col_of(row):
    return jnp.transpose(jnp.broadcast_to(row, (8, row.shape[1])))


def row_of(col):
    return jnp.transpose(jnp.broadcast_to(col, (col.shape[0], 8)))


def split3(a):
    hi = a.astype(BF16)
    rest = a - hi.astype(F32)
    mid = rest.astype(BF16)
    lo = (rest - mid.astype(F32)).astype(BF16)
    return hi, mid, lo


def nt(a, b):
    return lax.dot_general(a, b, (((1,), (1,)), ((), ())), preferred_element_type=F32)


def tn(a, b):
    return lax.dot_general(a, b, (((0,), (0,)), ((), ())), preferred_element_type=F32)


def nn(a, b):
    return jnp.dot(a, b, preferred_element_type=F32)


def wide(ref):
    v = ref[...].astype(F32)
    return jnp.concatenate([v[i:i + 1, :] for i in range(v.shape[0])], axis=1)


def greet(peers):
    barrier = pltpu.get_barrier_semaphore()
    for peer in peers:
        pl.semaphore_signal(barrier, inc=1, device_id=peer, device_id_type=MESH)
    return lambda: pl.semaphore_wait(barrier, len(peers))


ROOT = 0.7978845608028654
CUBIC = 0.044715


def block_kernel(
    ids_ref, prio_ref, mod_ref, x_any, dy_any, router_ref, w_in, b_in_ref, w_out, b_out_ref,
    summed, back_y, back_d, out, hidden_t, pre_act, slot_row, d_log_ref, loss_ref, small_ref,
    part_sum, land_a, land_b, own, x_buf, dy_buf, out_x, rows, rows_t, tok, acc, wbuf, sbuf, act, hbuf, stage, late,
    keycol, ids_row, mod_row, logp_ref, db_in, stats_ref, d_router, stat_work, stat_bufs, small_work, small_bufs,
    send_sem, sum_sem, recv_sem, own_sem, credit, x_send, x_recv, d_send, d_recv, y_send, y_recv, g_send, g_recv,
    self_sem, tok_sem, out_sem, i_sem, o_sem, a_sem, h_sem, hid_sem, s_sem, late_sem, stat_send, stat_recv,
):
    dp = lax.axis_index("dp")
    ep = lax.axis_index("ep")
    z, yy = dp // 4, lax.rem(dp, 4)
    xx, core = ep // 2, lax.rem(ep, 2)
    tiles = part_sum.shape[0]
    units = tiles // 4
    half = tiles // 2
    experts, capacity, width = out_x.shape
    n = experts * capacity
    pairs = experts // 2
    share = n // pairs
    fwd_tiles = hidden_t.shape[1] // WIDE
    steps = pairs * fwd_tiles
    groups = part_sum.reshape(tiles * 16, 16, width)
    late_from = tiles - late.shape[0]
    others = experts - 1
    out_d = x_buf.reshape(out_x.shape)
    tok_slots = tok.reshape(out_x.shape)

    def wrap(v):
        return lax.rem(v + 16, 4)

    peers = [(z * 4 + wrap(yy + j), ep) for j in range(1, 4)] + [(wrap(z + j) * 4 + yy, ep) for j in range(1, 4)]
    enter = greet(peers + [(dp, lax.rem(ep + j, experts)) for j in range(1, experts)])
    load_x = pltpu.make_async_copy(x_any, x_buf, tok_sem.at[0])
    load_dy = pltpu.make_async_copy(dy_any, dy_buf, tok_sem.at[1])
    load_x.start()
    load_dy.start()

    rings = (
        (yy, peers[0:3]),
        (z, peers[3:6]),
        None,
        (xx, [(dp, lax.rem(ep + 2 * j, experts)) for j in range(1, 4)]),
    )
    partner = (dp, xx * 2 + 1 - core)

    def small_sum(work, bufs, whole_rows, send_sems, recv_sems):
        head = pl.ds(0, whole_rows)
        full = pl.ds(0, work.shape[1])

        def pair():
            return pltpu.make_async_remote_copy(
                src_ref=work.at[2, head], dst_ref=bufs.at[2, 0, head], send_sem=send_sems.at[2, 0], recv_sem=recv_sems.at[2, 0],
                device_id=partner, device_id_type=MESH)

        def ring(axis):
            me, ring_peers = rings[axis]
            at = head if axis == 3 else full
            return [
                pltpu.make_async_remote_copy(
                    src_ref=work.at[axis, at], dst_ref=bufs.at[axis, me, at], send_sem=send_sems.at[axis, j],
                    recv_sem=recv_sems.at[axis, j], device_id=ring_peers[j], device_id_type=MESH)
                for j in range(3)
            ]

        def launch(axis):
            bufs[axis, rings[axis][0]] = work[axis]
            for copy in ring(axis):
                copy.start()

        def total(axis, at):
            for copy in ring(axis):
                copy.wait()
            return bufs[axis, 0, at, :] + bufs[axis, 1, at, :] + bufs[axis, 2, at, :] + bufs[axis, 3, at, :]

        def step(k, dst=None):
            if k == 0:
                launch(0)
            elif k == 1:
                work[1] = total(0, full)
                launch(1)
            elif k == 2:
                work[2] = total(1, full)
                pair().start()
            elif k == 3:
                pair().wait()
                work[3] = work[2]
                work[3, head, :] = work[2, head, :] + bufs[2, 0, head, :]
                launch(3)
            else:
                dst[...] = work[2]
                dst[head, :] = total(3, head)

        return step

    stat_step = small_sum(stat_work, stat_bufs, 48, stat_send, stat_recv)
    small_step = small_sum(small_work, small_bufs, experts, stat_send, stat_recv)

    ids = wide(ids_ref)
    key = ids * n + wide(prio_ref)
    low = ids * n
    keycol[...] = col_of(key)

    def count(j, total):
        col = keycol[pl.ds(pl.multiple_of(j * 128, 128), 128), :][:, 0:1]
        before = jnp.logical_and(col < key, col >= low)
        return total + jnp.sum(before.astype(F32), axis=0, keepdims=True)

    position = lax.fori_loop(0, n // 128, count, jnp.zeros((1, n), F32))
    slot = jnp.where(position < capacity, ids * capacity + position, NOWHERE)
    slot_row[...] = jnp.broadcast_to(slot, slot_row.shape)
    mod = wide(mod_ref)
    ids_row[...] = jnp.broadcast_to(ids, ids_row.shape)
    mod_row[...] = jnp.broadcast_to(mod, mod_row.shape)

    def hops(q):
        return q + q // 2 - 2 * (q // 3)

    def target(j):
        return wrap(xx + hops((j + 1) // 2)) * 2 + lax.rem(core + 1 - lax.rem(j, 2), 2)

    def pick(e):
        index = (lax.broadcasted_iota(jnp.int32, (capacity, n), 0) + e * capacity).astype(F32)
        return (index == slot_row[0:1, :]).astype(BF16)

    def x_copy(j):
        to = target(j)
        return pltpu.make_async_remote_copy(
            src_ref=out_x.at[to], dst_ref=rows.at[ep], send_sem=x_send, recv_sem=x_recv.at[j],
            device_id=(dp, to), device_id_type=MESH)

    def d_copy(j, s):
        to = target(j)
        at = pl.ds(pl.multiple_of(s * TILE, TILE), TILE)
        return pltpu.make_async_remote_copy(
            src_ref=out_d.at[to, :, at], dst_ref=tok_slots.at[ep, :, at], send_sem=d_send, recv_sem=d_recv.at[s],
            device_id=(dp, to), device_id_type=MESH)

    def load_i(it):
        slot = lax.rem(it, 2)
        at = pl.ds(pl.multiple_of(lax.rem(it, fwd_tiles) * WIDE, WIDE), WIDE)
        return pltpu.make_async_copy(w_in.at[:, at], wbuf.at[slot], i_sem.at[slot])

    def load_o(it):
        slot = lax.rem(it, 2)
        at = pl.ds(pl.multiple_of(lax.rem(it, fwd_tiles) * WIDE, WIDE), WIDE)
        return pltpu.make_async_copy(w_out.at[at], wbuf.at[2 + slot], o_sem.at[slot])

    def all_sent(sem):
        pltpu.make_async_copy(out_x.at[pl.ds(0, others)], out_x.at[pl.ds(0, others)], sem).wait()

    load_x.wait()
    enter()

    def send_x(i, carry):
        j = lax.rem(i + 1, others) + jnp.where(i == 1, 1, 0) - jnp.where(i == 2, 1, 0)
        out_x[target(j)] = nn(pick(target(j)), x_buf[...]).astype(BF16)
        x_copy(j).start()
        return carry

    lax.fori_loop(0, others, send_x, 0)
    load_i(0).start()
    load_i(1).start()
    load_o(0).start()
    rows[ep] = nn(pick(ep), x_buf[...]).astype(BF16)

    router3 = jnp.concatenate(split3(router_ref[...]), axis=0)
    logits3 = nt(router3, x_buf[...])
    logits = logits3[0:experts] + logits3[experts:2 * experts] + logits3[2 * experts:3 * experts]
    shifted = logits - jnp.max(logits, axis=0, keepdims=True)
    logp = shifted - jnp.log(jnp.sum(jnp.exp(shifted), axis=0, keepdims=True))
    logp_ref[...] = logp
    probs = jnp.exp(logp)
    onehot = (lax.broadcasted_iota(jnp.int32, (experts, n), 0).astype(F32) == ids).astype(F32)
    gate = jnp.sum(probs * onehot, axis=0, keepdims=True)
    entropy = -jnp.sum(probs * logp, axis=0, keepdims=True)
    for m in range(2):
        mask = (mod == m).astype(F32)
        stat_work[0, 24 * m:24 * m + 8, :] = jnp.broadcast_to(jnp.sum(probs * mask, axis=1, keepdims=True), (8, 128))
        stat_work[0, 24 * m + 8:24 * m + 16, :] = jnp.broadcast_to(jnp.sum(entropy * mask, axis=1, keepdims=True), (8, 128))
        stat_work[0, 24 * m + 16:24 * m + 24, :] = jnp.broadcast_to(jnp.sum(mask, axis=1, keepdims=True), (8, 128))
    stat_step(0)
    load_dy.wait()
    dy_buf[...] = (col_of(gate)[:, 0:1] * dy_buf[...].astype(F32)).astype(BF16)

    def pick_cotangent(j, carry):
        out_d[target(j)] = nn(pick(target(j)), dy_buf[...]).astype(BF16)
        return carry

    lax.fori_loop(0, others, pick_cotangent, 0)
    tok_slots[ep] = nn(pick(ep), dy_buf[...]).astype(BF16)
    stat_step(1)
    acc[...] = jnp.broadcast_to(b_out_ref[...].astype(F32), acc.shape)
    small_work[0] = jnp.zeros(small_work.shape[1:], F32)

    def origin(it):
        return wrap(xx - hops(it // fwd_tiles))

    def store_a(it):
        slot = lax.rem(it, 3)
        at = pl.ds(pl.multiple_of(origin(it) * (share // 16), share // 16), share // 16)
        return pltpu.make_async_copy(
            groups.at[pl.ds(slot * (share // 16), share // 16)], pre_act.at[lax.rem(it, fwd_tiles), at], a_sem.at[slot])

    def store_h(it):
        slot = lax.rem(it, 2)
        down = pl.ds(pl.multiple_of(lax.rem(it, fwd_tiles) * WIDE, WIDE), WIDE)
        at = pl.ds(pl.multiple_of(lax.rem(origin(it), 2) * share, share), share)
        return pltpu.make_async_copy(hbuf.at[slot], hidden_t.at[origin(it) // 2, down, at], h_sem.at[slot])

    def first_matmul(it):
        at = pl.ds(pl.multiple_of(lax.rem(it, fwd_tiles) * WIDE, WIDE), WIDE)
        chunk = rows[pl.ds(origin(it) * 2, 2)].reshape(share, width)
        a = nn(chunk, wbuf[lax.rem(it, 2)]) + b_in_ref[:, at].astype(F32)
        groups[pl.ds(lax.rem(it, 3) * (share // 16), share // 16)] = a.reshape(share // 16, 16, WIDE)

    def rest_of_step(it):
        a = groups[pl.ds(lax.rem(it, 3) * (share // 16), share // 16)].reshape(share, WIDE)
        t = jnp.tanh(ROOT * (a + CUBIC * (a * a * a)))
        hidden = (a * (0.5 * (1.0 + t))).astype(BF16)
        hbuf[lax.rem(it, 2)] = jnp.transpose(hidden)
        at = pl.ds(pl.multiple_of(origin(it) * share, share), share)
        acc[at, :] += nn(hidden, wbuf[2 + lax.rem(it, 2)])

    def forward(it, carry):
        nxt = it + 1
        store_a(it).start()
        load_o(it).wait()
        load_o(nxt).start()

        @pl.when(lax.rem(nxt, fwd_tiles) == 0)
        def _():
            q = nxt // fwd_tiles
            x_copy(2 * q - 1).wait_recv()
            x_copy(2 * q).wait_recv()

        load_i(nxt).wait()

        @pl.when(nxt + 1 < steps)
        def _():
            load_i(nxt + 1).start()

        @pl.when(it >= 2)
        def _():
            store_a(it - 2).wait()
            store_h(it - 2).wait()

        rest_of_step(it)
        first_matmul(nxt)
        store_h(it).start()
        for k, when in ((2, 1), (3, 2)):
            @pl.when(it == when)
            def _():
                stat_step(k)

        @pl.when(it == 3)
        def _():
            for s in range(3):
                for j in (1, 3, 2, 4, 5, 6, 0):
                    d_copy(j, s).start()

        return carry

    x_copy(0).wait_recv()
    load_i(0).wait()
    first_matmul(jnp.int32(0))
    lax.fori_loop(0, steps - 1, forward, 0)
    last = jnp.int32(steps - 1)

    def load_hid(i):
        base = 2 * lax.rem(i, 2)
        at = pl.ds(pl.multiple_of(lax.rem(i, 4) * WIDE, WIDE), WIDE)
        return [pltpu.make_async_copy(hidden_t.at[h, at], wbuf.at[base + h], hid_sem.at[base + h]) for h in range(2)]

    for copy in load_hid(jnp.int32(0)):
        copy.start()
    store_a(last).start()
    load_o(last).wait()
    store_a(last - 2).wait()
    store_h(last - 2).wait()
    rest_of_step(last)
    store_h(last).start()

    def place(stream):
        way = 1 - 2 * lax.rem(stream, 2)
        first_z = stream // 2
        pa = yy * (1 - first_z) + z * first_z
        pb = z * (1 - first_z) + yy * first_z

        def along(move):
            on_y = z * 4 + wrap(yy + move)
            on_z = wrap(z + move) * 4 + yy
            return on_y * (1 - first_z) + on_z * first_z, on_z * (1 - first_z) + on_y * first_z

        return way, pa, pb, along(way), along(-way)

    def send(tile, k, end=False):
        way, pa, pb, (next_a, next_b), _ = place(lax.rem(tile, 4))
        whole = late.at[tile - late_from] if end else summed.at[tile]
        if k < 3:
            src, dst, to = part_sum.at[tile, wrap(pa - way * (k + 1))], land_a.at[lax.rem(tile, half), k], next_a
        elif k < 6:
            src, dst, to = part_sum.at[tile, pa, wrap(pb - way * (k - 2))], land_b.at[lax.rem(tile, half), k - 3], next_b
        elif k < 9:
            src = whole.at[pa, wrap(pb - way * (k - 6))]
            dst, to = src, next_b
            if k == 6 and not end:
                src = own.at[tile]
        else:
            src = whole.at[wrap(pa - way * (k - 9))]
            dst, to = src, next_a
        return pltpu.make_async_remote_copy(
            src_ref=src, dst_ref=dst, send_sem=send_sem.at[tile],
            recv_sem=sum_sem.at[lax.rem(tile, half), k] if k < 6 else recv_sem.at[tile, k - 6],
            device_id=(to, ep), device_id_type=MESH)

    def sent(tile):
        count = 3 * (5 * 16 + 5 * 8)
        return pltpu.make_async_copy(acc.at[pl.ds(0, count)], acc.at[pl.ds(count, count)], send_sem.at[tile])

    def direct(tile):
        way, pa, _, _, _ = place(lax.rem(tile, 4))
        first_z = lax.rem(tile, 4) // 2
        row = late.at[tile - late_from, pa]
        copies = []
        for m, move in enumerate((way, -way, 2 * way)):
            to = (z * 4 + wrap(yy + move)) * (1 - first_z) + (wrap(z + move) * 4 + yy) * first_z
            copies.append(pltpu.make_async_remote_copy(
                src_ref=row, dst_ref=row, send_sem=send_sem.at[tile], recv_sem=recv_sem.at[tile, 3 + m],
                device_id=(to, ep), device_id_type=MESH))
        return copies

    def act_on(tile, k, action):
        if k < 6:
            action(send(tile, k))
        else:
            @pl.when(tile < late_from)
            def _():
                action(send(tile, k))

            @pl.when(tile >= late_from)
            def _():
                action(send(tile, k, True))

    def start(tile, k):
        if k < 6:
            @pl.when(tile >= half)
            def _():
                pl.semaphore_wait(credit.at[tile - half, k // 3], 1)

        act_on(tile, k, lambda copy: copy.start())

    def keep(tile):
        way, pa, pb, _, _ = place(lax.rem(tile, 4))
        return pltpu.make_async_copy(own.at[tile], summed.at[tile, pa, pb], own_sem.at[lax.rem(tile, half)])

    def keep_late(tile):
        spot = tile - late_from
        return pltpu.make_async_copy(late.at[spot], summed.at[tile], late_sem.at[spot])

    def advance(tile, k):
        way, pa, pb, _, (prev_a, prev_b) = place(lax.rem(tile, 4))
        spot = lax.rem(tile, half)
        if k >= 10:
            @pl.when(tile < late_from)
            def _():
                send(tile, k - 1).wait_recv()
                if k < 12:
                    send(tile, k).start()

            if k == 10:
                @pl.when(tile >= late_from)
                def _():
                    for copy in direct(tile):
                        copy.wait_recv()
                    keep_late(tile).start()

            return

        act_on(tile, k - 1, lambda copy: copy.wait_recv())
        if k <= 3:
            block = wrap(pa - way * (k + 1))
            part_sum[tile, block] = part_sum[tile, block] + land_a[spot, k - 1]
        elif k <= 6:
            block = wrap(pb - way * (k - 2))
            total = part_sum[tile, pa, block] + land_b[spot, k - 4]
            if k < 6:
                part_sum[tile, pa, block] = total
            else:
                @pl.when(tile < late_from)
                def _():
                    own[tile] = total.astype(BF16)
                    keep(tile).start()

                @pl.when(tile >= late_from)
                def _():
                    late[tile - late_from, pa, pb] = total.astype(BF16)
        elif k == 9:
            @pl.when(tile < late_from)
            def _():
                keep(tile).wait()
                send(tile, 9).start()

            @pl.when(tile >= late_from)
            def _():
                for copy in direct(tile):
                    copy.start()
        if k <= 6:
            back_to = prev_a if k <= 3 else prev_b

            @pl.when(tile < half)
            def _():
                pl.semaphore_signal(credit.at[tile, (k - 1) // 3], inc=1, device_id=(back_to, ep), device_id_type=MESH)

        if k < 9:
            start(tile, k)

    def wave(t, ages):
        for k in ages:
            unit = t - k

            @pl.when(jnp.logical_and(unit >= 0, unit < units))
            def _():
                def streams(stream, carry):
                    advance(unit * 4 + stream, k)
                    return carry

                lax.fori_loop(0, 4, streams, 0)

    def quarter(t, stream):
        for p, ages in enumerate(((6, 5), (4, 3), (2,), (1,))):
            @pl.when(stream == p)
            def _():
                wave(t, ages)

    def exchange(src, dst, send_sems, recv_sems):
        copies = []
        for j in range(1, experts):
            to = lax.rem(ep + j, experts)
            copies.append(pltpu.make_async_remote_copy(
                src_ref=src.at[to], dst_ref=dst.at[ep], send_sem=send_sems, recv_sem=recv_sems,
                device_id=(dp, to), device_id_type=MESH))
        return copies

    def place_tile(tile, a, grad):
        for b in range(4):
            for j in range(3):
                at = b * (width // 16) + j * 16
                part_sum[tile, a, b, :, j * TILE:(j + 1) * TILE] = grad[at:at + 16, :]

    def load_rest(i):
        slot = lax.rem(i, 2)
        at = pl.ds(pl.multiple_of(i * TILE, TILE), TILE)
        lanes = pl.ds(pl.multiple_of(lax.rem(i, WIDE // TILE) * TILE, TILE), TILE)
        return (
            pltpu.make_async_copy(pre_act.at[i // (WIDE // TILE), :, :, lanes], sbuf.at[slot], s_sem.at[slot]),
            pltpu.make_async_copy(w_in.at[:, at], wbuf.at[slot, :, pl.ds(0, TILE)], i_sem.at[slot]),
            pltpu.make_async_copy(w_out.at[at], wbuf.at[2 + slot, pl.ds(0, TILE)], o_sem.at[slot]),
        )

    store_a(last - 1).wait()
    store_a(last).wait()
    store_h(last - 1).wait()
    store_h(last).wait()

    def out_tile(i, carry):
        unit, stream = i // 4, lax.rem(i, 4)
        quarter(unit, stream)

        @pl.when(stream == 0)
        def _():
            slices = out_x.at[pl.ds(0, others), :, pl.ds(0, TILE)]
            pltpu.make_async_copy(slices, slices, d_recv.at[unit]).wait()

        at = pl.ds(pl.multiple_of(unit * TILE, TILE), TILE)
        for copy in load_hid(i):
            copy.wait()

        @pl.when(i + 1 < half)
        def _():
            for copy in load_hid(i + 1):
                copy.start()

        base = 2 * lax.rem(i, 2)
        grad = nn(wbuf[base], tok[0:WIDE, at]) + nn(wbuf[base + 1], tok[WIDE:, at])
        for a in range(4):
            place_tile(i, a, grad[a * (width // 4):(a + 1) * (width // 4)])
        start(i, 0)
        return carry

    lax.fori_loop(0, half, out_tile, 0)
    for copy in load_rest(jnp.int32(0)):
        copy.start()
    stat_step(4, stats_ref)
    all_sent(x_send)
    out_x[...] = acc[...].astype(BF16).reshape(out_x.shape)
    send_y = exchange(out_x, back_y, y_send, y_recv)
    for copy in send_y:
        copy.start()
    self_y = pltpu.make_async_copy(out_x.at[ep], back_y.at[ep], self_sem.at[0])
    self_y.start()
    small_work[0, 12:13, :] = jnp.sum(tok[...].astype(F32), axis=0, keepdims=True)
    rows_t[...] = jnp.transpose(rows[...].reshape(n, width))
    acc[...] = jnp.zeros_like(acc)
    chunks = 4
    size = n // chunks

    def in_tile(i, carry):
        g = i + half
        quarter(g // 4, lax.rem(g, 4))
        slot = lax.rem(i, 2)
        for copy in load_rest(i):
            copy.wait()

        @pl.when(i + 1 < half)
        def _():
            for copy in load_rest(i + 1):
                copy.start()

        total = jnp.zeros((1, TILE), F32)
        for c in range(chunks):
            part = pl.ds(c * size, size)
            d_hidden = nt(tok[part, :], wbuf[2 + slot, 0:TILE, :]).astype(BF16)
            a = sbuf[slot, c * (size // 16):(c + 1) * (size // 16)].reshape(size, TILE)
            sq = a * a
            t = jnp.tanh(ROOT * (a + CUBIC * (sq * a)))
            slope = 0.5 * (1.0 + t) + (0.5 * ROOT) * a * (1.0 - t * t) * (1.0 + (3 * CUBIC) * sq)
            d_act = d_hidden.astype(F32) * slope
            total += jnp.sum(d_act, axis=0, keepdims=True)
            d_act_bf = d_act.astype(BF16)
            act[part, :] = d_act_bf
            acc[part, :] += nt(d_act_bf, wbuf[slot, :, 0:TILE])
        db_in[:, pl.ds(pl.multiple_of(i * TILE, TILE), TILE)] = total
        grad = nn(rows_t[...], act[...])
        for a in range(4):
            place_tile(g, a, grad[a * (width // 4):(a + 1) * (width // 4)])
        start(g, 0)

        @pl.when(i == half - 2)
        def _():
            all_sent(y_recv)
            self_y.wait()
            back.start()

        return carry

    back = pltpu.make_async_copy(back_y, dy_buf.reshape(back_y.shape), tok_sem.at[1])
    lax.fori_loop(0, half, in_tile, 0)

    rows[...] = acc[...].astype(BF16).reshape(rows.shape)
    send_g = exchange(rows, back_d, g_send, g_recv)
    for copy in send_g:
        copy.start()
    self_g = pltpu.make_async_copy(rows.at[ep], back_d.at[ep], self_sem.at[1])
    self_g.start()

    for i in range(4):
        small_work[0, 8 + i:9 + i, :] = db_in[:, i * width:(i + 1) * width]
    d_router[...] = jnp.zeros_like(d_router)
    loss, terms, inv = global_terms(stats_ref[...], experts)
    loss_ref[...] = jnp.broadcast_to(loss, loss_ref.shape)

    def token_loads(i):
        at = pl.ds(pl.multiple_of(i * CHUNK, CHUNK), CHUNK)
        return (
            pltpu.make_async_copy(dy_any.at[at], wbuf.at[2, pl.ds(0, CHUNK)], o_sem.at[0]),
            pltpu.make_async_copy(x_any.at[at], wbuf.at[3, pl.ds(0, CHUNK)], o_sem.at[1]),
        )

    def out_store(i):
        at = pl.ds(pl.multiple_of(i * CHUNK, CHUNK), CHUNK)
        return pltpu.make_async_copy(stage, out.at[at], out_sem)

    for copy in token_loads(jnp.int32(0)):
        copy.start()
    back.wait()
    pieces = n // CHUNK

    def combine(i):
        lanes = pl.ds(pl.multiple_of(i * CHUNK, CHUNK), CHUNK)
        slot_col = col_of(slot_row[0:1, lanes])[:, 0:1]
        chosen = (lax.broadcasted_iota(jnp.int32, (CHUNK, n), 1).astype(F32) == slot_col).astype(BF16)
        y_tok = nn(chosen, dy_buf[...])
        logp = logp_ref[:, lanes]
        probs = jnp.exp(logp)
        onehot = (lax.broadcasted_iota(jnp.int32, (experts, CHUNK), 0).astype(F32) == ids_row[:, lanes]).astype(F32)
        gate = jnp.sum(probs * onehot, axis=0, keepdims=True)
        for copy in token_loads(i):
            copy.wait()

        @pl.when(i > 0)
        def _():
            out_store(i - 1).wait()

        stage[...] = (col_of(gate)[:, 0:1] * y_tok).astype(BF16)
        out_store(i).start()
        d_gate = row_of(jnp.sum(wbuf[2, 0:CHUNK, :].astype(F32) * y_tok, axis=1, keepdims=True))[0:1]
        is_text = mod_row[:, lanes] == 1.0
        global_part = jnp.where(is_text, terms[1][:, 0:1], terms[0][:, 0:1])
        inv_count = jnp.where(is_text, inv[1][:, 0:1], inv[0][:, 0:1])
        d_probs = onehot * d_gate + global_part - logp * inv_count
        d_log = probs * (d_probs - jnp.sum(d_probs * probs, axis=0, keepdims=True))
        d_log_ref[:, lanes] = d_log
        d_router[...] += nn(jnp.concatenate(split3(d_log), axis=0), wbuf[3, 0:CHUNK, :])

        @pl.when(i + 1 < pieces)
        def _():
            for copy in token_loads(i + 1):
                copy.start()

    def rest(t, carry):
        wave(t, range(12, 4, -1))
        combine(t - units)
        wave(t, range(4, 0, -1))
        return carry

    first = units + pieces
    lax.fori_loop(units, first, rest, 0)
    out_store(jnp.int32(pieces - 1)).wait()
    small_work[0, 0:experts, :] = d_router[0:experts] + d_router[experts:2 * experts] + d_router[2 * experts:]

    small_step(0)
    for k in range(1, 5):
        wave(first + k - 1, range(12, 8, -1))
        small_step(k, small_ref)
        wave(first + k - 1, range(8, 0, -1))

    def tail(t, carry):
        wave(t, range(12, 0, -1))
        return carry

    lax.fori_loop(first + 4, units + 11, tail, 0)

    def drain(tile, carry):
        sent(tile).wait()
        return carry

    lax.fori_loop(0, tiles, drain, 0)
    for sem in (d_send, y_send, g_send, g_recv):
        all_sent(sem)
    self_g.wait()
    for i in range(late.shape[0]):
        keep_late(jnp.int32(late_from + i)).wait()


def global_terms(stats, experts):
    loss = jnp.zeros((1, 128), F32)
    terms = []
    inv = []
    for m in range(2):
        base = 24 * m
        count = stats[base + 16:base + 17]
        mean = stats[base:base + 8] / count
        log_mean = jnp.log(mean)
        loss = loss + stats[base + 8:base + 9] / count + jnp.sum(mean * log_mean, axis=0, keepdims=True)
        terms.append(log_mean / count)
        inv.append(1.0 / count)
    return loss, terms, inv


def final_kernel(slot_ref, d_log_ref, back_any, router_ref, small_ref, loss_ref, summed, out_any,
                 dx, dw_in, dw_out, out, d_router_ref, db_in_ref, db_out_ref, aux_ref,
                 buf, back, out_buf, dx_buf, load_sem, store_sem, back_sem, out_sem, dx_sem):
    n, width = dx.shape
    tiles = buf.shape[0]
    half = tiles // 2
    units = tiles // 4
    experts = d_log_ref.shape[0]
    chunk = 2 * CHUNK
    pieces = n // chunk
    per_piece = tiles // (2 * pieces)

    load_back = pltpu.make_async_copy(back_any, back, back_sem)
    load_back.start()

    def loads(t):
        return [
            pltpu.make_async_copy(summed.at[t, :, :, :, pl.ds(j * TILE, TILE)], buf.at[t, :, :, j], load_sem.at[t])
            for j in range(3)
        ]

    def store(t):
        tile = buf.at[t].reshape(width, TILE)
        if t < half:
            unit, stream = t // 4, t % 4
            dst = dw_out.at[pl.ds(stream * width, width), pl.ds(unit * TILE, TILE)]
        else:
            dst = dw_in.at[:, pl.ds((t - half) * TILE, TILE)]
        return pltpu.make_async_copy(tile, dst, store_sem.at[t])

    for t in range(tiles):
        for copy in loads(t):
            copy.start()
    load_out = pltpu.make_async_copy(out_any, out_buf, out_sem.at[0])
    load_out.start()

    d_router_ref[...] = small_ref[0:experts, :]
    for i in range(4):
        db_in_ref[:, i * width:(i + 1) * width] = small_ref[8 + i:9 + i, :].astype(BF16)
    db_out_ref[...] = small_ref[12:13, :].astype(BF16)
    aux_ref[0, 0] = loss_ref[0, 0]
    r = split3(router_ref[...])
    rights = jnp.concatenate([r[0], r[1], r[0], r[1], r[2], r[0]], axis=0)

    def dx_store(i):
        at = pl.ds(i * chunk, chunk)
        return pltpu.make_async_copy(dx_buf.at[at], dx.at[at], dx_sem.at[i])

    def move(i):
        for t in range(i * per_piece, (i + 1) * per_piece):
            pltpu.make_async_copy(buf.at[t], buf.at[t], load_sem.at[t]).wait()
            store(t).start()

    load_back.wait()
    for i in range(pieces):
        lanes = pl.ds(i * chunk, chunk)
        d = split3(d_log_ref[:, lanes])
        lefts = jnp.concatenate([d[0], d[0], d[1], d[1], d[0], d[2]], axis=0)
        routed = tn(lefts, rights).astype(BF16)
        slot_col = col_of(slot_ref[0:1, lanes])[:, 0:1]
        chosen = (lax.broadcasted_iota(jnp.int32, (chunk, n), 1).astype(F32) == slot_col).astype(BF16)
        dx_buf[lanes, :] = (nn(chosen, back[...]) + routed.astype(F32)).astype(BF16)
        dx_store(i).start()
        move(2 * i)
        move(2 * i + 1)
    load_out.wait()
    store_out = pltpu.make_async_copy(out_buf, out, out_sem.at[1])
    store_out.start()
    for t in range(tiles):
        store(t).wait()
    for i in range(pieces):
        dx_store(i).wait()
    store_out.wait()


def vmem(count):
    return [pl.BlockSpec(memory_space=pltpu.VMEM)] * count


def cost(flops, size):
    return pl.CostEstimate(flops=int(flops), bytes_accessed=int(size), transcendentals=0)


def solution(mesh):
    token_spec = P(ALL_AXES)
    expert_spec = P("ep")

    def local_step(x, modality, router, expert_ids, priority, w_in, b_in, w_out, b_out, dy):
        n, width = x.shape
        experts = router.shape[1]
        hid = w_in.shape[2]
        capacity = n // experts
        tiles = hid // TILE
        share = n // (experts // 2)
        w_in, w_out = w_in[0], w_out[0]
        ids, prio, mod = (a.reshape(n // 128, 128) for a in (expert_ids, priority, modality))
        router_t = jnp.transpose(router)
        shape = jax.ShapeDtypeStruct
        anywhere = pl.BlockSpec(memory_space=pl.ANY)
        dma = pltpu.SemaphoreType.DMA
        slots = (experts, capacity, width)
        mm = 2 * n * width * hid
        others = experts - 1

        summed, back_y, d_back, out, _, _, slot, d_log, loss, small = pl.pallas_call(
            block_kernel,
            out_shape=(
                shape((2 * tiles, 4, 4, 16, width), BF16), shape(slots, BF16), shape(slots, BF16), shape((n, width), BF16),
                shape((n // WIDE, hid, WIDE), BF16), shape((hid // WIDE, n // 16, 16, WIDE), F32),
                shape((8, n), F32), shape((experts, n), F32), shape((8, 128), F32), shape((16, width), F32),
            ),
            in_specs=vmem(3) + [anywhere] * 2 + vmem(1) + [anywhere] + vmem(1) + [anywhere] + vmem(1),
            out_specs=(*[anywhere] * 6, *vmem(4)),
            scratch_shapes=[
                pltpu.VMEM((2 * tiles, 4, 4, 16, width), F32),
                pltpu.VMEM((tiles, 3, 4, 16, width), F32),
                pltpu.VMEM((tiles, 3, 16, width), F32),
                pltpu.VMEM((2 * tiles, 16, width), BF16),
                pltpu.VMEM((n, width), BF16),
                pltpu.VMEM((n, width), BF16),
                pltpu.VMEM(slots, BF16),
                pltpu.VMEM(slots, BF16),
                pltpu.VMEM((width, n), BF16),
                pltpu.VMEM((n, width), BF16),
                pltpu.VMEM((n, width), F32),
                pltpu.VMEM((4, WIDE, WIDE), BF16),
                pltpu.VMEM((2, n // 16, 16, TILE), F32),
                pltpu.VMEM((n, TILE), BF16),
                pltpu.VMEM((2, WIDE, share), BF16),
                pltpu.VMEM((CHUNK, width), BF16),
                pltpu.VMEM((4, 4, 4, 16, width), BF16),
                pltpu.VMEM((n, 8), F32),
                pltpu.VMEM((8, n), F32),
                pltpu.VMEM((8, n), F32),
                pltpu.VMEM((experts, n), F32),
                pltpu.VMEM((1, hid), F32),
                pltpu.VMEM((48, 128), F32),
                pltpu.VMEM((3 * experts, width), F32),
                pltpu.VMEM((4, 48, 128), F32), pltpu.VMEM((4, 4, 48, 128), F32),
                pltpu.VMEM((4, 16, width), F32), pltpu.VMEM((4, 4, 16, width), F32),
                dma((2 * tiles,)), dma((tiles, 6)), dma((2 * tiles, 6)), dma((tiles,)), pltpu.SemaphoreType.REGULAR((tiles, 2)),
                dma, dma((others,)), dma, dma((3,)), dma, dma, dma, dma,
                dma((2,)), dma((2,)), dma, dma((2,)), dma((2,)), dma((3,)), dma((2,)), dma((4,)), dma((2,)), dma((4,)),
                dma((4, 3)), dma((4, 3)),
            ],
            compiler_params=pltpu.CompilerParams(collective_id=1, has_side_effects=True, vmem_limit_bytes=67_000_000),
            cost_estimate=cost(6 * mm, 6 * n * hid), name="block",
        )(ids, prio, mod, x, dy, router_t, w_in, b_in, w_out, b_out)

        d_x, d_w_in, d_w_out, out, d_router, d_b_in, d_b_out, aux = pl.pallas_call(
            final_kernel,
            out_shape=(
                shape((n, width), BF16), shape((width, hid), BF16), shape((hid, width), BF16), shape((n, width), BF16),
                shape((experts, width), F32), shape((1, hid), BF16), shape((1, width), BF16), shape((1, 1), F32),
            ),
            in_specs=vmem(2) + [anywhere] + vmem(3) + [anywhere] * 2,
            out_specs=(*[anywhere] * 4, *vmem(3), pl.BlockSpec(memory_space=pltpu.SMEM)),
            scratch_shapes=[
                pltpu.VMEM((2 * tiles, 4, 4, 3, 16, TILE), BF16),
                pltpu.VMEM((n, width), BF16), pltpu.VMEM((n, width), BF16), pltpu.VMEM((n, width), BF16),
                dma((2 * tiles,)), dma((2 * tiles,)), dma, dma((2,)), dma((n // (2 * CHUNK),)),
            ],
            compiler_params=pltpu.CompilerParams(vmem_limit_bytes=66_000_000),
            cost_estimate=cost(2 * n * n * width, 8 * width * hid), name="final",
        )(slot, d_log, d_back.reshape(n, width), router_t, small, loss, summed, out)
        return out, aux[0, 0], d_x, jnp.transpose(d_router), d_w_in[None], d_b_in, d_w_out[None], d_b_out

    return jax.shard_map(
        local_step,
        mesh=mesh,
        in_specs=(token_spec, token_spec, P(), token_spec, token_spec, expert_spec, expert_spec, expert_spec, expert_spec, token_spec),
        out_specs=(token_spec, P(), token_spec, P(), expert_spec, expert_spec, expert_spec, expert_spec),
        check_vma=False,
    )
```
